32 devices in a mesh: lat: 4 (over y, x), lon: 8 (over z, core).
Axes of the slice: x: 2, y: 2, z: 4, core: 2. Of those that a mesh axis runs over, the one named last changes fastest.
Arguments:
- ensemble: bfloat16 [32, 32, 10240], P('lon', 'lat'), may hold values from -0.625 to 0.625
- innovation: float32 [64, 64, 128], P('lon', 'lat'), may hold values from -6 to 6
- obs_weight: float32 [64, 64, 128], P('lon', 'lat'), may hold values from 0.5 to 20
- lat_offset: int32 [64], P('lat'), may hold values from 0 to 3
- lat_weight: float32 [64], P('lat'), may hold values from 0 to 1
- band_widths: int32 [80], replicated, may hold values from 1 to 63
Outputs:
- coefficients: float32 [2, 2], replicated
- next_vector: bfloat16 [32, 32, 5120], P('lon', 'lat')
The draws below stay inside these ranges and needn't reach their ends.
All inputs are finite; a program needn't handle non-finite values.
Results may differ from the reference program's by a relative error of at most 0.0014.
Values sent between devices are 32-bit elements; how exact they have to be, the bound alone decides.
No kernel may reach another device: no remote copies, remote signals or barrier semaphores. Data moves between devices by JAX's collectives and lax.ppermute only.
A program may use at most 64 MiB of HBM per device.

```python
import math
import jax
import jax.numpy as jnp
from jax import lax

M = 80
LEV = 64
FIELDS = 2
ITERS = 2
NCLAT = 32
NCLON = 32
NFLAT = 64
NFLON = 64


def with_ends(drawn, own_key, least, largest):
    place = [jax.random.randint(jax.random.fold_in(own_key, axis), (), 0, length) for axis, length in enumerate(drawn.shape)]
    widest = drawn.shape.index(max(drawn.shape))
    neighbour = place[:widest] + [(place[widest] + 1) % drawn.shape[widest]] + place[widest + 1:]
    return drawn.at[tuple(place)].set(least).at[tuple(neighbour)].set(largest)


def block_scale(rng, shape, shards, low, high):
    level = 1.0
    for position, blocks in shards:
        steps = jax.random.uniform(jax.random.fold_in(jax.random.fold_in(rng, 6), position), (blocks,), jnp.float32, low / len(shards), high / len(shards))
        level = level * jnp.repeat(jnp.exp(steps), shape[position] // blocks).reshape((-1,) + (1,) * (len(shape) - 1 - position))
    return level


def bell_draw(key, shape, deviation, limit, cuts=(), held_as=jnp.bfloat16):
    level = block_scale(key, shape, cuts, -0.22, 0.18) if cuts else 1.0
    array = jax.random.normal(key, shape, jnp.float32) * deviation * level
    return jnp.minimum(jnp.maximum(array, -limit), limit).astype(held_as)


def setup_inputs(seed: int = 0) -> dict:
    streams_of = jax.random.split(jax.random.key(seed), 7)
    ensemble = bell_draw(streams_of[0], (NCLON, NCLAT, M * FIELDS * LEV), M ** -0.5, 0.625, ((0, 8), (1, 4)))
    innovation = bell_draw(streams_of[1], (NFLON, NFLAT, FIELDS * LEV), 1.0, 6.0, ((0, 8), (1, 4)), jnp.float32)
    obs_weight = jnp.clip(jnp.exp(math.log(20.0) - 3.6888795 * jax.random.uniform(streams_of[2], (NFLON, NFLAT, FIELDS * LEV), jnp.float32) ** block_scale(streams_of[2], (NFLON, NFLAT, FIELDS * LEV), ((0, 8), (1, 4)), -0.2, 0.2)), 0.5, 20.0)
    lat_offset = with_ends(jax.random.randint(streams_of[3], (NFLAT,), 0, 4), jax.random.fold_in(streams_of[3], 1), 0, 3).astype(jnp.int32)
    lat_weight = jnp.clip(1.0 * jax.random.uniform(streams_of[4], (NFLAT,), jnp.float32) ** block_scale(streams_of[4], (NFLAT,), ((0, 4),), -0.2, 0.2), 0.0, 1.0)
    band_widths = with_ends(jax.random.randint(streams_of[5], (M,), 1, LEV), jax.random.fold_in(streams_of[5], 1), 1, LEV - 1).astype(jnp.int32)
    return dict(ensemble=ensemble, innovation=innovation, obs_weight=obs_weight, lat_offset=lat_offset, lat_weight=lat_weight, band_widths=band_widths)


EVEN_TAPS = (-0.0234375, 0.2265625, 0.8671875, -0.0703125)
ODD_TAPS = (-0.0703125, 0.8671875, 0.2265625, -0.0234375)
EPSILON = 1e-06

def tent_matrix(band_widths, levels):
    level_ids = jnp.arange(levels, dtype=jnp.int32)
    distance = jnp.abs(level_ids[:, None] - level_ids[None, :]).astype(jnp.float32)
    widths = (band_widths + 1).astype(jnp.float32)[:, None, None]
    return jnp.maximum(0.0, 1.0 - distance[None] / widths) / widths

def tap_sum(padded, taps, first, length):
    result = taps[0] * padded[first:first + length]
    for offset in range(1, 4):
        result = result + taps[offset] * padded[first + offset:first + offset + length]
    return result

def fold_taps(padded, taps, first, length):
    result = taps[0] * padded[first:first + 2 * length:2]
    for offset in range(1, 4):
        start_at = first - 2 * offset
        result = result + taps[offset] * padded[start_at:start_at + 2 * length:2]
    return result

def localize_rows(values, tent):
    shaped = values.reshape(values.shape[0], M, LEV)
    mapped = jnp.einsum('aml,mlk->amk', shaped, tent, precision=lax.Precision.HIGHEST)
    return mapped.reshape(values.shape[0], M * LEV)

def reference(ensemble, innovation, obs_weight, lat_offset, lat_weight, band_widths):
    tent = tent_matrix(band_widths, LEV)
    fine_rows = jnp.arange(NFLAT, dtype=jnp.int32)
    lower = fine_rows // 2 - 2 + lat_offset
    columns = jnp.arange(NCLAT, dtype=jnp.int32)
    interp = (1.0 - lat_weight)[:, None] * (columns[None, :] == lower[:, None]) + lat_weight[:, None] * (columns[None, :] == lower[:, None] + 1)
    entries = float(NCLON * NCLAT * M * LEV)

    def combine(vector):

        def one_column(pieces):
            ens_col, vec_col = pieces
            weights = localize_rows(vec_col, tent)
            shaped = ens_col.astype(jnp.float32).reshape(NCLAT, M, FIELDS, LEV)
            summed = lax.optimization_barrier(jnp.sum(shaped * weights.reshape(NCLAT, M, 1, LEV), axis=1))
            return summed.reshape(NCLAT, FIELDS * LEV)
        return lax.map(one_column, (ensemble, vector))

    def spread(coarse):

        def one_column(pieces):
            ens_col, grad_col = pieces
            shaped = ens_col.astype(jnp.float32).reshape(NCLAT, M, FIELDS, LEV)
            summed = lax.optimization_barrier(jnp.sum(shaped * grad_col.reshape(NCLAT, 1, FIELDS, LEV), axis=2))
            return localize_rows(summed.reshape(NCLAT, M * LEV), tent)
        return lax.map(one_column, (ensemble, coarse))

    def prolong(increment):
        fine_lat = jnp.einsum('ri,cil->crl', interp, increment, precision=lax.Precision.HIGHEST)
        padded = jnp.concatenate([fine_lat[-2:], fine_lat, fine_lat[:2]], axis=0)
        even_cols = tap_sum(padded, EVEN_TAPS, 0, NCLON)
        odd_cols = tap_sum(padded, ODD_TAPS, 1, NCLON)
        return jnp.stack([even_cols, odd_cols], axis=1).reshape(NFLON, NFLAT, FIELDS * LEV)

    def restrict(fine):
        padded = jnp.concatenate([fine[-3:], fine, fine[:3]], axis=0)
        coarse_lon = fold_taps(padded, EVEN_TAPS, 7, NCLON) + fold_taps(padded, ODD_TAPS, 6, NCLON)
        return jnp.einsum('ri,crl->cil', interp, coarse_lon, precision=lax.Precision.HIGHEST)

    def hessian(vector):
        return vector + spread(restrict(obs_weight * prolong(combine(vector))))
    current = spread(restrict(obs_weight * innovation))
    basis = []
    diagonal = []
    off_diagonal = []
    for step in range(ITERS):
        norm_value = jnp.sqrt(jnp.sum(current * current) / entries + EPSILON)
        normed = current / norm_value
        image = hessian(normed)
        basis.append(normed)
        dots = [jnp.sum(member * image) / entries for member in basis]
        for member, weight in zip(basis, dots):
            image = image - weight * member
        diagonal.append(dots[-1])
        off_diagonal.append(norm_value)
        current = image
    coefficients = jnp.stack([jnp.stack(diagonal), jnp.stack(off_diagonal)]).astype(jnp.float32)
    return (coefficients, current.astype(jnp.bfloat16))
```

```python
import jax
import jax.numpy as jnp
from jax import lax
from jax.experimental import pallas as pl
from jax.experimental.pallas import tpu as pltpu
from jax.sharding import PartitionSpec as P

M = 80
LEV = 64
FIELDS = 2

EVEN_TAPS = (-0.0234375, 0.2265625, 0.8671875, -0.0703125)
ODD_TAPS = (-0.0703125, 0.8671875, 0.2265625, -0.0234375)
EPSILON = 1e-06

F32 = jnp.float32
BF16 = jnp.bfloat16
CH = FIELDS * LEV
PAIRS = M // 2
PAD = 8
VMEM_SPEC = pl.BlockSpec(memory_space=pltpu.VMEM)


def in_vmem(value):
    return pltpu.with_memory_space_constraint(value, pltpu.VMEM)


def kernel_call(body, outs, operands, scratch=()):
    return pl.pallas_call(
        body,
        out_shape=outs,
        in_specs=[VMEM_SPEC] * len(operands),
        out_specs=jax.tree.map(lambda _: VMEM_SPEC, outs),
        scratch_shapes=list(scratch),
    )(*[in_vmem(operand) for operand in operands])


def split(value):
    high = value.astype(BF16)
    return high, (value - high.astype(F32)).astype(BF16)


def pair_distances():
    row = lax.broadcasted_iota(jnp.int32, (CH, CH), 0)
    col = lax.broadcasted_iota(jnp.int32, (CH, CH), 1)
    distance = jnp.where(row // LEV == col // LEV, jnp.abs(row - col), CH)
    return distance.astype(F32).astype(BF16).reshape(CH // 16, 16, CH)


def hat(widths_ref, pair, distances):
    widths = jnp.broadcast_to(widths_ref[pair : pair + 1, :], (16, CH)).astype(BF16)
    return jnp.maximum(widths[None] - distances, jnp.zeros((), BF16)).reshape(CH, CH)


def product(value, matrix):
    cells = value.shape[0]
    parts = jnp.concatenate(split(value), axis=0)
    both = jnp.dot(parts, matrix, preferred_element_type=F32)
    return both[:cells] + both[cells:]


def swap_halves(value):
    return pltpu.roll(value, LEV, 1)


def members(ens_ref, pair):
    first = ens_ref[:, pair * 2 * CH : (pair * 2 + 1) * CH].astype(F32)
    second = ens_ref[:, (pair * 2 + 1) * CH : (pair * 2 + 2) * CH].astype(F32)
    return first, second


def field_sum(first, second, coarse, low_half):
    left, right = first * coarse, second * coarse
    return jnp.where(low_half, left, right) + swap_halves(jnp.where(low_half, right, left))


def gram(ens_ref, widths_ref, scales_ref, coarse):
    distances = pair_distances()
    low_half = lax.broadcasted_iota(jnp.int32, coarse.shape, 1) < LEV
    total = jnp.zeros(coarse.shape, F32)
    for pair in range(PAIRS):
        matrix = hat(widths_ref, pair, distances)
        first, second = members(ens_ref, pair)
        summed = field_sum(first, second, coarse, low_half)
        scale = scales_ref[pair : pair + 1, :]
        twice = product(product(summed, matrix), matrix) * (scale * scale)
        swapped = swap_halves(twice)
        total = total + (
            first * jnp.where(low_half, twice, swapped)
            + second * jnp.where(low_half, swapped, twice)
        )
    return total


def lat_coefficients(stencil_ref, fine):
    weight, offset = stencil_ref[0:fine, :], stencil_ref[fine : 2 * fine, :]
    result = []
    for step in range(5):
        lower = jnp.where(offset == float(step), 1.0 - weight, 0.0)
        result.append(lower + jnp.where(offset == float(step - 1), weight, 0.0))
    return result


def restrict_block(even, odd, coefs, spill_ref, sum_ref, cols, rows):
    fine = 2 * rows + 8
    blocks = []
    for col in range(cols):
        folded = None
        for tap in range(4):
            term = EVEN_TAPS[tap] * even[col + 3 - tap] + ODD_TAPS[tap] * odd[col + 3 - tap]
            folded = term if folded is None else folded + term
        total = None
        for step in range(5):
            slot = col * 5 + step
            spill_ref[slot] = coefs[step] * folded
            term = spill_ref[slot, 8 - 2 * step : 8 - 2 * step + 2 * rows, :]
            total = term if total is None else total + term
        sum_ref[col] = total
        blocks.append(
            sum_ref[col, pl.ds(0, rows, stride=2), :] + sum_ref[col, pl.ds(1, rows, stride=2), :]
        )
    return jnp.concatenate(blocks, axis=0)


def middle(mid_ref, left_ref, right_ref, weight_ref, coefs, dup_ref, spill_ref, sum_ref):
    cols, rows = mid_ref.shape[0], mid_ref.shape[1] - 2
    fine = 2 * rows + 8
    lat = []
    for col in range(cols + 6):
        if col < 3:
            block = left_ref[col]
        elif col < cols + 3:
            block = mid_ref[col - 3]
        else:
            block = right_ref[col - cols - 3]
        dup_ref[col] = jnp.zeros(dup_ref.shape[1:], F32)
        dup_ref[col, pl.ds(PAD, rows + 2, stride=2), :] = block
        dup_ref[col, pl.ds(PAD + 1, rows + 2, stride=2), :] = block
        total = None
        for step in range(5):
            term = coefs[step] * dup_ref[col, 2 + 2 * step : 2 + 2 * step + fine, :]
            total = term if total is None else total + term
        lat.append(total)
    even, odd = [], []
    for at in range(cols + 3):
        first = sum(EVEN_TAPS[tap] * lat[at + tap] for tap in range(4))
        second = sum(ODD_TAPS[tap] * lat[at + tap] for tap in range(4))
        even.append(first * weight_ref[2 * at + 1, 0:fine, :])
        odd.append(second * weight_ref[2 * at, 0:fine, :])
    return restrict_block(even, odd, coefs, spill_ref, sum_ref, cols, rows)


def start_kernel(cols, rows):
    fine = 2 * rows + 8

    def body(weight_ref, stencil_ref, ens_ref, widths_ref, scales_ref, coarse_ref, image_ref, spill_ref, sum_ref):
        coefs = lat_coefficients(stencil_ref, fine)
        even = [weight_ref[2 * at + 1, fine : 2 * fine, :] for at in range(cols + 3)]
        odd = [weight_ref[2 * at, fine : 2 * fine, :] for at in range(cols + 3)]
        coarse = restrict_block(even, odd, coefs, spill_ref, sum_ref, cols, rows)
        coarse_ref[...] = coarse
        image_ref[...] = gram(ens_ref, widths_ref, scales_ref, coarse)

    return body


def step_kernel(cols, rows):
    fine = 2 * rows + 8

    def body(mid_ref, left_ref, right_ref, weight_ref, stencil_ref, ens_ref, widths_ref, scales_ref,
             coarse_ref, image_ref, dup_ref, spill_ref, sum_ref):
        coefs = lat_coefficients(stencil_ref, fine)
        coarse = middle(mid_ref, left_ref, right_ref, weight_ref, coefs, dup_ref, spill_ref, sum_ref)
        coarse_ref[...] = coarse
        image_ref[...] = gram(ens_ref, widths_ref, scales_ref, coarse)

    return body


def last_kernel(cols, rows, devices):
    fine = 2 * rows + 8

    def body(mid_ref, left_ref, right_ref, weight_ref, stencil_ref, y0_ref, b0_ref, y1_ref, b1_ref,
             coarse_ref, dots_ref, dup_ref, spill_ref, sum_ref):
        coefs = lat_coefficients(stencil_ref, fine)
        coarse = middle(mid_ref, left_ref, right_ref, weight_ref, coefs, dup_ref, spill_ref, sum_ref)
        coarse_ref[...] = coarse
        lane = lax.broadcasted_iota(jnp.int32, (1, CH), 1)
        row = jnp.zeros((1, CH), F32)
        b0, b1, y1 = b0_ref[...], b1_ref[...], y1_ref[...]
        pairs = (y0_ref[...] * b0, y1 * b0, y1 * b1, coarse * b1)
        for place, terms in enumerate(pairs):
            total = jnp.sum(jnp.sum(terms, axis=0, keepdims=True), axis=1, keepdims=True)
            row = jnp.where(lane == place, total, row)
        dots_ref[...] = jnp.broadcast_to(row, (devices, CH))

    return body


def final_kernel(entries):
    def body(dots_ref, y0_ref, y1_ref, y2_ref, ens_ref, widths_ref, scales_ref, coef_ref, vector_ref):
        sums = jnp.sum(dots_ref[...], axis=0, keepdims=True)
        lane = lax.broadcasted_iota(jnp.int32, (1, CH), 1)

        def pick(place):
            return jnp.sum(jnp.where(lane == place, sums, 0.0), axis=1, keepdims=True)

        m00, m01, m11, m12 = (pick(place) for place in range(4))
        beta0 = jnp.sqrt(m00 / entries + EPSILON)
        alpha0 = (m00 + m01) / (entries * beta0 * beta0)
        s1 = 1.0 / beta0
        s0 = (1.0 - alpha0) * s1
        u1u1 = s0 * s0 * m00 + 2.0 * s0 * s1 * m01 + s1 * s1 * m11
        beta1 = jnp.sqrt(u1u1 / entries + EPSILON)
        u0u1 = s0 * m00 + s1 * m01
        u0lu1 = s0 * m01 + s1 * m11
        u1lu1 = s0 * s0 * m01 + 2.0 * s0 * s1 * m11 + s1 * s1 * m12
        c0 = (u0u1 + u0lu1) / (entries * beta0 * beta1)
        alpha1 = (u1u1 + u1lu1) / (entries * beta1 * beta1)
        r1 = 1.0 / beta1
        keep = (1.0 - alpha1) * r1
        k0 = keep * s0 - c0 / beta0
        k1 = keep * s1 + s0 * r1
        k2 = s1 * r1
        row = lax.broadcasted_iota(jnp.int32, (2, 2), 0)
        col = lax.broadcasted_iota(jnp.int32, (2, 2), 1)
        coef_ref[...] = jnp.where(
            row == 0, jnp.where(col == 0, alpha0, alpha1), jnp.where(col == 0, beta0, beta1)
        )
        coarse = k0 * y0_ref[...] + k1 * y1_ref[...] + k2 * y2_ref[...]
        distances = pair_distances()
        low_half = lax.broadcasted_iota(jnp.int32, coarse.shape, 1) < LEV
        for pair in range(PAIRS):
            matrix = hat(widths_ref, pair, distances)
            first, second = members(ens_ref, pair)
            summed = field_sum(first, second, coarse, low_half)
            out = product(summed, matrix) * scales_ref[pair : pair + 1, :]
            vector_ref[:, pair * CH : (pair + 1) * CH] = out.astype(BF16)

    return body


def shift(value, axis, step):
    count = lax.axis_size(axis)
    return lax.ppermute(value, axis, [(at, (at + step) % count) for at in range(count)])


def per_device(ensemble, innovation, obs_weight, lat_offset, lat_weight, band_widths):
    cols, rows = ensemble.shape[0], ensemble.shape[1]
    cells = cols * rows
    fine_rows = innovation.shape[1]
    fine = fine_rows + 8
    lat_count, lon_count = lax.axis_size("lat"), lax.axis_size("lon")
    devices = lat_count * lon_count
    entries = float(cells * M * LEV * devices)
    position = lax.axis_index("lat")
    keep_low = (position > 0).astype(F32)
    keep_high = (position < lat_count - 1).astype(F32)

    ens = ensemble.reshape(cells, M * CH)
    widths = jnp.broadcast_to(
        (band_widths + 1).astype(F32).reshape(PAIRS, 2, 1), (PAIRS, 2, LEV)
    ).reshape(PAIRS, CH)
    scales = 1.0 / (widths * widths)

    weighted = obs_weight * innovation
    weight_row = jnp.broadcast_to(lat_weight[:, None], (fine_rows, CH))
    offset_row = jnp.broadcast_to(lat_offset.astype(F32)[:, None], (fine_rows, CH))

    def edge(at):
        part = slice(at, at + 4)
        fields = jnp.concatenate([obs_weight[:, part], weighted[:, part]], axis=1)
        stencil = jnp.concatenate([weight_row[part], offset_row[part]], axis=0)
        return jnp.concatenate([fields, stencil[None]], axis=0)

    low = shift(edge(fine_rows - 4), "lat", 1)
    high = shift(edge(0), "lat", -1)
    low_fields, high_fields = low[:-1] * keep_low, high[:-1] * keep_high
    stencil = jnp.concatenate(
        [low[-1, :4], weight_row, high[-1, :4], low[-1, 4:], offset_row, high[-1, 4:]], axis=0
    )
    tall = jnp.concatenate(
        [low_fields[:, :4], obs_weight, high_fields[:, :4],
         low_fields[:, 4:], weighted, high_fields[:, 4:]], axis=1
    )
    left = shift(tall[-3:], "lon", 1)
    right = shift(tall[:3], "lon", -1)
    weight = jnp.concatenate([left, tall, right], axis=0)

    cell_block = pltpu.VMEM((cells, CH), F32)
    restrict_scratch = (
        pltpu.VMEM((cols * 5, fine, CH), F32),
        pltpu.VMEM((cols, 2 * rows, CH), F32),
    )
    middle_scratch = (pltpu.VMEM((cols + 6, fine + 16, CH), F32),) + restrict_scratch

    def padded(image):
        block = image.reshape(cols, rows, CH)
        low_row = shift(block[:, -1], "lat", 1) * keep_low
        high_row = shift(block[:, 0], "lat", -1) * keep_high
        mid = jnp.concatenate([low_row[:, None], block, high_row[:, None]], axis=1)
        return mid, shift(mid[-3:], "lon", 1), shift(mid[:3], "lon", -1)

    y0, b0 = kernel_call(
        start_kernel(cols, rows), (cell_block, cell_block),
        (weight, stencil, ens, widths, scales), restrict_scratch,
    )
    y1, b1 = kernel_call(
        step_kernel(cols, rows), (cell_block, cell_block),
        (*padded(b0), weight, stencil, ens, widths, scales), middle_scratch,
    )
    y2, dots = kernel_call(
        last_kernel(cols, rows, devices), (cell_block, pltpu.VMEM((devices, CH), F32)),
        (*padded(b1), weight, stencil, y0, b0, y1, b1), middle_scratch,
    )
    shared = lax.all_to_all(dots.reshape(devices, 1, CH), ("lat", "lon"), 0, 0).reshape(devices, CH)
    coefficients, vector = kernel_call(
        final_kernel(entries),
        (jax.ShapeDtypeStruct((2, 2), F32), jax.ShapeDtypeStruct((cells, M * LEV), BF16)),
        (shared, y0, y1, y2, ens, widths, scales),
    )
    return coefficients, vector.reshape(cols, rows, M * LEV)


def solution(mesh):
    return jax.shard_map(
        per_device,
        mesh=mesh,
        in_specs=(
            P("lon", "lat", None),
            P("lon", "lat", None),
            P("lon", "lat", None),
            P("lat"),
            P("lat"),
            P(),
        ),
        out_specs=(P(), P("lon", "lat", None)),
        check_vma=False,
    )
```

```python
import jax
import jax.numpy as jnp
from jax import lax
from jax.experimental import pallas as pl
from jax.experimental.pallas import tpu as pltpu
from jax.sharding import PartitionSpec as P

M = 80
LEV = 64
FIELDS = 2

EVEN_TAPS = (-0.0234375, 0.2265625, 0.8671875, -0.0703125)
ODD_TAPS = (-0.0703125, 0.8671875, 0.2265625, -0.0234375)
EPSILON = 1e-06

F32 = jnp.float32
BF16 = jnp.bfloat16
CH = FIELDS * LEV
PAIRS = M // 2
PAD = 8
FINE_HALO = 6
VMEM_SPEC = pl.BlockSpec(memory_space=pltpu.VMEM)


def in_vmem(value):
    return pltpu.with_memory_space_constraint(value, pltpu.VMEM)


def kernel_call(body, outs, operands, scratch=()):
    return pl.pallas_call(
        body,
        out_shape=outs,
        in_specs=[VMEM_SPEC] * len(operands),
        out_specs=jax.tree.map(lambda _: VMEM_SPEC, outs),
        scratch_shapes=list(scratch),
    )(*[in_vmem(operand) for operand in operands])


def split(value):
    high = value.astype(BF16)
    return high, (value - high.astype(F32)).astype(BF16)


def pair_distances():
    row = lax.broadcasted_iota(jnp.int32, (CH, CH), 0)
    col = lax.broadcasted_iota(jnp.int32, (CH, CH), 1)
    distance = jnp.where(row // LEV == col // LEV, jnp.abs(row - col), CH)
    return distance.astype(F32).astype(BF16).reshape(CH // 16, 16, CH)


def hat(widths_ref, pair, distances):
    widths = jnp.broadcast_to(widths_ref[pair : pair + 1, :], (16, CH)).astype(BF16)
    return jnp.maximum(widths[None] - distances, jnp.zeros((), BF16)).reshape(CH, CH)


def product(value, matrix):
    cells = value.shape[0]
    parts = jnp.concatenate(split(value), axis=0)
    both = jnp.dot(parts, matrix, preferred_element_type=F32)
    return both[:cells] + both[cells:]


def swap_halves(value):
    return pltpu.roll(value, LEV, 1)


def members(ens_refs, pair):
    result = []
    for member in (2 * pair, 2 * pair + 1):
        parts = [ref[:, member * CH : (member + 1) * CH].astype(F32) for ref in ens_refs]
        result.append(parts[0] if len(parts) == 1 else jnp.concatenate(parts, axis=0))
    return result


def field_sum(first, second, coarse, low_half):
    left, right = first * coarse, second * coarse
    return jnp.where(low_half, left, right) + swap_halves(jnp.where(low_half, right, left))


def gram(ens_refs, widths_ref, scales_ref, coarse):
    distances = pair_distances()
    low_half = lax.broadcasted_iota(jnp.int32, coarse.shape, 1) < LEV
    total = jnp.zeros(coarse.shape, F32)
    for pair in range(PAIRS):
        matrix = hat(widths_ref, pair, distances)
        first, second = members(ens_refs, pair)
        summed = field_sum(first, second, coarse, low_half)
        scale = scales_ref[pair : pair + 1, :]
        twice = product(product(summed, matrix), matrix) * (scale * scale)
        swapped = swap_halves(twice)
        total = total + (
            first * jnp.where(low_half, twice, swapped)
            + second * jnp.where(low_half, swapped, twice)
        )
    return total


def prepare_kernel():
    depth = FINE_HALO

    def body(weight_ref, innovation_ref, lat_weight_ref, lat_offset_ref, band_ref,
             up_ref, down_ref, own_ref, own_stencil_ref, widths_ref, scales_ref):
        fine_cols, fine_rows = weight_ref.shape[0], weight_ref.shape[1]
        for col in range(fine_cols):
            weight = weight_ref[col]
            weighted = weight * innovation_ref[col]
            own_ref[col, 0:fine_rows, :] = weight
            own_ref[col, fine_rows : 2 * fine_rows, :] = weighted
            at = 2 * depth * col
            up_ref[at : at + depth, :] = weight[fine_rows - depth :]
            up_ref[at + depth : at + 2 * depth, :] = weighted[fine_rows - depth :]
            down_ref[at : at + depth, :] = weight[:depth]
            down_ref[at + depth : at + 2 * depth, :] = weighted[:depth]
        row = lax.broadcasted_iota(jnp.int32, (fine_rows, fine_rows), 0)
        col = lax.broadcasted_iota(jnp.int32, (fine_rows, fine_rows), 1)

        def column(line):
            spread = jnp.broadcast_to(line, (fine_rows, fine_rows))
            values = jnp.sum(jnp.where(row == col, spread, 0.0), axis=1, keepdims=True)
            return jnp.broadcast_to(values, (fine_rows, CH))

        weight = column(lat_weight_ref[...])
        offset = column(lat_offset_ref[...].astype(F32))
        own_stencil_ref[0:fine_rows, :] = weight
        own_stencil_ref[fine_rows : 2 * fine_rows, :] = offset
        at = 2 * depth * fine_cols
        up_ref[at : at + depth, :] = weight[fine_rows - depth :]
        up_ref[at + depth : at + 2 * depth, :] = offset[fine_rows - depth :]
        down_ref[at : at + depth, :] = weight[:depth]
        down_ref[at + depth : at + 2 * depth, :] = offset[:depth]
        bands = jnp.broadcast_to((band_ref[...] + 1).astype(F32), (PAIRS, M))
        pair = lax.broadcasted_iota(jnp.int32, (PAIRS, M), 0)
        member = lax.broadcasted_iota(jnp.int32, (PAIRS, M), 1)
        first = jnp.sum(jnp.where(member == 2 * pair, bands, 0.0), axis=1, keepdims=True)
        second = jnp.sum(jnp.where(member == 2 * pair + 1, bands, 0.0), axis=1, keepdims=True)
        lane = lax.broadcasted_iota(jnp.int32, (PAIRS, CH), 1)
        widths = jnp.where(lane < LEV, first, second)
        widths_ref[...] = widths
        scales_ref[...] = 1.0 / (widths * widths)

    return body


def join_kernel():
    depth = FINE_HALO

    def body(low_ref, high_ref, own_ref, own_stencil_ref, flags_ref, tall_ref, stencil_ref):
        fine_cols, fine_rows = own_ref.shape[0], own_ref.shape[1] // 2
        total = fine_rows + 2 * depth
        keep_low, keep_high = flags_ref[0:1, :], flags_ref[1:2, :]
        for part in range(2):
            base = part * total
            for col in range(fine_cols):
                at = 2 * depth * col + part * depth
                tall_ref[col, base : base + depth, :] = low_ref[at : at + depth, :] * keep_low
                tall_ref[col, base + depth : base + depth + fine_rows, :] = own_ref[
                    col, part * fine_rows : (part + 1) * fine_rows, :
                ]
                tall_ref[col, base + depth + fine_rows : base + total, :] = (
                    high_ref[at : at + depth, :] * keep_high
                )
            at = 2 * depth * fine_cols + part * depth
            stencil_ref[base : base + depth, :] = low_ref[at : at + depth, :]
            stencil_ref[base + depth : base + depth + fine_rows, :] = own_stencil_ref[
                part * fine_rows : (part + 1) * fine_rows, :
            ]
            stencil_ref[base + depth + fine_rows : base + total, :] = high_ref[at : at + depth, :]

    return body


def edges_kernel(cols, rows):
    def body(ens_ref, after_ref, up_ref, down_ref):
        row = lax.broadcasted_iota(jnp.int32, (8, CH), 0)
        for member in range(M):
            lanes = slice(member * CH, (member + 1) * CH)
            block = ens_ref[:, lanes].astype(F32)
            for ref, at in ((up_ref, rows - 1), (down_ref, 0)):
                picked = jnp.zeros((8, CH), F32)
                for col in range(cols):
                    line = block[col * rows + at : col * rows + at + 1]
                    picked = jnp.where(row == col, jnp.broadcast_to(line, (8, CH)), picked)
                ref[:, lanes] = picked[:cols]

    return body


def fine_span(rows, halo):
    return FINE_HALO - 4 - 2 * halo, 2 * rows + 8 + 4 * halo


def lat_coefficients(stencil_ref, rows, halo):
    first, count = fine_span(rows, halo)
    total = 2 * rows + 2 * FINE_HALO
    weight = stencil_ref[first : first + count, :]
    offset = stencil_ref[total + first : total + first + count, :]
    result = []
    for step in range(5):
        lower = jnp.where(offset == float(step), 1.0 - weight, 0.0)
        result.append(lower + jnp.where(offset == float(step - 1), weight, 0.0))
    return result


def restrict_block(even, odd, coefs, spill_ref, sum_ref, cols, rows, halo):
    count = fine_span(rows, halo)[1]
    out = rows + 2 * halo
    for col in range(cols):
        folded = None
        for tap in range(4):
            term = EVEN_TAPS[tap] * even[col + 3 - tap] + ODD_TAPS[tap] * odd[col + 3 - tap]
            folded = term if folded is None else folded + term
        total = None
        for step in range(5):
            slot = col * 5 + step
            spill_ref[slot, 0:count, :] = coefs[step] * folded
            term = spill_ref[slot, 8 - 2 * step : 8 - 2 * step + 2 * out, :]
            total = term if total is None else total + term
        sum_ref[col, 0 : 2 * out, :] = total
    blocks = [
        sum_ref[col, pl.ds(2 * halo, rows, stride=2), :]
        + sum_ref[col, pl.ds(2 * halo + 1, rows, stride=2), :]
        for col in range(cols)
    ]
    return jnp.concatenate(blocks, axis=0)


def middle(mid_ref, left_ref, right_ref, weight_ref, coefs, dup_ref, spill_ref, sum_ref, rows, halo):
    cols = mid_ref.shape[0]
    first, count = fine_span(rows, halo)
    given = rows + 2 * halo + 2
    lat = []
    for col in range(cols + 6):
        if col < 3:
            block = left_ref[col]
        elif col < cols + 3:
            block = mid_ref[col - 3]
        else:
            block = right_ref[col - cols - 3]
        dup_ref[col] = jnp.zeros(dup_ref.shape[1:], F32)
        dup_ref[col, pl.ds(PAD, given, stride=2), :] = block
        dup_ref[col, pl.ds(PAD + 1, given, stride=2), :] = block
        total = None
        for step in range(5):
            at = 2 + 2 * step
            term = coefs[step] * dup_ref[col, at : at + count, :]
            total = term if total is None else total + term
        lat.append(total)
    even, odd = [], []
    for at in range(cols + 3):
        left = sum(EVEN_TAPS[tap] * lat[at + tap] for tap in range(4))
        right = sum(ODD_TAPS[tap] * lat[at + tap] for tap in range(4))
        even.append(left * weight_ref[2 * at + 1, first : first + count, :])
        odd.append(right * weight_ref[2 * at, first : first + count, :])
    return restrict_block(even, odd, coefs, spill_ref, sum_ref, cols, rows, halo)


def start_kernel(cols, rows):
    first, count = fine_span(rows, 0)
    base = 2 * rows + 2 * FINE_HALO + first

    def body(weight_ref, stencil_ref, ens_ref, widths_ref, scales_ref, coarse_ref, image_ref, spill_ref, sum_ref):
        coefs = lat_coefficients(stencil_ref, rows, 0)
        even = [weight_ref[2 * at + 1, base : base + count, :] for at in range(cols + 3)]
        odd = [weight_ref[2 * at, base : base + count, :] for at in range(cols + 3)]
        coarse = restrict_block(even, odd, coefs, spill_ref, sum_ref, cols, rows, 0)
        coarse_ref[...] = coarse
        image_ref[...] = gram((ens_ref,), widths_ref, scales_ref, coarse)

    return body


def step_kernel(cols, rows):
    cells = cols * rows

    def body(mid_ref, left_ref, right_ref, weight_ref, stencil_ref, flags_ref, ens_ref, ens_low_ref, ens_high_ref,
             widths_ref, scales_ref, coarse_ref, image_ref, padded_ref, dup_ref, spill_ref, sum_ref, rim_ref):
        coefs = lat_coefficients(stencil_ref, rows, 1)
        coarse = middle(
            mid_ref, left_ref, right_ref, weight_ref, coefs, dup_ref, spill_ref, sum_ref, rows, 1
        )
        coarse_ref[...] = coarse
        end = 2 * rows + 2
        for col in range(cols):
            low = sum_ref[col, 0:1, :] + sum_ref[col, 1:2, :]
            high = sum_ref[col, end : end + 1, :] + sum_ref[col, end + 1 : end + 2, :]
            rim_ref[col : col + 1, :] = low * flags_ref[0:1, :]
            rim_ref[cols + col : cols + col + 1, :] = high * flags_ref[1:2, :]
        image = gram(
            (ens_ref, ens_low_ref, ens_high_ref), widths_ref, scales_ref,
            jnp.concatenate([coarse, rim_ref[...]], axis=0),
        )
        image_ref[...] = image[:cells]
        for col in range(cols):
            padded_ref[col, 0:1, :] = image[cells + col : cells + col + 1]
            padded_ref[col, 1 : rows + 1, :] = image[col * rows : (col + 1) * rows]
            padded_ref[col, rows + 1 : rows + 2, :] = image[
                cells + cols + col : cells + cols + col + 1
            ]

    return body


def last_kernel(rows, devices):
    def body(mid_ref, left_ref, right_ref, weight_ref, stencil_ref, y0_ref, b0_ref, y1_ref, b1_ref,
             coarse_ref, dots_ref, dup_ref, spill_ref, sum_ref):
        coefs = lat_coefficients(stencil_ref, rows, 0)
        coarse = middle(
            mid_ref, left_ref, right_ref, weight_ref, coefs, dup_ref, spill_ref, sum_ref, rows, 0
        )
        coarse_ref[...] = coarse
        lane = lax.broadcasted_iota(jnp.int32, (1, CH), 1)
        row = jnp.zeros((1, CH), F32)
        b0, b1, y1 = b0_ref[...], b1_ref[...], y1_ref[...]
        pairs = (y0_ref[...] * b0, y1 * b0, y1 * b1, coarse * b1)
        for place, terms in enumerate(pairs):
            total = jnp.sum(jnp.sum(terms, axis=0, keepdims=True), axis=1, keepdims=True)
            row = jnp.where(lane == place, total, row)
        dots_ref[...] = jnp.broadcast_to(row, (devices, CH))

    return body


def final_kernel(entries):
    def body(dots_ref, y0_ref, y1_ref, y2_ref, ens_ref, widths_ref, scales_ref, coef_ref, vector_ref):
        sums = jnp.sum(dots_ref[...], axis=0, keepdims=True)
        lane = lax.broadcasted_iota(jnp.int32, (1, CH), 1)

        def pick(place):
            return jnp.sum(jnp.where(lane == place, sums, 0.0), axis=1, keepdims=True)

        m00, m01, m11, m12 = (pick(place) for place in range(4))
        beta0 = jnp.sqrt(m00 / entries + EPSILON)
        alpha0 = (m00 + m01) / (entries * beta0 * beta0)
        s1 = 1.0 / beta0
        s0 = (1.0 - alpha0) * s1
        u1u1 = s0 * s0 * m00 + 2.0 * s0 * s1 * m01 + s1 * s1 * m11
        beta1 = jnp.sqrt(u1u1 / entries + EPSILON)
        u0u1 = s0 * m00 + s1 * m01
        u0lu1 = s0 * m01 + s1 * m11
        u1lu1 = s0 * s0 * m01 + 2.0 * s0 * s1 * m11 + s1 * s1 * m12
        c0 = (u0u1 + u0lu1) / (entries * beta0 * beta1)
        alpha1 = (u1u1 + u1lu1) / (entries * beta1 * beta1)
        r1 = 1.0 / beta1
        keep = (1.0 - alpha1) * r1
        k0 = keep * s0 - c0 / beta0
        k1 = keep * s1 + s0 * r1
        k2 = s1 * r1
        row = lax.broadcasted_iota(jnp.int32, (2, 2), 0)
        col = lax.broadcasted_iota(jnp.int32, (2, 2), 1)
        coef_ref[...] = jnp.where(
            row == 0, jnp.where(col == 0, alpha0, alpha1), jnp.where(col == 0, beta0, beta1)
        )
        coarse = k0 * y0_ref[...] + k1 * y1_ref[...] + k2 * y2_ref[...]
        distances = pair_distances()
        low_half = lax.broadcasted_iota(jnp.int32, coarse.shape, 1) < LEV
        for pair in range(PAIRS):
            matrix = hat(widths_ref, pair, distances)
            first, second = members((ens_ref,), pair)
            summed = field_sum(first, second, coarse, low_half)
            out = product(summed, matrix) * scales_ref[pair : pair + 1, :]
            vector_ref[:, pair * CH : (pair + 1) * CH] = out.astype(BF16)

    return body


def from_neighbours(up, down, axis, paired):
    count = lax.axis_size(axis)
    if paired and count % 2 == 0:
        odd = lax.axis_index(axis) % 2 == 1
        outer = [(at, (at + 1) % count if at % 2 else (at - 1) % count) for at in range(count)]
        inner = [(at, at + 1 - 2 * (at % 2)) for at in range(count)]
        far = lax.ppermute(jnp.where(odd, up, down), axis, outer)
        near = lax.ppermute(jnp.where(odd, down, up), axis, inner)
        return jnp.where(odd, near, far), jnp.where(odd, far, near)
    low = lax.ppermute(up, axis, [(at, (at + 1) % count) for at in range(count)])
    high = lax.ppermute(down, axis, [((at + 1) % count, at) for at in range(count)])
    return low, high


def per_device(ensemble, innovation, obs_weight, lat_offset, lat_weight, band_widths):
    cols, rows = ensemble.shape[0], ensemble.shape[1]
    cells = cols * rows
    fine_cols, fine_rows = innovation.shape[0], innovation.shape[1]
    total = fine_rows + 2 * FINE_HALO
    lat_count, lon_count = lax.axis_size("lat"), lax.axis_size("lon")
    devices = lat_count * lon_count
    entries = float(cells * M * LEV * devices)
    position = lax.axis_index("lat")
    keeps = jnp.stack([position > 0, position < lat_count - 1]).astype(F32)
    flags = jnp.broadcast_to(keeps[:, None], (2, CH))
    keep_low, keep_high = keeps[0], keeps[1]

    edge_block = pltpu.VMEM(((fine_cols + 1) * 2 * FINE_HALO, CH), F32)
    pair_block = pltpu.VMEM((PAIRS, CH), F32)
    up, down, own, own_stencil, widths, scales = pl.pallas_call(
        prepare_kernel(),
        out_shape=(
            edge_block, edge_block, pltpu.VMEM((fine_cols, 2 * fine_rows, CH), F32),
            pltpu.VMEM((2 * fine_rows, CH), F32), pair_block, pair_block,
        ),
        in_specs=[VMEM_SPEC] * 5,
        out_specs=(VMEM_SPEC,) * 6,
    )(obs_weight, innovation, lat_weight[None], lat_offset[None], band_widths[None])
    low, high = from_neighbours(up, down, "lat", False)
    tall, stencil = kernel_call(
        join_kernel(),
        (pltpu.VMEM((fine_cols, 2 * total, CH), F32), pltpu.VMEM((2 * total, CH), F32)),
        (low, high, own, own_stencil, flags),
    )
    left, right = from_neighbours(tall[-3:], tall[:3], "lon", True)
    weight = jnp.concatenate([left, tall, right], axis=0)

    ens = ensemble.reshape(cells, M * CH)
    edge_rows = pltpu.VMEM((cols, M * CH), F32)
    ens_up, ens_down = kernel_call(edges_kernel(cols, rows), (edge_rows, edge_rows), (ens, stencil))
    ens_low, ens_high = from_neighbours(ens_up, ens_down, "lat", False)

    cell_block = pltpu.VMEM((cells, CH), F32)
    restrict_scratch = (
        pltpu.VMEM((cols * 5, total, CH), F32),
        pltpu.VMEM((cols, 2 * rows + 8, CH), F32),
    )
    middle_scratch = (pltpu.VMEM((cols + 6, total + 16, CH), F32),) + restrict_scratch

    y0, b0 = kernel_call(
        start_kernel(cols, rows), (cell_block, cell_block),
        (weight, stencil, ens, widths, scales), restrict_scratch,
    )
    block = b0.reshape(cols, rows, CH)
    low_rows, high_rows = from_neighbours(block[:, -2:], block[:, :2], "lat", False)
    mid = jnp.concatenate([low_rows * keep_low, block, high_rows * keep_high], axis=1)
    y1, b1, mid1 = kernel_call(
        step_kernel(cols, rows), (cell_block, cell_block, pltpu.VMEM((cols, rows + 2, CH), F32)),
        (mid, *from_neighbours(mid[-3:], mid[:3], "lon", True), weight, stencil, flags,
         ens, ens_low, ens_high, widths, scales),
        middle_scratch + (pltpu.VMEM((2 * cols, CH), F32),),
    )
    y2, dots = kernel_call(
        last_kernel(rows, devices), (cell_block, pltpu.VMEM((devices, CH), F32)),
        (mid1, *from_neighbours(mid1[-3:], mid1[:3], "lon", True), weight, stencil, y0, b0, y1, b1),
        middle_scratch,
    )
    shared = lax.all_to_all(dots.reshape(devices, 1, CH), ("lat", "lon"), 0, 0).reshape(devices, CH)
    coefficients, vector = kernel_call(
        final_kernel(entries),
        (jax.ShapeDtypeStruct((2, 2), F32), jax.ShapeDtypeStruct((cells, M * LEV), BF16)),
        (shared, y0, y1, y2, ens, widths, scales),
    )
    return coefficients, vector.reshape(cols, rows, M * LEV)


def solution(mesh):
    return jax.shard_map(
        per_device,
        mesh=mesh,
        in_specs=(
            P("lon", "lat", None),
            P("lon", "lat", None),
            P("lon", "lat", None),
            P("lat"),
            P("lat"),
            P(),
        ),
        out_specs=(P(), P("lon", "lat", None)),
        check_vma=False,
    )
```

```python
import jax
import jax.numpy as jnp
from jax import lax
from jax.experimental import pallas as pl
from jax.experimental.pallas import tpu as pltpu
from jax.sharding import PartitionSpec as P

M = 80
LEV = 64
FIELDS = 2

EVEN_TAPS = (-0.0234375, 0.2265625, 0.8671875, -0.0703125)
ODD_TAPS = (-0.0703125, 0.8671875, 0.2265625, -0.0234375)
EPSILON = 1e-06

F32 = jnp.float32
BF16 = jnp.bfloat16
CH = FIELDS * LEV
PAIRS = M // 2
PAD = 8
FINE_HALO = 6
VMEM_SPEC = pl.BlockSpec(memory_space=pltpu.VMEM)


def in_vmem(value):
    return pltpu.with_memory_space_constraint(value, pltpu.VMEM)


def kernel_call(body, outs, operands, scratch=()):
    return pl.pallas_call(
        body,
        out_shape=outs,
        in_specs=[VMEM_SPEC] * len(operands),
        out_specs=jax.tree.map(lambda _: VMEM_SPEC, outs),
        scratch_shapes=list(scratch),
    )(*[in_vmem(operand) for operand in operands])


def split(value):
    high = value.astype(BF16)
    return high, (value - high.astype(F32)).astype(BF16)


def pair_distances():
    row = lax.broadcasted_iota(jnp.int32, (CH, CH), 0)
    col = lax.broadcasted_iota(jnp.int32, (CH, CH), 1)
    distance = jnp.where(row // LEV == col // LEV, jnp.abs(row - col), CH)
    return distance.astype(F32).astype(BF16).reshape(CH // 16, 16, CH)


def hat(widths_ref, pair, distances):
    widths = jnp.broadcast_to(widths_ref[pair : pair + 1, :], (16, CH)).astype(BF16)
    return jnp.maximum(widths[None] - distances, jnp.zeros((), BF16)).reshape(CH, CH)


def product(value, matrix):
    cells = value.shape[0]
    parts = jnp.concatenate(split(value), axis=0)
    both = jnp.dot(parts, matrix, preferred_element_type=F32)
    return both[:cells] + both[cells:]


def swap_halves(value):
    return pltpu.roll(value, LEV, 1)


def members(ens_refs, pair):
    result = []
    for member in (2 * pair, 2 * pair + 1):
        parts = [ref[:, member * CH : (member + 1) * CH].astype(F32) for ref in ens_refs]
        result.append(parts[0] if len(parts) == 1 else jnp.concatenate(parts, axis=0))
    return result


def field_sum(first, second, coarse, low_half):
    left, right = first * coarse, second * coarse
    return jnp.where(low_half, left, right) + swap_halves(jnp.where(low_half, right, left))


def gram(ens_refs, widths_ref, scales_ref, coarse):
    distances = pair_distances()
    low_half = lax.broadcasted_iota(jnp.int32, coarse.shape, 1) < LEV
    total = jnp.zeros(coarse.shape, F32)
    for pair in range(PAIRS):
        matrix = hat(widths_ref, pair, distances)
        first, second = members(ens_refs, pair)
        summed = field_sum(first, second, coarse, low_half)
        scale = scales_ref[pair : pair + 1, :]
        twice = product(product(summed, matrix), matrix) * (scale * scale)
        swapped = swap_halves(twice)
        total = total + (
            first * jnp.where(low_half, twice, swapped)
            + second * jnp.where(low_half, swapped, twice)
        )
    return total


def prepare_kernel():
    depth = FINE_HALO

    def body(weight_ref, innovation_ref, lat_weight_ref, lat_offset_ref, band_ref,
             up_ref, down_ref, own_ref, own_stencil_ref, widths_ref, scales_ref):
        fine_cols, fine_rows = weight_ref.shape[0], weight_ref.shape[1]
        for col in range(fine_cols):
            weight = weight_ref[col]
            weighted = weight * innovation_ref[col]
            own_ref[col, 0:fine_rows, :] = weight
            own_ref[col, fine_rows : 2 * fine_rows, :] = weighted
            at = 2 * depth * col
            up_ref[at : at + depth, :] = weight[fine_rows - depth :]
            up_ref[at + depth : at + 2 * depth, :] = weighted[fine_rows - depth :]
            down_ref[at : at + depth, :] = weight[:depth]
            down_ref[at + depth : at + 2 * depth, :] = weighted[:depth]
        row = lax.broadcasted_iota(jnp.int32, (fine_rows, fine_rows), 0)
        col = lax.broadcasted_iota(jnp.int32, (fine_rows, fine_rows), 1)

        def column(line):
            spread = jnp.broadcast_to(line, (fine_rows, fine_rows))
            values = jnp.sum(jnp.where(row == col, spread, 0.0), axis=1, keepdims=True)
            return jnp.broadcast_to(values, (fine_rows, CH))

        weight = column(lat_weight_ref[...])
        offset = column(lat_offset_ref[...].astype(F32))
        own_stencil_ref[0:fine_rows, :] = weight
        own_stencil_ref[fine_rows : 2 * fine_rows, :] = offset
        at = 2 * depth * fine_cols
        up_ref[at : at + depth, :] = weight[fine_rows - depth :]
        up_ref[at + depth : at + 2 * depth, :] = offset[fine_rows - depth :]
        down_ref[at : at + depth, :] = weight[:depth]
        down_ref[at + depth : at + 2 * depth, :] = offset[:depth]
        bands = jnp.broadcast_to((band_ref[...] + 1).astype(F32), (PAIRS, M))
        pair = lax.broadcasted_iota(jnp.int32, (PAIRS, M), 0)
        member = lax.broadcasted_iota(jnp.int32, (PAIRS, M), 1)
        first = jnp.sum(jnp.where(member == 2 * pair, bands, 0.0), axis=1, keepdims=True)
        second = jnp.sum(jnp.where(member == 2 * pair + 1, bands, 0.0), axis=1, keepdims=True)
        lane = lax.broadcasted_iota(jnp.int32, (PAIRS, CH), 1)
        widths = jnp.where(lane < LEV, first, second)
        widths_ref[...] = widths
        scales_ref[...] = 1.0 / (widths * widths)

    return body


def join_kernel():
    depth = FINE_HALO

    def body(low_ref, high_ref, own_ref, own_stencil_ref, flags_ref, tall_ref, stencil_ref):
        fine_cols, fine_rows = own_ref.shape[0], own_ref.shape[1] // 2
        total = fine_rows + 2 * depth
        keep_low, keep_high = flags_ref[0:1, :], flags_ref[1:2, :]
        for part in range(2):
            base = part * total
            for col in range(fine_cols):
                at = 2 * depth * col + part * depth
                tall_ref[col, base : base + depth, :] = low_ref[at : at + depth, :] * keep_low
                tall_ref[col, base + depth : base + depth + fine_rows, :] = own_ref[
                    col, part * fine_rows : (part + 1) * fine_rows, :
                ]
                tall_ref[col, base + depth + fine_rows : base + total, :] = (
                    high_ref[at : at + depth, :] * keep_high
                )
            at = 2 * depth * fine_cols + part * depth
            stencil_ref[base : base + depth, :] = low_ref[at : at + depth, :]
            stencil_ref[base + depth : base + depth + fine_rows, :] = own_stencil_ref[
                part * fine_rows : (part + 1) * fine_rows, :
            ]
            stencil_ref[base + depth + fine_rows : base + total, :] = high_ref[at : at + depth, :]

    return body


def edges_kernel(cols, rows):
    def body(ens_ref, after_ref, up_ref, down_ref):
        row = lax.broadcasted_iota(jnp.int32, (8, CH), 0)
        for member in range(M):
            lanes = slice(member * CH, (member + 1) * CH)
            block = ens_ref[:, lanes].astype(F32)
            for ref, at in ((up_ref, rows - 1), (down_ref, 0)):
                picked = jnp.zeros((8, CH), F32)
                for col in range(cols):
                    line = block[col * rows + at : col * rows + at + 1]
                    picked = jnp.where(row == col, jnp.broadcast_to(line, (8, CH)), picked)
                ref[:, lanes] = picked[:cols]

    return body


def fine_span(rows, halo):
    return FINE_HALO - 4 - 2 * halo, 2 * rows + 8 + 4 * halo


def lat_coefficients(stencil_ref, rows, halo):
    first, count = fine_span(rows, halo)
    total = 2 * rows + 2 * FINE_HALO
    weight = stencil_ref[first : first + count, :]
    offset = stencil_ref[total + first : total + first + count, :]
    result = []
    for step in range(5):
        lower = jnp.where(offset == float(step), 1.0 - weight, 0.0)
        result.append(lower + jnp.where(offset == float(step - 1), weight, 0.0))
    return result


def restrict_block(even, odd, coefs, spill_ref, sum_ref, cols, rows, halo):
    count = fine_span(rows, halo)[1]
    out = rows + 2 * halo
    for col in range(cols):
        folded = None
        for tap in range(4):
            term = EVEN_TAPS[tap] * even[col + 3 - tap] + ODD_TAPS[tap] * odd[col + 3 - tap]
            folded = term if folded is None else folded + term
        total = None
        for step in range(5):
            slot = col * 5 + step
            spill_ref[slot, 0:count, :] = coefs[step] * folded
            term = spill_ref[slot, 8 - 2 * step : 8 - 2 * step + 2 * out, :]
            total = term if total is None else total + term
        sum_ref[col, 0 : 2 * out, :] = total
    blocks = [
        sum_ref[col, pl.ds(2 * halo, rows, stride=2), :]
        + sum_ref[col, pl.ds(2 * halo + 1, rows, stride=2), :]
        for col in range(cols)
    ]
    return jnp.concatenate(blocks, axis=0)


def middle(mid_ref, left_ref, right_ref, weight_ref, coefs, dup_ref, spill_ref, sum_ref, rows, halo, mask=None):
    cols = mid_ref.shape[0]
    first, count = fine_span(rows, halo)
    given = rows + 2 * halo + 2
    lat = []
    for col in range(cols + 6):
        if col < 3:
            block = left_ref[col]
        elif col < cols + 3:
            block = mid_ref[col - 3]
        else:
            block = right_ref[col - cols - 3]
        if mask is not None:
            block = block * mask
        dup_ref[col] = jnp.zeros(dup_ref.shape[1:], F32)
        dup_ref[col, pl.ds(PAD, given, stride=2), :] = block
        dup_ref[col, pl.ds(PAD + 1, given, stride=2), :] = block
        total = None
        for step in range(5):
            at = 2 + 2 * step
            term = coefs[step] * dup_ref[col, at : at + count, :]
            total = term if total is None else total + term
        lat.append(total)
    even, odd = [], []
    for at in range(cols + 3):
        left = sum(EVEN_TAPS[tap] * lat[at + tap] for tap in range(4))
        right = sum(ODD_TAPS[tap] * lat[at + tap] for tap in range(4))
        even.append(left * weight_ref[2 * at + 1, first : first + count, :])
        odd.append(right * weight_ref[2 * at, first : first + count, :])
    return restrict_block(even, odd, coefs, spill_ref, sum_ref, cols, rows, halo)


def start_kernel(cols, rows):
    first, count = fine_span(rows, 0)
    base = 2 * rows + 2 * FINE_HALO + first

    def body(weight_ref, stencil_ref, ens_ref, widths_ref, scales_ref, coarse_ref, image_ref, spill_ref, sum_ref):
        coefs = lat_coefficients(stencil_ref, rows, 0)
        even = [weight_ref[2 * at + 1, base : base + count, :] for at in range(cols + 3)]
        odd = [weight_ref[2 * at, base : base + count, :] for at in range(cols + 3)]
        coarse = restrict_block(even, odd, coefs, spill_ref, sum_ref, cols, rows, 0)
        coarse_ref[...] = coarse
        image_ref[...] = gram((ens_ref,), widths_ref, scales_ref, coarse)

    return body


def step_kernel(cols, rows):
    cells = cols * rows

    def body(mid_ref, left_ref, right_ref, weight_ref, stencil_ref, flags_ref, ens_ref, ens_low_ref, ens_high_ref,
             widths_ref, scales_ref, coarse_ref, image_ref, padded_ref, dup_ref, spill_ref, sum_ref, rim_ref):
        coefs = lat_coefficients(stencil_ref, rows, 1)
        row = lax.broadcasted_iota(jnp.int32, (rows + 4, CH), 0)
        inside = jnp.where(row < 2, flags_ref[0:1, :], jnp.where(row < rows + 2, 1.0, flags_ref[1:2, :]))
        coarse = middle(
            mid_ref, left_ref, right_ref, weight_ref, coefs, dup_ref, spill_ref, sum_ref, rows, 1, inside
        )
        coarse_ref[...] = coarse
        end = 2 * rows + 2
        for col in range(cols):
            low = sum_ref[col, 0:1, :] + sum_ref[col, 1:2, :]
            high = sum_ref[col, end : end + 1, :] + sum_ref[col, end + 1 : end + 2, :]
            rim_ref[col : col + 1, :] = low * flags_ref[0:1, :]
            rim_ref[cols + col : cols + col + 1, :] = high * flags_ref[1:2, :]
        image = gram(
            (ens_ref, ens_low_ref, ens_high_ref), widths_ref, scales_ref,
            jnp.concatenate([coarse, rim_ref[...]], axis=0),
        )
        image_ref[...] = image[:cells]
        for col in range(cols):
            padded_ref[col, 0:1, :] = image[cells + col : cells + col + 1]
            padded_ref[col, 1 : rows + 1, :] = image[col * rows : (col + 1) * rows]
            padded_ref[col, rows + 1 : rows + 2, :] = image[
                cells + cols + col : cells + cols + col + 1
            ]

    return body


def last_kernel(rows, devices):
    def body(mid_ref, left_ref, right_ref, weight_ref, stencil_ref, y0_ref, b0_ref, y1_ref, b1_ref,
             coarse_ref, dots_ref, dup_ref, spill_ref, sum_ref):
        coefs = lat_coefficients(stencil_ref, rows, 0)
        coarse = middle(
            mid_ref, left_ref, right_ref, weight_ref, coefs, dup_ref, spill_ref, sum_ref, rows, 0
        )
        coarse_ref[...] = coarse
        lane = lax.broadcasted_iota(jnp.int32, (1, CH), 1)
        row = jnp.zeros((1, CH), F32)
        b0, b1, y1 = b0_ref[...], b1_ref[...], y1_ref[...]
        pairs = (y0_ref[...] * b0, y1 * b0, y1 * b1, coarse * b1)
        for place, terms in enumerate(pairs):
            total = jnp.sum(jnp.sum(terms, axis=0, keepdims=True), axis=1, keepdims=True)
            row = jnp.where(lane == place, total, row)
        dots_ref[...] = jnp.broadcast_to(row, (devices, CH))

    return body


def final_kernel(entries):
    def body(dots_ref, y0_ref, y1_ref, y2_ref, ens_ref, widths_ref, scales_ref, coef_ref, vector_ref):
        sums = jnp.sum(dots_ref[...], axis=0, keepdims=True)
        lane = lax.broadcasted_iota(jnp.int32, (1, CH), 1)

        def pick(place):
            return jnp.sum(jnp.where(lane == place, sums, 0.0), axis=1, keepdims=True)

        m00, m01, m11, m12 = (pick(place) for place in range(4))
        beta0 = jnp.sqrt(m00 / entries + EPSILON)
        alpha0 = (m00 + m01) / (entries * beta0 * beta0)
        s1 = 1.0 / beta0
        s0 = (1.0 - alpha0) * s1
        u1u1 = s0 * s0 * m00 + 2.0 * s0 * s1 * m01 + s1 * s1 * m11
        beta1 = jnp.sqrt(u1u1 / entries + EPSILON)
        u0u1 = s0 * m00 + s1 * m01
        u0lu1 = s0 * m01 + s1 * m11
        u1lu1 = s0 * s0 * m01 + 2.0 * s0 * s1 * m11 + s1 * s1 * m12
        c0 = (u0u1 + u0lu1) / (entries * beta0 * beta1)
        alpha1 = (u1u1 + u1lu1) / (entries * beta1 * beta1)
        r1 = 1.0 / beta1
        keep = (1.0 - alpha1) * r1
        k0 = keep * s0 - c0 / beta0
        k1 = keep * s1 + s0 * r1
        k2 = s1 * r1
        row = lax.broadcasted_iota(jnp.int32, (2, 2), 0)
        col = lax.broadcasted_iota(jnp.int32, (2, 2), 1)
        coef_ref[...] = jnp.where(
            row == 0, jnp.where(col == 0, alpha0, alpha1), jnp.where(col == 0, beta0, beta1)
        )
        coarse = k0 * y0_ref[...] + k1 * y1_ref[...] + k2 * y2_ref[...]
        distances = pair_distances()
        low_half = lax.broadcasted_iota(jnp.int32, coarse.shape, 1) < LEV
        for pair in range(PAIRS):
            matrix = hat(widths_ref, pair, distances)
            first, second = members((ens_ref,), pair)
            summed = field_sum(first, second, coarse, low_half)
            out = product(summed, matrix) * scales_ref[pair : pair + 1, :]
            vector_ref[:, pair * CH : (pair + 1) * CH] = out.astype(BF16)

    return body


def from_neighbours(up, down, axis, paired):
    count = lax.axis_size(axis)
    if paired and count % 2 == 0:
        odd = lax.axis_index(axis) % 2 == 1
        outer = [(at, (at + 1) % count if at % 2 else (at - 1) % count) for at in range(count)]
        inner = [(at, at + 1 - 2 * (at % 2)) for at in range(count)]
        far = lax.ppermute(jnp.where(odd, up, down), axis, outer)
        near = lax.ppermute(jnp.where(odd, down, up), axis, inner)
        return jnp.where(odd, near, far), jnp.where(odd, far, near)
    low = lax.ppermute(up, axis, [(at, (at + 1) % count) for at in range(count)])
    high = lax.ppermute(down, axis, [((at + 1) % count, at) for at in range(count)])
    return low, high


def per_device(ensemble, innovation, obs_weight, lat_offset, lat_weight, band_widths):
    cols, rows = ensemble.shape[0], ensemble.shape[1]
    cells = cols * rows
    fine_cols, fine_rows = innovation.shape[0], innovation.shape[1]
    total = fine_rows + 2 * FINE_HALO
    lat_count, lon_count = lax.axis_size("lat"), lax.axis_size("lon")
    devices = lat_count * lon_count
    entries = float(cells * M * LEV * devices)
    position = lax.axis_index("lat")
    keeps = jnp.stack([position > 0, position < lat_count - 1]).astype(F32)
    flags = jnp.broadcast_to(keeps[:, None], (2, CH))

    edge_block = pltpu.VMEM(((fine_cols + 1) * 2 * FINE_HALO, CH), F32)
    pair_block = pltpu.VMEM((PAIRS, CH), F32)
    up, down, own, own_stencil, widths, scales = pl.pallas_call(
        prepare_kernel(),
        out_shape=(
            edge_block, edge_block, pltpu.VMEM((fine_cols, 2 * fine_rows, CH), F32),
            pltpu.VMEM((2 * fine_rows, CH), F32), pair_block, pair_block,
        ),
        in_specs=[VMEM_SPEC] * 5,
        out_specs=(VMEM_SPEC,) * 6,
    )(obs_weight, innovation, lat_weight[None], lat_offset[None], band_widths[None])
    low, high = from_neighbours(up, down, "lat", False)
    tall, stencil = kernel_call(
        join_kernel(),
        (pltpu.VMEM((fine_cols, 2 * total, CH), F32), pltpu.VMEM((2 * total, CH), F32)),
        (low, high, own, own_stencil, flags),
    )
    left, right = from_neighbours(tall[-3:], tall[:3], "lon", True)
    weight = jnp.concatenate([left, tall, right], axis=0)

    ens = ensemble.reshape(cells, M * CH)
    edge_rows = pltpu.VMEM((cols, M * CH), F32)
    ens_up, ens_down = kernel_call(edges_kernel(cols, rows), (edge_rows, edge_rows), (ens, stencil))
    ens_low, ens_high = from_neighbours(ens_up, ens_down, "lat", False)

    cell_block = pltpu.VMEM((cells, CH), F32)
    restrict_scratch = (
        pltpu.VMEM((cols * 5, total, CH), F32),
        pltpu.VMEM((cols, 2 * rows + 8, CH), F32),
    )
    middle_scratch = (pltpu.VMEM((cols + 6, total + 16, CH), F32),) + restrict_scratch

    y0, b0 = kernel_call(
        start_kernel(cols, rows), (cell_block, cell_block),
        (weight, stencil, ens, widths, scales), restrict_scratch,
    )
    block = b0.reshape(cols, rows, CH)
    low_rows, high_rows = from_neighbours(block[:, -2:], block[:, :2], "lat", False)
    mid = jnp.concatenate([low_rows, block, high_rows], axis=1)
    y1, b1, mid1 = kernel_call(
        step_kernel(cols, rows), (cell_block, cell_block, pltpu.VMEM((cols, rows + 2, CH), F32)),
        (mid, *from_neighbours(mid[-3:], mid[:3], "lon", True), weight, stencil, flags,
         ens, ens_low, ens_high, widths, scales),
        middle_scratch + (pltpu.VMEM((2 * cols, CH), F32),),
    )
    y2, dots = kernel_call(
        last_kernel(rows, devices), (cell_block, pltpu.VMEM((devices, CH), F32)),
        (mid1, *from_neighbours(mid1[-3:], mid1[:3], "lon", True), weight, stencil, y0, b0, y1, b1),
        middle_scratch,
    )
    shared = lax.all_to_all(dots.reshape(devices, 1, CH), ("lat", "lon"), 0, 0).reshape(devices, CH)
    coefficients, vector = kernel_call(
        final_kernel(entries),
        (jax.ShapeDtypeStruct((2, 2), F32), jax.ShapeDtypeStruct((cells, M * LEV), BF16)),
        (shared, y0, y1, y2, ens, widths, scales),
    )
    return coefficients, vector.reshape(cols, rows, M * LEV)


def solution(mesh):
    return jax.shard_map(
        per_device,
        mesh=mesh,
        in_specs=(
            P("lon", "lat", None),
            P("lon", "lat", None),
            P("lon", "lat", None),
            P("lat"),
            P("lat"),
            P(),
        ),
        out_specs=(P(), P("lon", "lat", None)),
        check_vma=False,
    )
```

```python
import jax
import jax.numpy as jnp
from jax import lax
from jax.experimental import pallas as pl
from jax.experimental.pallas import tpu as pltpu
from jax.sharding import PartitionSpec as P

M = 80
LEV = 64
FIELDS = 2

EVEN_TAPS = (-0.0234375, 0.2265625, 0.8671875, -0.0703125)
ODD_TAPS = (-0.0703125, 0.8671875, 0.2265625, -0.0234375)
EPSILON = 1e-06

F32 = jnp.float32
BF16 = jnp.bfloat16
CH = FIELDS * LEV
PAIRS = M // 2
PAD = 8
FINE_HALO = 6
VMEM_SPEC = pl.BlockSpec(memory_space=pltpu.VMEM)
SMALL = pltpu.CompilerParams(vmem_limit_bytes=8 << 20)


def in_vmem(value):
    return pltpu.with_memory_space_constraint(value, pltpu.VMEM)


def kernel_call(body, outs, operands, scratch=()):
    return pl.pallas_call(
        body,
        out_shape=outs,
        in_specs=[VMEM_SPEC] * len(operands),
        out_specs=jax.tree.map(lambda _: VMEM_SPEC, outs),
        scratch_shapes=list(scratch),
        compiler_params=SMALL,
    )(*[in_vmem(operand) for operand in operands])


def split(value):
    high = value.astype(BF16)
    return high, (value - high.astype(F32)).astype(BF16)


def pair_distances():
    row = lax.broadcasted_iota(jnp.int32, (CH, CH), 0)
    col = lax.broadcasted_iota(jnp.int32, (CH, CH), 1)
    distance = jnp.where(row // LEV == col // LEV, jnp.abs(row - col), CH)
    return distance.astype(F32).astype(BF16).reshape(CH // 16, 16, CH)


def hat(widths_ref, pair, distances):
    widths = jnp.broadcast_to(widths_ref[pair : pair + 1, :], (16, CH)).astype(BF16)
    return jnp.maximum(widths[None] - distances, jnp.zeros((), BF16)).reshape(CH, CH)


def product(value, matrix):
    cells = value.shape[0]
    parts = jnp.concatenate(split(value), axis=0)
    both = jnp.dot(parts, matrix, preferred_element_type=F32)
    return both[:cells] + both[cells:]


def swap_halves(value):
    return pltpu.roll(value, LEV, 1)


def members(ens_refs, pair):
    result = []
    for member in (2 * pair, 2 * pair + 1):
        parts = [ref[:, member * CH : (member + 1) * CH].astype(F32) for ref in ens_refs]
        result.append(parts[0] if len(parts) == 1 else jnp.concatenate(parts, axis=0))
    return result


def field_sum(first, second, coarse, low_half):
    left, right = first * coarse, second * coarse
    return jnp.where(low_half, left, right) + swap_halves(jnp.where(low_half, right, left))


def gram(ens_refs, widths_ref, scales_ref, coarse):
    distances = pair_distances()
    low_half = lax.broadcasted_iota(jnp.int32, coarse.shape, 1) < LEV
    total = jnp.zeros(coarse.shape, F32)
    for pair in range(PAIRS):
        matrix = hat(widths_ref, pair, distances)
        first, second = members(ens_refs, pair)
        summed = field_sum(first, second, coarse, low_half)
        scale = scales_ref[pair : pair + 1, :]
        twice = product(product(summed, matrix), matrix) * (scale * scale)
        swapped = swap_halves(twice)
        total = total + (
            first * jnp.where(low_half, twice, swapped)
            + second * jnp.where(low_half, swapped, twice)
        )
    return total


def prepare_kernel():
    depth = FINE_HALO

    def body(weight_ref, innovation_ref, lat_weight_ref, lat_offset_ref, band_ref,
             up_ref, down_ref, own_ref, own_stencil_ref, widths_ref, scales_ref):
        fine_cols, fine_rows = weight_ref.shape[0], weight_ref.shape[1]
        for col in range(fine_cols):
            weight = weight_ref[col]
            weighted = weight * innovation_ref[col]
            own_ref[col, 0:fine_rows, :] = weight
            own_ref[col, fine_rows : 2 * fine_rows, :] = weighted
            at = 2 * depth * col
            up_ref[at : at + depth, :] = weight[fine_rows - depth :]
            up_ref[at + depth : at + 2 * depth, :] = weighted[fine_rows - depth :]
            down_ref[at : at + depth, :] = weight[:depth]
            down_ref[at + depth : at + 2 * depth, :] = weighted[:depth]
        row = lax.broadcasted_iota(jnp.int32, (fine_rows, fine_rows), 0)
        col = lax.broadcasted_iota(jnp.int32, (fine_rows, fine_rows), 1)

        def column(line):
            spread = jnp.broadcast_to(line, (fine_rows, fine_rows))
            values = jnp.sum(jnp.where(row == col, spread, 0.0), axis=1, keepdims=True)
            return jnp.broadcast_to(values, (fine_rows, CH))

        weight = column(lat_weight_ref[...])
        offset = column(lat_offset_ref[...].astype(F32))
        own_stencil_ref[0:fine_rows, :] = weight
        own_stencil_ref[fine_rows : 2 * fine_rows, :] = offset
        at = 2 * depth * fine_cols
        up_ref[at : at + depth, :] = weight[fine_rows - depth :]
        up_ref[at + depth : at + 2 * depth, :] = offset[fine_rows - depth :]
        down_ref[at : at + depth, :] = weight[:depth]
        down_ref[at + depth : at + 2 * depth, :] = offset[:depth]
        bands = jnp.broadcast_to((band_ref[...] + 1).astype(F32), (PAIRS, M))
        pair = lax.broadcasted_iota(jnp.int32, (PAIRS, M), 0)
        member = lax.broadcasted_iota(jnp.int32, (PAIRS, M), 1)
        first = jnp.sum(jnp.where(member == 2 * pair, bands, 0.0), axis=1, keepdims=True)
        second = jnp.sum(jnp.where(member == 2 * pair + 1, bands, 0.0), axis=1, keepdims=True)
        lane = lax.broadcasted_iota(jnp.int32, (PAIRS, CH), 1)
        widths = jnp.where(lane < LEV, first, second)
        widths_ref[...] = widths
        scales_ref[...] = 1.0 / (widths * widths)

    return body


def join_kernel():
    depth = FINE_HALO

    def body(low_ref, high_ref, own_ref, own_stencil_ref, flags_ref, tall_ref, stencil_ref):
        fine_cols, fine_rows = own_ref.shape[0], own_ref.shape[1] // 2
        total = fine_rows + 2 * depth
        keep_low, keep_high = flags_ref[0:1, :], flags_ref[1:2, :]
        for part in range(2):
            base = part * total
            for col in range(fine_cols):
                at = 2 * depth * col + part * depth
                tall_ref[col, base : base + depth, :] = low_ref[at : at + depth, :] * keep_low
                tall_ref[col, base + depth : base + depth + fine_rows, :] = own_ref[
                    col, part * fine_rows : (part + 1) * fine_rows, :
                ]
                tall_ref[col, base + depth + fine_rows : base + total, :] = (
                    high_ref[at : at + depth, :] * keep_high
                )
            at = 2 * depth * fine_cols + part * depth
            stencil_ref[base : base + depth, :] = low_ref[at : at + depth, :]
            stencil_ref[base + depth : base + depth + fine_rows, :] = own_stencil_ref[
                part * fine_rows : (part + 1) * fine_rows, :
            ]
            stencil_ref[base + depth + fine_rows : base + total, :] = high_ref[at : at + depth, :]

    return body


def edges_kernel(cols, rows):
    def body(ens_ref, after_ref, up_ref, down_ref):
        row = lax.broadcasted_iota(jnp.int32, (8, CH), 0)
        for member in range(M):
            lanes = slice(member * CH, (member + 1) * CH)
            block = ens_ref[:, lanes].astype(F32)
            for ref, at in ((up_ref, rows - 1), (down_ref, 0)):
                picked = jnp.zeros((8, CH), F32)
                for col in range(cols):
                    line = block[col * rows + at : col * rows + at + 1]
                    picked = jnp.where(row == col, jnp.broadcast_to(line, (8, CH)), picked)
                ref[:, lanes] = picked[:cols]

    return body


def fine_span(rows, halo):
    return FINE_HALO - 4 - 2 * halo, 2 * rows + 8 + 4 * halo


def lat_coefficients(stencil_ref, rows, halo):
    first, count = fine_span(rows, halo)
    total = 2 * rows + 2 * FINE_HALO
    weight = stencil_ref[first : first + count, :]
    offset = stencil_ref[total + first : total + first + count, :]
    result = []
    for step in range(5):
        lower = jnp.where(offset == float(step), 1.0 - weight, 0.0)
        result.append(lower + jnp.where(offset == float(step - 1), weight, 0.0))
    return result


def restrict_block(even, odd, coefs, spill_ref, sum_ref, cols, rows, halo):
    count = fine_span(rows, halo)[1]
    out = rows + 2 * halo
    for col in range(cols):
        folded = None
        for tap in range(4):
            term = EVEN_TAPS[tap] * even[col + 3 - tap] + ODD_TAPS[tap] * odd[col + 3 - tap]
            folded = term if folded is None else folded + term
        total = None
        for step in range(5):
            slot = col * 5 + step
            spill_ref[slot, 0:count, :] = coefs[step] * folded
            term = spill_ref[slot, 8 - 2 * step : 8 - 2 * step + 2 * out, :]
            total = term if total is None else total + term
        sum_ref[col, 0 : 2 * out, :] = total
    blocks = [
        sum_ref[col, pl.ds(2 * halo, rows, stride=2), :]
        + sum_ref[col, pl.ds(2 * halo + 1, rows, stride=2), :]
        for col in range(cols)
    ]
    return jnp.concatenate(blocks, axis=0)


def middle(mid_ref, left_ref, right_ref, weight_ref, coefs, dup_ref, spill_ref, sum_ref, rows, halo, mask=None):
    cols = mid_ref.shape[0]
    first, count = fine_span(rows, halo)
    given = rows + 2 * halo + 2
    lat = []
    for col in range(cols + 6):
        if col < 3:
            block = left_ref[col]
        elif col < cols + 3:
            block = mid_ref[col - 3]
        else:
            block = right_ref[col - cols - 3]
        if mask is not None:
            block = block * mask
        dup_ref[col] = jnp.zeros(dup_ref.shape[1:], F32)
        dup_ref[col, pl.ds(PAD, given, stride=2), :] = block
        dup_ref[col, pl.ds(PAD + 1, given, stride=2), :] = block
        total = None
        for step in range(5):
            at = 2 + 2 * step
            term = coefs[step] * dup_ref[col, at : at + count, :]
            total = term if total is None else total + term
        lat.append(total)
    even, odd = [], []
    for at in range(cols + 3):
        left = sum(EVEN_TAPS[tap] * lat[at + tap] for tap in range(4))
        right = sum(ODD_TAPS[tap] * lat[at + tap] for tap in range(4))
        even.append(left * weight_ref[2 * at + 1, first : first + count, :])
        odd.append(right * weight_ref[2 * at, first : first + count, :])
    return restrict_block(even, odd, coefs, spill_ref, sum_ref, cols, rows, halo)


def start_kernel(cols, rows):
    first, count = fine_span(rows, 0)
    base = 2 * rows + 2 * FINE_HALO + first

    def body(weight_ref, stencil_ref, ens_ref, widths_ref, scales_ref, coarse_ref, image_ref, spill_ref, sum_ref):
        coefs = lat_coefficients(stencil_ref, rows, 0)
        even = [weight_ref[2 * at + 1, base : base + count, :] for at in range(cols + 3)]
        odd = [weight_ref[2 * at, base : base + count, :] for at in range(cols + 3)]
        coarse = restrict_block(even, odd, coefs, spill_ref, sum_ref, cols, rows, 0)
        coarse_ref[...] = coarse
        image_ref[...] = gram((ens_ref,), widths_ref, scales_ref, coarse)

    return body


def step_kernel(cols, rows):
    cells = cols * rows

    def body(mid_ref, left_ref, right_ref, weight_ref, stencil_ref, flags_ref, ens_ref, ens_low_ref, ens_high_ref,
             widths_ref, scales_ref, coarse_ref, image_ref, padded_ref, dup_ref, spill_ref, sum_ref, rim_ref):
        coefs = lat_coefficients(stencil_ref, rows, 1)
        row = lax.broadcasted_iota(jnp.int32, (rows + 4, CH), 0)
        inside = jnp.where(row < 2, flags_ref[0:1, :], jnp.where(row < rows + 2, 1.0, flags_ref[1:2, :]))
        coarse = middle(
            mid_ref, left_ref, right_ref, weight_ref, coefs, dup_ref, spill_ref, sum_ref, rows, 1, inside
        )
        coarse_ref[...] = coarse
        end = 2 * rows + 2
        for col in range(cols):
            low = sum_ref[col, 0:1, :] + sum_ref[col, 1:2, :]
            high = sum_ref[col, end : end + 1, :] + sum_ref[col, end + 1 : end + 2, :]
            rim_ref[col : col + 1, :] = low * flags_ref[0:1, :]
            rim_ref[cols + col : cols + col + 1, :] = high * flags_ref[1:2, :]
        image = gram(
            (ens_ref, ens_low_ref, ens_high_ref), widths_ref, scales_ref,
            jnp.concatenate([coarse, rim_ref[...]], axis=0),
        )
        image_ref[...] = image[:cells]
        for col in range(cols):
            padded_ref[col, 0:1, :] = image[cells + col : cells + col + 1]
            padded_ref[col, 1 : rows + 1, :] = image[col * rows : (col + 1) * rows]
            padded_ref[col, rows + 1 : rows + 2, :] = image[
                cells + cols + col : cells + cols + col + 1
            ]

    return body


def last_kernel(rows, devices):
    def body(mid_ref, left_ref, right_ref, weight_ref, stencil_ref, y0_ref, b0_ref, y1_ref, b1_ref,
             coarse_ref, dots_ref, dup_ref, spill_ref, sum_ref):
        coefs = lat_coefficients(stencil_ref, rows, 0)
        coarse = middle(
            mid_ref, left_ref, right_ref, weight_ref, coefs, dup_ref, spill_ref, sum_ref, rows, 0
        )
        coarse_ref[...] = coarse
        lane = lax.broadcasted_iota(jnp.int32, (1, CH), 1)
        row = jnp.zeros((1, CH), F32)
        b0, b1, y1 = b0_ref[...], b1_ref[...], y1_ref[...]
        pairs = (y0_ref[...] * b0, y1 * b0, y1 * b1, coarse * b1)
        for place, terms in enumerate(pairs):
            total = jnp.sum(jnp.sum(terms, axis=0, keepdims=True), axis=1, keepdims=True)
            row = jnp.where(lane == place, total, row)
        dots_ref[...] = jnp.broadcast_to(row, (devices, CH))

    return body


def spread_kernel(cells):
    def body(y0_ref, y1_ref, y2_ref, ens_ref, widths_ref, scales_ref, spread_ref):
        distances = pair_distances()
        low_half = lax.broadcasted_iota(jnp.int32, (cells, CH), 1) < LEV
        coarse = (y0_ref[...], y1_ref[...], y2_ref[...])
        for pair in range(PAIRS):
            matrix = hat(widths_ref, pair, distances)
            first, second = members((ens_ref,), pair)
            summed = [field_sum(first, second, part, low_half) for part in coarse]
            out = product(jnp.concatenate(summed, axis=0), matrix) * scales_ref[pair : pair + 1, :]
            spread_ref[:, pair * CH : (pair + 1) * CH] = out

    return body


def final_kernel(entries, cells):
    def body(dots_ref, spread_ref, coef_ref, vector_ref):
        sums = jnp.sum(dots_ref[...], axis=0, keepdims=True)
        lane = lax.broadcasted_iota(jnp.int32, (1, CH), 1)

        def pick(place):
            return jnp.sum(jnp.where(lane == place, sums, 0.0), axis=1, keepdims=True)

        m00, m01, m11, m12 = (pick(place) for place in range(4))
        beta0 = jnp.sqrt(m00 / entries + EPSILON)
        alpha0 = (m00 + m01) / (entries * beta0 * beta0)
        s1 = 1.0 / beta0
        s0 = (1.0 - alpha0) * s1
        u1u1 = s0 * s0 * m00 + 2.0 * s0 * s1 * m01 + s1 * s1 * m11
        beta1 = jnp.sqrt(u1u1 / entries + EPSILON)
        u0u1 = s0 * m00 + s1 * m01
        u0lu1 = s0 * m01 + s1 * m11
        u1lu1 = s0 * s0 * m01 + 2.0 * s0 * s1 * m11 + s1 * s1 * m12
        c0 = (u0u1 + u0lu1) / (entries * beta0 * beta1)
        alpha1 = (u1u1 + u1lu1) / (entries * beta1 * beta1)
        r1 = 1.0 / beta1
        keep = (1.0 - alpha1) * r1
        k0 = keep * s0 - c0 / beta0
        k1 = keep * s1 + s0 * r1
        k2 = s1 * r1
        row = lax.broadcasted_iota(jnp.int32, (2, 2), 0)
        col = lax.broadcasted_iota(jnp.int32, (2, 2), 1)
        coef_ref[...] = jnp.where(
            row == 0, jnp.where(col == 0, alpha0, alpha1), jnp.where(col == 0, beta0, beta1)
        )
        for pair in range(PAIRS):
            lanes = slice(pair * CH, (pair + 1) * CH)
            out = k0 * spread_ref[0:cells, lanes] + k1 * spread_ref[cells : 2 * cells, lanes]
            vector_ref[:, lanes] = (out + k2 * spread_ref[2 * cells :, lanes]).astype(BF16)

    return body


def from_neighbours(up, down, axis, paired):
    count = lax.axis_size(axis)
    if paired and count % 2 == 0:
        odd = lax.axis_index(axis) % 2 == 1
        outer = [(at, (at + 1) % count if at % 2 else (at - 1) % count) for at in range(count)]
        inner = [(at, at + 1 - 2 * (at % 2)) for at in range(count)]
        far = lax.ppermute(jnp.where(odd, up, down), axis, outer)
        near = lax.ppermute(jnp.where(odd, down, up), axis, inner)
        return jnp.where(odd, near, far), jnp.where(odd, far, near)
    low = lax.ppermute(up, axis, [(at, (at + 1) % count) for at in range(count)])
    high = lax.ppermute(down, axis, [((at + 1) % count, at) for at in range(count)])
    return low, high


def per_device(ensemble, innovation, obs_weight, lat_offset, lat_weight, band_widths):
    cols, rows = ensemble.shape[0], ensemble.shape[1]
    cells = cols * rows
    fine_cols, fine_rows = innovation.shape[0], innovation.shape[1]
    total = fine_rows + 2 * FINE_HALO
    lat_count, lon_count = lax.axis_size("lat"), lax.axis_size("lon")
    devices = lat_count * lon_count
    entries = float(cells * M * LEV * devices)
    position = lax.axis_index("lat")
    keeps = jnp.stack([position > 0, position < lat_count - 1]).astype(F32)
    flags = jnp.broadcast_to(keeps[:, None], (2, CH))

    edge_block = pltpu.VMEM(((fine_cols + 1) * 2 * FINE_HALO, CH), F32)
    pair_block = pltpu.VMEM((PAIRS, CH), F32)
    up, down, own, own_stencil, widths, scales = pl.pallas_call(
        prepare_kernel(),
        out_shape=(
            edge_block, edge_block, pltpu.VMEM((fine_cols, 2 * fine_rows, CH), F32),
            pltpu.VMEM((2 * fine_rows, CH), F32), pair_block, pair_block,
        ),
        in_specs=[VMEM_SPEC] * 5,
        out_specs=(VMEM_SPEC,) * 6,
    )(obs_weight, innovation, lat_weight[None], lat_offset[None], band_widths[None])
    low, high = from_neighbours(up, down, "lat", False)
    tall, stencil = kernel_call(
        join_kernel(),
        (pltpu.VMEM((fine_cols, 2 * total, CH), F32), pltpu.VMEM((2 * total, CH), F32)),
        (low, high, own, own_stencil, flags),
    )
    left, right = from_neighbours(tall[-3:], tall[:3], "lon", True)
    weight = jnp.concatenate([left, tall, right], axis=0)

    ens = ensemble.reshape(cells, M * CH)
    edge_rows = pltpu.VMEM((cols, M * CH), F32)
    ens_up, ens_down = kernel_call(
        edges_kernel(cols, rows), (edge_rows, edge_rows), (ens, own_stencil)
    )
    ens_low, ens_high = from_neighbours(ens_up, ens_down, "lat", False)

    cell_block = pltpu.VMEM((cells, CH), F32)
    restrict_scratch = (
        pltpu.VMEM((cols * 5, total, CH), F32),
        pltpu.VMEM((cols, 2 * rows + 8, CH), F32),
    )
    middle_scratch = (pltpu.VMEM((cols + 6, total + 16, CH), F32),) + restrict_scratch

    y0, b0 = kernel_call(
        start_kernel(cols, rows), (cell_block, cell_block),
        (weight, stencil, ens, widths, scales), restrict_scratch,
    )
    block = b0.reshape(cols, rows, CH)
    low_rows, high_rows = from_neighbours(block[:, -2:], block[:, :2], "lat", False)
    mid = jnp.concatenate([low_rows, block, high_rows], axis=1)
    y1, b1, mid1 = kernel_call(
        step_kernel(cols, rows), (cell_block, cell_block, pltpu.VMEM((cols, rows + 2, CH), F32)),
        (mid, *from_neighbours(mid[-3:], mid[:3], "lon", True), weight, stencil, flags,
         ens, ens_low, ens_high, widths, scales),
        middle_scratch + (pltpu.VMEM((2 * cols, CH), F32),),
    )
    y2, dots = kernel_call(
        last_kernel(rows, devices), (cell_block, pltpu.VMEM((devices, CH), F32)),
        (mid1, *from_neighbours(mid1[-3:], mid1[:3], "lon", True), weight, stencil, y0, b0, y1, b1),
        middle_scratch,
    )
    shared = lax.all_to_all(dots.reshape(devices, 1, CH), ("lat", "lon"), 0, 0).reshape(devices, CH)
    spreads = kernel_call(
        spread_kernel(cells), pltpu.VMEM((3 * cells, M * LEV), F32),
        (y0, y1, y2, ens, widths, scales),
    )
    coefficients, vector = kernel_call(
        final_kernel(entries, cells),
        (jax.ShapeDtypeStruct((2, 2), F32), jax.ShapeDtypeStruct((cells, M * LEV), BF16)),
        (shared, spreads),
    )
    return coefficients, vector.reshape(cols, rows, M * LEV)


def solution(mesh):
    return jax.shard_map(
        per_device,
        mesh=mesh,
        in_specs=(
            P("lon", "lat", None),
            P("lon", "lat", None),
            P("lon", "lat", None),
            P("lat"),
            P("lat"),
            P(),
        ),
        out_specs=(P(), P("lon", "lat", None)),
        check_vma=False,
    )
```

```python
import jax
import jax.numpy as jnp
from jax import lax
from jax.experimental import pallas as pl
from jax.experimental.pallas import tpu as pltpu
from jax.sharding import PartitionSpec as P

M = 80
LEV = 64
FIELDS = 2

EVEN_TAPS = (-0.0234375, 0.2265625, 0.8671875, -0.0703125)
ODD_TAPS = (-0.0703125, 0.8671875, 0.2265625, -0.0234375)
EPSILON = 1e-06


F32 = jnp.float32
BF16 = jnp.bfloat16
CH = FIELDS * LEV
PAIRS = M // 2
PAD = 8
FINE_HALO = 6
VMEM_SPEC = pl.BlockSpec(memory_space=pltpu.VMEM)


def in_vmem(value):
    return pltpu.with_memory_space_constraint(value, pltpu.VMEM)


def kernel_call(body, outs, operands, scratch=()):
    return pl.pallas_call(
        body,
        out_shape=outs,
        in_specs=[VMEM_SPEC] * len(operands),
        out_specs=jax.tree.map(lambda _: VMEM_SPEC, outs),
        scratch_shapes=list(scratch),
    )(*[in_vmem(operand) for operand in operands])


def split(value):
    high = value.astype(BF16)
    return high, (value - high.astype(F32)).astype(BF16)


def pair_distances():
    row = lax.broadcasted_iota(jnp.int32, (CH, CH), 0)
    col = lax.broadcasted_iota(jnp.int32, (CH, CH), 1)
    distance = jnp.where(row // LEV == col // LEV, jnp.abs(row - col), CH)
    return distance.astype(F32).astype(BF16).reshape(CH // 16, 16, CH)


def hat(widths_ref, pair, distances):
    widths = jnp.broadcast_to(widths_ref[pair : pair + 1, :], (16, CH)).astype(BF16)
    return jnp.maximum(widths[None] - distances, jnp.zeros((), BF16)).reshape(CH, CH)


def product(value, matrix):
    cells = value.shape[0]
    parts = jnp.concatenate(split(value), axis=0)
    both = jnp.dot(parts, matrix, preferred_element_type=F32)
    return both[:cells] + both[cells:]


def swap_halves(value):
    return pltpu.roll(value, LEV, 1)


def members(ens_refs, pair):
    result = []
    for member in (2 * pair, 2 * pair + 1):
        parts = [ref[:, member * CH : (member + 1) * CH].astype(F32) for ref in ens_refs]
        result.append(parts[0] if len(parts) == 1 else jnp.concatenate(parts, axis=0))
    return result


def field_sum(first, second, coarse, low_half):
    left, right = first * coarse, second * coarse
    return jnp.where(low_half, left, right) + swap_halves(jnp.where(low_half, right, left))


def gram(ens_refs, widths_ref, scales_ref, coarse):
    distances = pair_distances()
    low_half = lax.broadcasted_iota(jnp.int32, coarse.shape, 1) < LEV
    total = jnp.zeros(coarse.shape, F32)
    for pair in range(PAIRS):
        matrix = hat(widths_ref, pair, distances)
        first, second = members(ens_refs, pair)
        summed = field_sum(first, second, coarse, low_half)
        scale = scales_ref[pair : pair + 1, :]
        twice = product(product(summed, matrix), matrix) * (scale * scale)
        swapped = swap_halves(twice)
        total = total + (
            first * jnp.where(low_half, twice, swapped)
            + second * jnp.where(low_half, swapped, twice)
        )
    return total


def prepare_kernel(cols, rows):
    depth = FINE_HALO
    fine_cols, fine_rows = 2 * cols, 2 * rows
    spans = rows + 4

    def body(weight_ref, innovation_ref, lat_weight_ref, lat_offset_ref, band_ref,
             up_ref, down_ref, part_ref, wide_up_ref, wide_down_ref, own_ref, own_stencil_ref,
             widths_ref, scales_ref, spill_ref, sum_ref):
        row = lax.broadcasted_iota(jnp.int32, (fine_rows, fine_rows), 0)
        col = lax.broadcasted_iota(jnp.int32, (fine_rows, fine_rows), 1)

        def column(line):
            spread = jnp.broadcast_to(line, (fine_rows, fine_rows))
            values = jnp.sum(jnp.where(row == col, spread, 0.0), axis=1, keepdims=True)
            return jnp.broadcast_to(values, (fine_rows, CH))

        upper = column(lat_weight_ref[...])
        offset = column(lat_offset_ref[...].astype(F32))
        weighted = []
        for at in range(fine_cols):
            weight = weight_ref[at]
            own_ref[at] = weight
            wide_up_ref[depth * at : depth * (at + 1), :] = weight[fine_rows - depth :]
            wide_down_ref[depth * at : depth * (at + 1), :] = weight[:depth]
            weighted.append(weight * innovation_ref[at])
        coefs = stencil_coefficients(upper, offset)
        blank = jnp.zeros((8, CH), F32)
        for at in range(cols + 4):
            folded = None
            for tap in range(4):
                for taps, centre in ((EVEN_TAPS, at - tap), (ODD_TAPS, at - 1 - tap)):
                    if 0 <= centre < cols:
                        term = taps[tap] * weighted[2 * centre + (taps is ODD_TAPS)]
                        folded = term if folded is None else folded + term
            total = None
            for step in range(5):
                slot = at * 5 + step
                spill_ref[slot, 0:8, :] = blank
                spill_ref[slot, 8 + fine_rows : 16 + fine_rows, :] = blank
                spill_ref[slot, 8 : 8 + fine_rows, :] = coefs[step] * folded
                term = spill_ref[slot, 8 - 2 * step : 8 - 2 * step + 2 * spans, :]
                total = term if total is None else total + term
            sum_ref[at] = total
            down_ref[2 * at : 2 * at + 2, :] = (
                sum_ref[at, pl.ds(0, 2, stride=2), :] + sum_ref[at, pl.ds(1, 2, stride=2), :]
            )
            part_ref[at] = (
                sum_ref[at, pl.ds(4, rows, stride=2), :] + sum_ref[at, pl.ds(5, rows, stride=2), :]
            )
            end = 2 * rows + 4
            up_ref[2 * at : 2 * at + 2, :] = (
                sum_ref[at, pl.ds(end, 2, stride=2), :] + sum_ref[at, pl.ds(end + 1, 2, stride=2), :]
            )
        own_stencil_ref[0:fine_rows, :] = upper
        own_stencil_ref[fine_rows : 2 * fine_rows, :] = offset
        at = depth * fine_cols
        wide_up_ref[at : at + depth, :] = upper[fine_rows - depth :]
        wide_up_ref[at + depth : at + 2 * depth, :] = offset[fine_rows - depth :]
        wide_down_ref[at : at + depth, :] = upper[:depth]
        wide_down_ref[at + depth : at + 2 * depth, :] = offset[:depth]
        bands = jnp.broadcast_to((band_ref[...] + 1).astype(F32), (PAIRS, M))
        pair = lax.broadcasted_iota(jnp.int32, (PAIRS, M), 0)
        member = lax.broadcasted_iota(jnp.int32, (PAIRS, M), 1)
        first = jnp.sum(jnp.where(member == 2 * pair, bands, 0.0), axis=1, keepdims=True)
        second = jnp.sum(jnp.where(member == 2 * pair + 1, bands, 0.0), axis=1, keepdims=True)
        lane = lax.broadcasted_iota(jnp.int32, (PAIRS, CH), 1)
        widths = jnp.where(lane < LEV, first, second)
        widths_ref[...] = widths
        scales_ref[...] = 1.0 / (widths * widths)

    return body


def gather_kernel(cols, rows):
    def body(low_ref, high_ref, part_ref, flags_ref, left_ref, own_ref, right_ref):
        keep_low, keep_high = flags_ref[0:1, :], flags_ref[1:2, :]
        middle_rows = jnp.zeros((rows - 4, CH), F32)
        for at in range(cols + 4):
            low = low_ref[2 * at : 2 * at + 2, :] * keep_low
            high = high_ref[2 * at : 2 * at + 2, :] * keep_high
            block = part_ref[at] + jnp.concatenate([low, middle_rows, high], axis=0)
            if at < 2:
                left_ref[at * rows : (at + 1) * rows, :] = block
            elif at < cols + 2:
                own_ref[(at - 2) * rows : (at - 1) * rows, :] = block
            else:
                right_ref[(at - cols - 2) * rows : (at - cols - 1) * rows, :] = block

    return body


def join_kernel(cols, rows):
    depth = FINE_HALO
    fine_cols, fine_rows = 2 * cols, 2 * rows

    def body(low_ref, high_ref, own_ref, own_stencil_ref, flags_ref, tall_ref, stencil_ref):
        total = fine_rows + 2 * depth
        keep_low, keep_high = flags_ref[0:1, :], flags_ref[1:2, :]
        for col in range(fine_cols):
            edge = slice(depth * col, depth * (col + 1))
            tall_ref[col, 0:depth, :] = low_ref[edge, :] * keep_low
            tall_ref[col, depth : depth + fine_rows, :] = own_ref[col]
            tall_ref[col, depth + fine_rows : total, :] = high_ref[edge, :] * keep_high
        for part in range(2):
            base = part * total
            at = depth * (fine_cols + part)
            stencil_ref[base : base + depth, :] = low_ref[at : at + depth, :]
            stencil_ref[base + depth : base + depth + fine_rows, :] = own_stencil_ref[
                part * fine_rows : (part + 1) * fine_rows, :
            ]
            stencil_ref[base + depth + fine_rows : base + total, :] = high_ref[at : at + depth, :]

    return body


def edges_kernel(cols, rows):
    def body(ens_ref, after_ref, up_ref, down_ref):
        row = lax.broadcasted_iota(jnp.int32, (8, CH), 0)
        for member in range(M):
            lanes = slice(member * CH, (member + 1) * CH)
            block = ens_ref[:, lanes].astype(F32)
            for ref, at in ((up_ref, rows - 1), (down_ref, 0)):
                picked = jnp.zeros((8, CH), F32)
                for col in range(cols):
                    line = block[col * rows + at : col * rows + at + 1]
                    picked = jnp.where(row == col, jnp.broadcast_to(line, (8, CH)), picked)
                ref[:, lanes] = picked[:cols]

    return body


def fine_span(rows, halo):
    return FINE_HALO - 4 - 2 * halo, 2 * rows + 8 + 4 * halo


def lat_coefficients(stencil_ref, rows, halo):
    first, count = fine_span(rows, halo)
    total = 2 * rows + 2 * FINE_HALO
    return stencil_coefficients(
        stencil_ref[first : first + count, :], stencil_ref[total + first : total + first + count, :]
    )


def stencil_coefficients(weight, offset):
    result = []
    for step in range(5):
        lower = jnp.where(offset == float(step), 1.0 - weight, 0.0)
        result.append(lower + jnp.where(offset == float(step - 1), weight, 0.0))
    return result


def restrict_block(even, odd, coefs, spill_ref, sum_ref, cols, rows, halo):
    count = fine_span(rows, halo)[1]
    out = rows + 2 * halo
    for col in range(cols):
        folded = None
        for tap in range(4):
            term = EVEN_TAPS[tap] * even[col + 3 - tap] + ODD_TAPS[tap] * odd[col + 3 - tap]
            folded = term if folded is None else folded + term
        total = None
        for step in range(5):
            slot = col * 5 + step
            spill_ref[slot, 0:count, :] = coefs[step] * folded
            term = spill_ref[slot, 8 - 2 * step : 8 - 2 * step + 2 * out, :]
            total = term if total is None else total + term
        sum_ref[col, 0 : 2 * out, :] = total
    blocks = [
        sum_ref[col, pl.ds(2 * halo, rows, stride=2), :]
        + sum_ref[col, pl.ds(2 * halo + 1, rows, stride=2), :]
        for col in range(cols)
    ]
    return jnp.concatenate(blocks, axis=0)


def middle(mid_ref, left_ref, right_ref, weight_ref, coefs, dup_ref, spill_ref, sum_ref, rows, halo, mask=None):
    cols = mid_ref.shape[0]
    first, count = fine_span(rows, halo)
    given = rows + 2 * halo + 2
    lat = []
    for col in range(cols + 6):
        if col < 3:
            block = left_ref[col]
        elif col < cols + 3:
            block = mid_ref[col - 3]
        else:
            block = right_ref[col - cols - 3]
        if mask is not None:
            block = block * mask
        dup_ref[col] = jnp.zeros(dup_ref.shape[1:], F32)
        dup_ref[col, pl.ds(PAD, given, stride=2), :] = block
        dup_ref[col, pl.ds(PAD + 1, given, stride=2), :] = block
        total = None
        for step in range(5):
            at = 2 + 2 * step
            term = coefs[step] * dup_ref[col, at : at + count, :]
            total = term if total is None else total + term
        lat.append(total)
    even, odd = [], []
    for at in range(cols + 3):
        left = sum(EVEN_TAPS[tap] * lat[at + tap] for tap in range(4))
        right = sum(ODD_TAPS[tap] * lat[at + tap] for tap in range(4))
        even.append(left * weight_ref[2 * at + 1, first : first + count, :])
        odd.append(right * weight_ref[2 * at, first : first + count, :])
    return restrict_block(even, odd, coefs, spill_ref, sum_ref, cols, rows, halo)


def start_kernel(cols, rows):
    def body(own_ref, left_ref, right_ref, ens_ref, widths_ref, scales_ref, coarse_ref, image_ref):
        coarse_ref[...] = own_ref[...]
        coarse_ref[0 : 2 * rows, :] += left_ref[...]
        coarse_ref[(cols - 2) * rows : cols * rows, :] += right_ref[...]
        image_ref[...] = gram((ens_ref,), widths_ref, scales_ref, coarse_ref[...])

    return body


def step_kernel(cols, rows):
    cells = cols * rows

    def body(mid_ref, left_ref, right_ref, weight_ref, stencil_ref, flags_ref, ens_ref, ens_low_ref, ens_high_ref,
             widths_ref, scales_ref, coarse_ref, image_ref, padded_ref, dup_ref, spill_ref, sum_ref, rim_ref):
        coefs = lat_coefficients(stencil_ref, rows, 1)
        row = lax.broadcasted_iota(jnp.int32, (rows + 4, CH), 0)
        inside = jnp.where(row < 2, flags_ref[0:1, :], jnp.where(row < rows + 2, 1.0, flags_ref[1:2, :]))
        coarse = middle(
            mid_ref, left_ref, right_ref, weight_ref, coefs, dup_ref, spill_ref, sum_ref, rows, 1, inside
        )
        coarse_ref[...] = coarse
        end = 2 * rows + 2
        for col in range(cols):
            low = sum_ref[col, 0:1, :] + sum_ref[col, 1:2, :]
            high = sum_ref[col, end : end + 1, :] + sum_ref[col, end + 1 : end + 2, :]
            rim_ref[col : col + 1, :] = low * flags_ref[0:1, :]
            rim_ref[cols + col : cols + col + 1, :] = high * flags_ref[1:2, :]
        image = gram(
            (ens_ref, ens_low_ref, ens_high_ref), widths_ref, scales_ref,
            jnp.concatenate([coarse, rim_ref[...]], axis=0),
        )
        image_ref[...] = image[:cells]
        for col in range(cols):
            padded_ref[col, 0:1, :] = image[cells + col : cells + col + 1]
            padded_ref[col, 1 : rows + 1, :] = image[col * rows : (col + 1) * rows]
            padded_ref[col, rows + 1 : rows + 2, :] = image[
                cells + cols + col : cells + cols + col + 1
            ]

    return body


def last_kernel(rows, devices):
    def body(mid_ref, left_ref, right_ref, weight_ref, stencil_ref, y0_ref, b0_ref, y1_ref, b1_ref,
             coarse_ref, dots_ref, dup_ref, spill_ref, sum_ref):
        coefs = lat_coefficients(stencil_ref, rows, 0)
        coarse = middle(
            mid_ref, left_ref, right_ref, weight_ref, coefs, dup_ref, spill_ref, sum_ref, rows, 0
        )
        coarse_ref[...] = coarse
        lane = lax.broadcasted_iota(jnp.int32, (1, CH), 1)
        row = jnp.zeros((1, CH), F32)
        b0, b1, y1 = b0_ref[...], b1_ref[...], y1_ref[...]
        pairs = (y0_ref[...] * b0, y1 * b0, y1 * b1, coarse * b1)
        for place, terms in enumerate(pairs):
            total = jnp.sum(jnp.sum(terms, axis=0, keepdims=True), axis=1, keepdims=True)
            row = jnp.where(lane == place, total, row)
        dots_ref[...] = jnp.broadcast_to(row, (devices, CH))

    return body


def final_kernel(entries):
    def body(dots_ref, y0_ref, y1_ref, y2_ref, ens_ref, widths_ref, scales_ref, coef_ref, vector_ref):
        sums = jnp.sum(dots_ref[...], axis=0, keepdims=True)
        lane = lax.broadcasted_iota(jnp.int32, (1, CH), 1)

        def pick(place):
            return jnp.sum(jnp.where(lane == place, sums, 0.0), axis=1, keepdims=True)

        m00, m01, m11, m12 = (pick(place) for place in range(4))
        beta0 = jnp.sqrt(m00 / entries + EPSILON)
        alpha0 = (m00 + m01) / (entries * beta0 * beta0)
        s1 = 1.0 / beta0
        s0 = (1.0 - alpha0) * s1
        u1u1 = s0 * s0 * m00 + 2.0 * s0 * s1 * m01 + s1 * s1 * m11
        beta1 = jnp.sqrt(u1u1 / entries + EPSILON)
        u0u1 = s0 * m00 + s1 * m01
        u0lu1 = s0 * m01 + s1 * m11
        u1lu1 = s0 * s0 * m01 + 2.0 * s0 * s1 * m11 + s1 * s1 * m12
        c0 = (u0u1 + u0lu1) / (entries * beta0 * beta1)
        alpha1 = (u1u1 + u1lu1) / (entries * beta1 * beta1)
        r1 = 1.0 / beta1
        keep = (1.0 - alpha1) * r1
        k0 = keep * s0 - c0 / beta0
        k1 = keep * s1 + s0 * r1
        k2 = s1 * r1
        row = lax.broadcasted_iota(jnp.int32, (2, 2), 0)
        col = lax.broadcasted_iota(jnp.int32, (2, 2), 1)
        coef_ref[...] = jnp.where(
            row == 0, jnp.where(col == 0, alpha0, alpha1), jnp.where(col == 0, beta0, beta1)
        )
        coarse = k0 * y0_ref[...] + k1 * y1_ref[...] + k2 * y2_ref[...]
        distances = pair_distances()
        low_half = lax.broadcasted_iota(jnp.int32, coarse.shape, 1) < LEV
        for pair in range(PAIRS):
            matrix = hat(widths_ref, pair, distances)
            first, second = members((ens_ref,), pair)
            summed = field_sum(first, second, coarse, low_half)
            out = product(summed, matrix) * scales_ref[pair : pair + 1, :]
            vector_ref[:, pair * CH : (pair + 1) * CH] = out.astype(BF16)

    return body


def from_neighbours(up, down, axis, paired):
    count = lax.axis_size(axis)
    if paired and count % 2 == 0:
        odd = lax.axis_index(axis) % 2 == 1
        outer = [(at, (at + 1) % count if at % 2 else (at - 1) % count) for at in range(count)]
        inner = [(at, at + 1 - 2 * (at % 2)) for at in range(count)]
        far = lax.ppermute(jnp.where(odd, up, down), axis, outer)
        near = lax.ppermute(jnp.where(odd, down, up), axis, inner)
        return jnp.where(odd, near, far), jnp.where(odd, far, near)
    low = lax.ppermute(up, axis, [(at, (at + 1) % count) for at in range(count)])
    high = lax.ppermute(down, axis, [((at + 1) % count, at) for at in range(count)])
    return low, high


def per_device(ensemble, innovation, obs_weight, lat_offset, lat_weight, band_widths):
    cols, rows = ensemble.shape[0], ensemble.shape[1]
    cells = cols * rows
    fine_cols, fine_rows = innovation.shape[0], innovation.shape[1]
    total = fine_rows + 2 * FINE_HALO
    lat_count, lon_count = lax.axis_size("lat"), lax.axis_size("lon")
    devices = lat_count * lon_count
    entries = float(cells * M * LEV * devices)
    position = lax.axis_index("lat")
    keeps = jnp.stack([position > 0, position < lat_count - 1]).astype(F32)
    flags = jnp.broadcast_to(keeps[:, None], (2, CH))

    cell_block = pltpu.VMEM((cells, CH), F32)
    pair_block = pltpu.VMEM((PAIRS, CH), F32)
    rim_block = pltpu.VMEM((2 * (cols + 4), CH), F32)
    wide_block = pltpu.VMEM(((fine_cols + 2) * FINE_HALO, CH), F32)
    up, down, part, wide_up, wide_down, own, own_stencil, widths, scales = pl.pallas_call(
        prepare_kernel(cols, rows),
        out_shape=(
            rim_block, rim_block, pltpu.VMEM((cols + 4, rows, CH), F32), wide_block, wide_block,
            pltpu.VMEM((fine_cols, fine_rows, CH), F32),
            pltpu.VMEM((2 * fine_rows, CH), F32), pair_block, pair_block,
        ),
        in_specs=[VMEM_SPEC] * 5,
        out_specs=(VMEM_SPEC,) * 9,
        scratch_shapes=[
            pltpu.VMEM(((cols + 4) * 5, fine_rows + 16, CH), F32),
            pltpu.VMEM((cols + 4, fine_rows + 8, CH), F32),
        ],
    )(obs_weight, innovation, lat_weight[None], lat_offset[None], band_widths[None])
    low, high = from_neighbours(up, down, "lat", False)
    wide_low, wide_high = from_neighbours(wide_up, wide_down, "lat", False)
    side_block = pltpu.VMEM((2 * rows, CH), F32)
    to_left, own_part, to_right = kernel_call(
        gather_kernel(cols, rows), (side_block, cell_block, side_block), (low, high, part, flags)
    )
    left, right = from_neighbours(to_right, to_left, "lon", True)
    edge_rows = pltpu.VMEM((cols, M * CH), F32)
    ens = ensemble.reshape(cells, M * CH)
    ens_up, ens_down = kernel_call(
        edges_kernel(cols, rows), (edge_rows, edge_rows), (ens, to_left)
    )
    ens_low, ens_high = from_neighbours(ens_up, ens_down, "lat", False)
    tall, stencil = kernel_call(
        join_kernel(cols, rows),
        (pltpu.VMEM((fine_cols, total, CH), F32), pltpu.VMEM((2 * total, CH), F32)),
        (wide_low, wide_high, own, own_stencil, flags),
    )
    wide_left, wide_right = from_neighbours(tall[-3:], tall[:3], "lon", True)
    weight = jnp.concatenate([wide_left, tall, wide_right], axis=0)

    restrict_scratch = (
        pltpu.VMEM((cols * 5, total, CH), F32),
        pltpu.VMEM((cols, 2 * rows + 8, CH), F32),
    )
    middle_scratch = (pltpu.VMEM((cols + 6, total + 16, CH), F32),) + restrict_scratch

    y0, b0 = kernel_call(
        start_kernel(cols, rows), (cell_block, cell_block),
        (own_part, left, right, ens, widths, scales),
    )
    block = b0.reshape(cols, rows, CH)
    low_rows, high_rows = from_neighbours(block[:, -2:], block[:, :2], "lat", False)
    mid = jnp.concatenate([low_rows, block, high_rows], axis=1)
    mid_left, mid_right = from_neighbours(mid[-3:], mid[:3], "lon", True)
    y1, b1, mid1 = kernel_call(
        step_kernel(cols, rows), (cell_block, cell_block, pltpu.VMEM((cols, rows + 2, CH), F32)),
        (mid, mid_left, mid_right, weight, stencil, flags,
         ens, ens_low, ens_high, widths, scales),
        middle_scratch + (pltpu.VMEM((2 * cols, CH), F32),),
    )
    y2, dots = kernel_call(
        last_kernel(rows, devices), (cell_block, pltpu.VMEM((devices, CH), F32)),
        (mid1, *from_neighbours(mid1[-3:], mid1[:3], "lon", True), weight, stencil, y0, b0, y1, b1),
        middle_scratch,
    )
    shared = lax.all_to_all(dots.reshape(devices, 1, CH), ("lat", "lon"), 0, 0).reshape(devices, CH)
    coefficients, vector = kernel_call(
        final_kernel(entries),
        (jax.ShapeDtypeStruct((2, 2), F32), jax.ShapeDtypeStruct((cells, M * LEV), BF16)),
        (shared, y0, y1, y2, ens, widths, scales),
    )
    return coefficients, vector.reshape(cols, rows, M * LEV)


def solution(mesh):
    return jax.shard_map(
        per_device,
        mesh=mesh,
        in_specs=(
            P("lon", "lat", None),
            P("lon", "lat", None),
            P("lon", "lat", None),
            P("lat"),
            P("lat"),
            P(),
        ),
        out_specs=(P(), P("lon", "lat", None)),
        check_vma=False,
    )
```

```python
import jax
import jax.numpy as jnp
from jax import lax
from jax.experimental import pallas as pl
from jax.experimental.pallas import tpu as pltpu
from jax.sharding import PartitionSpec as P

M = 80
LEV = 64
FIELDS = 2

EVEN_TAPS = (-0.0234375, 0.2265625, 0.8671875, -0.0703125)
ODD_TAPS = (-0.0703125, 0.8671875, 0.2265625, -0.0234375)
EPSILON = 1e-06


F32 = jnp.float32
BF16 = jnp.bfloat16
CH = FIELDS * LEV
PAIRS = M // 2
PAD = 8
FINE_HALO = 6
VMEM_SPEC = pl.BlockSpec(memory_space=pltpu.VMEM)


def in_vmem(value):
    return pltpu.with_memory_space_constraint(value, pltpu.VMEM)


def kernel_call(body, outs, operands, scratch=()):
    return pl.pallas_call(
        body,
        out_shape=outs,
        in_specs=[VMEM_SPEC] * len(operands),
        out_specs=jax.tree.map(lambda _: VMEM_SPEC, outs),
        scratch_shapes=list(scratch),
    )(*[in_vmem(operand) for operand in operands])


def split(value):
    high = value.astype(BF16)
    return high, (value - high.astype(F32)).astype(BF16)


def pair_distances():
    row = lax.broadcasted_iota(jnp.int32, (CH, CH), 0)
    col = lax.broadcasted_iota(jnp.int32, (CH, CH), 1)
    distance = jnp.where(row // LEV == col // LEV, jnp.abs(row - col), CH)
    return distance.astype(F32).astype(BF16).reshape(CH // 16, 16, CH)


def hat(widths_ref, pair, distances):
    widths = jnp.broadcast_to(widths_ref[pair : pair + 1, :], (16, CH)).astype(BF16)
    return jnp.maximum(widths[None] - distances, jnp.zeros((), BF16)).reshape(CH, CH)


def product(value, matrix):
    cells = value.shape[0]
    parts = jnp.concatenate(split(value), axis=0)
    both = jnp.dot(parts, matrix, preferred_element_type=F32)
    return both[:cells] + both[cells:]


def swap_halves(value):
    return pltpu.roll(value, LEV, 1)


def members(ens_refs, pair):
    result = []
    for member in (2 * pair, 2 * pair + 1):
        parts = [ref[:, member * CH : (member + 1) * CH].astype(F32) for ref in ens_refs]
        result.append(parts[0] if len(parts) == 1 else jnp.concatenate(parts, axis=0))
    return result


def field_sum(first, second, coarse, low_half):
    left, right = first * coarse, second * coarse
    return jnp.where(low_half, left, right) + swap_halves(jnp.where(low_half, right, left))


def gram(ens_refs, widths_ref, scales_ref, coarse):
    distances = pair_distances()
    low_half = lax.broadcasted_iota(jnp.int32, coarse.shape, 1) < LEV
    total = jnp.zeros(coarse.shape, F32)
    for pair in range(PAIRS):
        matrix = hat(widths_ref, pair, distances)
        first, second = members(ens_refs, pair)
        summed = field_sum(first, second, coarse, low_half)
        scale = scales_ref[pair : pair + 1, :]
        twice = product(product(summed, matrix), matrix) * (scale * scale)
        swapped = swap_halves(twice)
        total = total + (
            first * jnp.where(low_half, twice, swapped)
            + second * jnp.where(low_half, swapped, twice)
        )
    return total


def prepare_kernel(cols, rows):
    depth = FINE_HALO
    fine_cols, fine_rows = 2 * cols, 2 * rows
    spans = rows + 4
    wide = 2 * (cols + 4)

    def body(weight_ref, innovation_ref, lat_weight_ref, lat_offset_ref, band_ref, ens_ref,
             up_ref, down_ref, part_ref, own_ref, own_stencil_ref, widths_ref, scales_ref, local_ref,
             spill_ref, sum_ref, done_ref):
        copy = pltpu.make_async_copy(ens_ref, local_ref, done_ref)
        copy.start()
        row = lax.broadcasted_iota(jnp.int32, (fine_rows, fine_rows), 0)
        col = lax.broadcasted_iota(jnp.int32, (fine_rows, fine_rows), 1)

        def column(line):
            spread = jnp.broadcast_to(line, (fine_rows, fine_rows))
            values = jnp.sum(jnp.where(row == col, spread, 0.0), axis=1, keepdims=True)
            return jnp.broadcast_to(values, (fine_rows, CH))

        upper = column(lat_weight_ref[...])
        offset = column(lat_offset_ref[...].astype(F32))
        weighted = []
        for at in range(fine_cols):
            weight = weight_ref[at]
            own_ref[at] = weight
            up_ref[wide + depth * at : wide + depth * (at + 1), :] = weight[fine_rows - depth :]
            down_ref[wide + depth * at : wide + depth * (at + 1), :] = weight[:depth]
            weighted.append(weight * innovation_ref[at])
        coefs = stencil_coefficients(upper, offset)
        blank = jnp.zeros((8, CH), F32)
        for at in range(cols + 4):
            folded = None
            for tap in range(4):
                for taps, centre in ((EVEN_TAPS, at - tap), (ODD_TAPS, at - 1 - tap)):
                    if 0 <= centre < cols:
                        term = taps[tap] * weighted[2 * centre + (taps is ODD_TAPS)]
                        folded = term if folded is None else folded + term
            total = None
            for step in range(5):
                slot = at * 5 + step
                spill_ref[slot, 0:8, :] = blank
                spill_ref[slot, 8 + fine_rows : 16 + fine_rows, :] = blank
                spill_ref[slot, 8 : 8 + fine_rows, :] = coefs[step] * folded
                term = spill_ref[slot, 8 - 2 * step : 8 - 2 * step + 2 * spans, :]
                total = term if total is None else total + term
            sum_ref[at] = total
            down_ref[2 * at : 2 * at + 2, :] = (
                sum_ref[at, pl.ds(0, 2, stride=2), :] + sum_ref[at, pl.ds(1, 2, stride=2), :]
            )
            part_ref[at] = (
                sum_ref[at, pl.ds(4, rows, stride=2), :] + sum_ref[at, pl.ds(5, rows, stride=2), :]
            )
            end = 2 * rows + 4
            up_ref[2 * at : 2 * at + 2, :] = (
                sum_ref[at, pl.ds(end, 2, stride=2), :] + sum_ref[at, pl.ds(end + 1, 2, stride=2), :]
            )
        own_stencil_ref[0:fine_rows, :] = upper
        own_stencil_ref[fine_rows : 2 * fine_rows, :] = offset
        at = wide + depth * fine_cols
        up_ref[at : at + depth, :] = upper[fine_rows - depth :]
        up_ref[at + depth : at + 2 * depth, :] = offset[fine_rows - depth :]
        down_ref[at : at + depth, :] = upper[:depth]
        down_ref[at + depth : at + 2 * depth, :] = offset[:depth]
        bands = jnp.broadcast_to((band_ref[...] + 1).astype(F32), (PAIRS, M))
        pair = lax.broadcasted_iota(jnp.int32, (PAIRS, M), 0)
        member = lax.broadcasted_iota(jnp.int32, (PAIRS, M), 1)
        first = jnp.sum(jnp.where(member == 2 * pair, bands, 0.0), axis=1, keepdims=True)
        second = jnp.sum(jnp.where(member == 2 * pair + 1, bands, 0.0), axis=1, keepdims=True)
        lane = lax.broadcasted_iota(jnp.int32, (PAIRS, CH), 1)
        widths = jnp.where(lane < LEV, first, second)
        widths_ref[...] = widths
        scales_ref[...] = 1.0 / (widths * widths)
        copy.wait()

    return body


def join_kernel(cols, rows):
    depth = FINE_HALO
    fine_cols, fine_rows = 2 * cols, 2 * rows
    wide = 2 * (cols + 4)
    total = fine_rows + 2 * depth

    def body(low_ref, high_ref, part_ref, own_ref, own_stencil_ref, flags_ref,
             left_ref, right_ref, coarse_ref, tall_ref, stencil_ref):
        keep_low, keep_high = flags_ref[0:1, :], flags_ref[1:2, :]
        middle_rows = jnp.zeros((rows - 4, CH), F32)
        for at in range(cols + 4):
            low = low_ref[2 * at : 2 * at + 2, :] * keep_low
            high = high_ref[2 * at : 2 * at + 2, :] * keep_high
            block = part_ref[at] + jnp.concatenate([low, middle_rows, high], axis=0)
            if at < 2:
                left_ref[at * rows : (at + 1) * rows, :] = block
            elif at < cols + 2:
                coarse_ref[(at - 2) * rows : (at - 1) * rows, :] = block
            else:
                right_ref[(at - cols - 2) * rows : (at - cols - 1) * rows, :] = block
        for col in range(fine_cols):
            edge = slice(wide + depth * col, wide + depth * (col + 1))
            pieces = (
                (0, low_ref[edge, :] * keep_low),
                (depth, own_ref[col]),
                (depth + fine_rows, high_ref[edge, :] * keep_high),
            )
            for first, piece in pieces:
                last = first + piece.shape[0]
                tall_ref[col, first:last, :] = piece
                if col < 3:
                    base = 2 * rows + total * col
                    left_ref[base + first : base + last, :] = piece
                if col >= fine_cols - 3:
                    base = 2 * rows + total * (col - fine_cols + 3)
                    right_ref[base + first : base + last, :] = piece
        for part in range(2):
            base = part * total
            at = wide + depth * (fine_cols + part)
            stencil_ref[base : base + depth, :] = low_ref[at : at + depth, :]
            stencil_ref[base + depth : base + depth + fine_rows, :] = own_stencil_ref[
                part * fine_rows : (part + 1) * fine_rows, :
            ]
            stencil_ref[base + depth + fine_rows : base + total, :] = high_ref[at : at + depth, :]

    return body


def edges_kernel(cols, rows):
    def body(ens_ref, after_ref, up_ref, down_ref):
        row = lax.broadcasted_iota(jnp.int32, (8, CH), 0)
        for member in range(M):
            lanes = slice(member * CH, (member + 1) * CH)
            block = ens_ref[:, lanes].astype(F32)
            for ref, at in ((up_ref, rows - 1), (down_ref, 0)):
                picked = jnp.zeros((8, CH), F32)
                for col in range(cols):
                    line = block[col * rows + at : col * rows + at + 1]
                    picked = jnp.where(row == col, jnp.broadcast_to(line, (8, CH)), picked)
                ref[:, lanes] = picked[:cols]

    return body


def fine_span(rows, halo):
    return FINE_HALO - 4 - 2 * halo, 2 * rows + 8 + 4 * halo


def lat_coefficients(stencil_ref, rows, halo):
    first, count = fine_span(rows, halo)
    total = 2 * rows + 2 * FINE_HALO
    return stencil_coefficients(
        stencil_ref[first : first + count, :], stencil_ref[total + first : total + first + count, :]
    )


def stencil_coefficients(weight, offset):
    result = []
    for step in range(5):
        lower = jnp.where(offset == float(step), 1.0 - weight, 0.0)
        result.append(lower + jnp.where(offset == float(step - 1), weight, 0.0))
    return result


def restrict_block(even, odd, coefs, spill_ref, sum_ref, cols, rows, halo):
    count = fine_span(rows, halo)[1]
    out = rows + 2 * halo
    for col in range(cols):
        folded = None
        for tap in range(4):
            term = EVEN_TAPS[tap] * even[col + 3 - tap] + ODD_TAPS[tap] * odd[col + 3 - tap]
            folded = term if folded is None else folded + term
        total = None
        for step in range(5):
            slot = col * 5 + step
            spill_ref[slot, 0:count, :] = coefs[step] * folded
            term = spill_ref[slot, 8 - 2 * step : 8 - 2 * step + 2 * out, :]
            total = term if total is None else total + term
        sum_ref[col, 0 : 2 * out, :] = total
    blocks = [
        sum_ref[col, pl.ds(2 * halo, rows, stride=2), :]
        + sum_ref[col, pl.ds(2 * halo + 1, rows, stride=2), :]
        for col in range(cols)
    ]
    return jnp.concatenate(blocks, axis=0)


def weight_column(weight_refs, at, rows, first, count):
    west_ref, tall_ref, east_ref = weight_refs
    fine_cols = tall_ref.shape[0]
    if 3 <= at < fine_cols + 3:
        return tall_ref[at - 3, first : first + count, :]
    ref, col = (west_ref, at) if at < 3 else (east_ref, at - fine_cols - 3)
    base = 2 * rows + tall_ref.shape[1] * col + first
    return ref[base : base + count, :]


def middle(mid_ref, left_ref, right_ref, weight_refs, coefs, dup_ref, spill_ref, sum_ref, rows, halo, mask=None):
    cols = mid_ref.shape[0]
    first, count = fine_span(rows, halo)
    given = rows + 2 * halo + 2
    lat = []
    for col in range(cols + 6):
        if col < 3:
            block = left_ref[col]
        elif col < cols + 3:
            block = mid_ref[col - 3]
        else:
            block = right_ref[col - cols - 3]
        if mask is not None:
            block = block * mask
        dup_ref[col] = jnp.zeros(dup_ref.shape[1:], F32)
        dup_ref[col, pl.ds(PAD, given, stride=2), :] = block
        dup_ref[col, pl.ds(PAD + 1, given, stride=2), :] = block
        total = None
        for step in range(5):
            at = 2 + 2 * step
            term = coefs[step] * dup_ref[col, at : at + count, :]
            total = term if total is None else total + term
        lat.append(total)
    even, odd = [], []
    for at in range(cols + 3):
        left = sum(EVEN_TAPS[tap] * lat[at + tap] for tap in range(4))
        right = sum(ODD_TAPS[tap] * lat[at + tap] for tap in range(4))
        even.append(left * weight_column(weight_refs, 2 * at + 1, rows, first, count))
        odd.append(right * weight_column(weight_refs, 2 * at, rows, first, count))
    return restrict_block(even, odd, coefs, spill_ref, sum_ref, cols, rows, halo)


def start_kernel(cols, rows):
    def body(own_ref, left_ref, right_ref, ens_ref, widths_ref, scales_ref, coarse_ref, image_ref):
        coarse_ref[...] = own_ref[...]
        coarse_ref[0 : 2 * rows, :] += left_ref[0 : 2 * rows, :]
        coarse_ref[(cols - 2) * rows : cols * rows, :] += right_ref[0 : 2 * rows, :]
        image_ref[...] = gram((ens_ref,), widths_ref, scales_ref, coarse_ref[...])

    return body


def step_kernel(cols, rows):
    cells = cols * rows

    def body(mid_ref, left_ref, right_ref, west_ref, tall_ref, east_ref, stencil_ref, flags_ref, ens_ref, ens_low_ref, ens_high_ref,
             widths_ref, scales_ref, coarse_ref, image_ref, padded_ref, dup_ref, spill_ref, sum_ref, rim_ref):
        coefs = lat_coefficients(stencil_ref, rows, 1)
        row = lax.broadcasted_iota(jnp.int32, (rows + 4, CH), 0)
        inside = jnp.where(row < 2, flags_ref[0:1, :], jnp.where(row < rows + 2, 1.0, flags_ref[1:2, :]))
        coarse = middle(
            mid_ref, left_ref, right_ref, (west_ref, tall_ref, east_ref), coefs, dup_ref, spill_ref, sum_ref, rows, 1, inside
        )
        coarse_ref[...] = coarse
        end = 2 * rows + 2
        for col in range(cols):
            low = sum_ref[col, 0:1, :] + sum_ref[col, 1:2, :]
            high = sum_ref[col, end : end + 1, :] + sum_ref[col, end + 1 : end + 2, :]
            rim_ref[col : col + 1, :] = low * flags_ref[0:1, :]
            rim_ref[cols + col : cols + col + 1, :] = high * flags_ref[1:2, :]
        image = gram(
            (ens_ref, ens_low_ref, ens_high_ref), widths_ref, scales_ref,
            jnp.concatenate([coarse, rim_ref[...]], axis=0),
        )
        image_ref[...] = image[:cells]
        for col in range(cols):
            padded_ref[col, 0:1, :] = image[cells + col : cells + col + 1]
            padded_ref[col, 1 : rows + 1, :] = image[col * rows : (col + 1) * rows]
            padded_ref[col, rows + 1 : rows + 2, :] = image[
                cells + cols + col : cells + cols + col + 1
            ]

    return body


def last_kernel(rows, devices):
    def body(mid_ref, left_ref, right_ref, west_ref, tall_ref, east_ref, stencil_ref, y0_ref, b0_ref, y1_ref, b1_ref,
             coarse_ref, dots_ref, dup_ref, spill_ref, sum_ref):
        coefs = lat_coefficients(stencil_ref, rows, 0)
        coarse = middle(
            mid_ref, left_ref, right_ref, (west_ref, tall_ref, east_ref), coefs, dup_ref, spill_ref, sum_ref, rows, 0
        )
        coarse_ref[...] = coarse
        lane = lax.broadcasted_iota(jnp.int32, (1, CH), 1)
        row = jnp.zeros((1, CH), F32)
        b0, b1, y1 = b0_ref[...], b1_ref[...], y1_ref[...]
        pairs = (y0_ref[...] * b0, y1 * b0, y1 * b1, coarse * b1)
        for place, terms in enumerate(pairs):
            total = jnp.sum(jnp.sum(terms, axis=0, keepdims=True), axis=1, keepdims=True)
            row = jnp.where(lane == place, total, row)
        dots_ref[...] = jnp.broadcast_to(row, (devices, CH))

    return body


def final_kernel(entries):
    def body(dots_ref, y0_ref, y1_ref, y2_ref, ens_ref, widths_ref, scales_ref, coef_ref, vector_ref):
        sums = jnp.sum(dots_ref[...], axis=0, keepdims=True)
        lane = lax.broadcasted_iota(jnp.int32, (1, CH), 1)

        def pick(place):
            return jnp.sum(jnp.where(lane == place, sums, 0.0), axis=1, keepdims=True)

        m00, m01, m11, m12 = (pick(place) for place in range(4))
        beta0 = jnp.sqrt(m00 / entries + EPSILON)
        alpha0 = (m00 + m01) / (entries * beta0 * beta0)
        s1 = 1.0 / beta0
        s0 = (1.0 - alpha0) * s1
        u1u1 = s0 * s0 * m00 + 2.0 * s0 * s1 * m01 + s1 * s1 * m11
        beta1 = jnp.sqrt(u1u1 / entries + EPSILON)
        u0u1 = s0 * m00 + s1 * m01
        u0lu1 = s0 * m01 + s1 * m11
        u1lu1 = s0 * s0 * m01 + 2.0 * s0 * s1 * m11 + s1 * s1 * m12
        c0 = (u0u1 + u0lu1) / (entries * beta0 * beta1)
        alpha1 = (u1u1 + u1lu1) / (entries * beta1 * beta1)
        r1 = 1.0 / beta1
        keep = (1.0 - alpha1) * r1
        k0 = keep * s0 - c0 / beta0
        k1 = keep * s1 + s0 * r1
        k2 = s1 * r1
        row = lax.broadcasted_iota(jnp.int32, (2, 2), 0)
        col = lax.broadcasted_iota(jnp.int32, (2, 2), 1)
        coef_ref[...] = jnp.where(
            row == 0, jnp.where(col == 0, alpha0, alpha1), jnp.where(col == 0, beta0, beta1)
        )
        coarse = k0 * y0_ref[...] + k1 * y1_ref[...] + k2 * y2_ref[...]
        distances = pair_distances()
        low_half = lax.broadcasted_iota(jnp.int32, coarse.shape, 1) < LEV
        for pair in range(PAIRS):
            matrix = hat(widths_ref, pair, distances)
            first, second = members((ens_ref,), pair)
            summed = field_sum(first, second, coarse, low_half)
            out = product(summed, matrix) * scales_ref[pair : pair + 1, :]
            vector_ref[:, pair * CH : (pair + 1) * CH] = out.astype(BF16)

    return body


def from_neighbours(up, down, axis, paired):
    count = lax.axis_size(axis)
    if paired and count % 2 == 0:
        odd = lax.axis_index(axis) % 2 == 1
        outer = [(at, (at + 1) % count if at % 2 else (at - 1) % count) for at in range(count)]
        inner = [(at, at + 1 - 2 * (at % 2)) for at in range(count)]
        far = lax.ppermute(jnp.where(odd, up, down), axis, outer)
        near = lax.ppermute(jnp.where(odd, down, up), axis, inner)
        return jnp.where(odd, near, far), jnp.where(odd, far, near)
    low = lax.ppermute(up, axis, [(at, (at + 1) % count) for at in range(count)])
    high = lax.ppermute(down, axis, [((at + 1) % count, at) for at in range(count)])
    return low, high


def per_device(ensemble, innovation, obs_weight, lat_offset, lat_weight, band_widths):
    cols, rows = ensemble.shape[0], ensemble.shape[1]
    cells = cols * rows
    fine_cols, fine_rows = innovation.shape[0], innovation.shape[1]
    total = fine_rows + 2 * FINE_HALO
    lat_count, lon_count = lax.axis_size("lat"), lax.axis_size("lon")
    devices = lat_count * lon_count
    entries = float(cells * M * LEV * devices)
    position = lax.axis_index("lat")
    keeps = jnp.stack([position > 0, position < lat_count - 1]).astype(F32)
    flags = jnp.broadcast_to(keeps[:, None], (2, CH))

    cell_block = pltpu.VMEM((cells, CH), F32)
    pair_block = pltpu.VMEM((PAIRS, CH), F32)
    message = pltpu.VMEM((2 * (cols + 4) + (fine_cols + 2) * FINE_HALO, CH), F32)
    ens_block = pltpu.VMEM((cells, M * CH), BF16)
    up, down, part, own, own_stencil, widths, scales, ens = pl.pallas_call(
        prepare_kernel(cols, rows),
        out_shape=(
            message, message, pltpu.VMEM((cols + 4, rows, CH), F32),
            pltpu.VMEM((fine_cols, fine_rows, CH), F32),
            pltpu.VMEM((2 * fine_rows, CH), F32), pair_block, pair_block, ens_block,
        ),
        in_specs=[VMEM_SPEC] * 5 + [pl.BlockSpec(memory_space=pltpu.HBM)],
        out_specs=(VMEM_SPEC,) * 8,
        scratch_shapes=[
            pltpu.VMEM(((cols + 4) * 5, fine_rows + 16, CH), F32),
            pltpu.VMEM((cols + 4, fine_rows + 8, CH), F32),
            pltpu.SemaphoreType.DMA,
        ],
    )(obs_weight, innovation, lat_weight[None], lat_offset[None], band_widths[None],
      ensemble.reshape(cells, M * CH))
    low, high = from_neighbours(up, down, "lat", False)
    side_block = pltpu.VMEM((2 * rows + 3 * total, CH), F32)
    to_left, to_right, own_part, tall, stencil = kernel_call(
        join_kernel(cols, rows),
        (side_block, side_block, cell_block,
         pltpu.VMEM((fine_cols, total, CH), F32), pltpu.VMEM((2 * total, CH), F32)),
        (low, high, part, own, own_stencil, flags),
    )
    west, east = from_neighbours(to_right, to_left, "lon", True)
    edge_rows = pltpu.VMEM((cols, M * CH), F32)
    ens_up, ens_down = kernel_call(
        edges_kernel(cols, rows), (edge_rows, edge_rows), (ens, to_left)
    )
    ens_low, ens_high = from_neighbours(ens_up, ens_down, "lat", False)

    restrict_scratch = (
        pltpu.VMEM((cols * 5, total, CH), F32),
        pltpu.VMEM((cols, 2 * rows + 8, CH), F32),
    )
    middle_scratch = (pltpu.VMEM((cols + 6, total + 16, CH), F32),) + restrict_scratch

    y0, b0 = kernel_call(
        start_kernel(cols, rows), (cell_block, cell_block),
        (own_part, west, east, ens, widths, scales),
    )
    block = b0.reshape(cols, rows, CH)
    low_rows, high_rows = from_neighbours(block[:, -2:], block[:, :2], "lat", False)
    mid = jnp.concatenate([low_rows, block, high_rows], axis=1)
    mid_left, mid_right = from_neighbours(mid[-3:], mid[:3], "lon", True)
    y1, b1, mid1 = kernel_call(
        step_kernel(cols, rows), (cell_block, cell_block, pltpu.VMEM((cols, rows + 2, CH), F32)),
        (mid, mid_left, mid_right, west, tall, east, stencil, flags,
         ens, ens_low, ens_high, widths, scales),
        middle_scratch + (pltpu.VMEM((2 * cols, CH), F32),),
    )
    y2, dots = kernel_call(
        last_kernel(rows, devices), (cell_block, pltpu.VMEM((devices, CH), F32)),
        (mid1, *from_neighbours(mid1[-3:], mid1[:3], "lon", True), west, tall, east, stencil, y0, b0, y1, b1),
        middle_scratch,
    )
    shared = lax.all_to_all(dots.reshape(devices, 1, CH), ("lat", "lon"), 0, 0).reshape(devices, CH)
    coefficients, vector = kernel_call(
        final_kernel(entries),
        (jax.ShapeDtypeStruct((2, 2), F32), jax.ShapeDtypeStruct((cells, M * LEV), BF16)),
        (shared, y0, y1, y2, ens, widths, scales),
    )
    return coefficients, vector.reshape(cols, rows, M * LEV)


def solution(mesh):
    return jax.shard_map(
        per_device,
        mesh=mesh,
        in_specs=(
            P("lon", "lat", None),
            P("lon", "lat", None),
            P("lon", "lat", None),
            P("lat"),
            P("lat"),
            P(),
        ),
        out_specs=(P(), P("lon", "lat", None)),
        check_vma=False,
    )
```

```python
import jax
import jax.numpy as jnp
from jax import lax
from jax.experimental import pallas as pl
from jax.experimental.pallas import tpu as pltpu
from jax.sharding import PartitionSpec as P

M = 80
LEV = 64
FIELDS = 2

EVEN_TAPS = (-0.0234375, 0.2265625, 0.8671875, -0.0703125)
ODD_TAPS = (-0.0703125, 0.8671875, 0.2265625, -0.0234375)
EPSILON = 1e-06


F32 = jnp.float32
BF16 = jnp.bfloat16
CH = FIELDS * LEV
PAIRS = M // 2
PAD = 8
FINE_HALO = 6
VMEM_SPEC = pl.BlockSpec(memory_space=pltpu.VMEM)


def in_vmem(value):
    return pltpu.with_memory_space_constraint(value, pltpu.VMEM)


def kernel_call(body, outs, operands, scratch=()):
    return pl.pallas_call(
        body,
        out_shape=outs,
        in_specs=[VMEM_SPEC] * len(operands),
        out_specs=jax.tree.map(lambda _: VMEM_SPEC, outs),
        scratch_shapes=list(scratch),
    )(*[in_vmem(operand) for operand in operands])


def split(value):
    high = value.astype(BF16)
    return high, (value - high.astype(F32)).astype(BF16)


def pair_distances():
    row = lax.broadcasted_iota(jnp.int32, (CH, CH), 0)
    col = lax.broadcasted_iota(jnp.int32, (CH, CH), 1)
    distance = jnp.where(row // LEV == col // LEV, jnp.abs(row - col), CH)
    return distance.astype(F32).astype(BF16).reshape(CH // 16, 16, CH)


def hat(widths_ref, pair, distances):
    widths = jnp.broadcast_to(widths_ref[pair : pair + 1, :], (16, CH)).astype(BF16)
    return jnp.maximum(widths[None] - distances, jnp.zeros((), BF16)).reshape(CH, CH)


def product(value, matrix):
    cells = value.shape[0]
    parts = jnp.concatenate(split(value), axis=0)
    both = jnp.dot(parts, matrix, preferred_element_type=F32)
    return both[:cells] + both[cells:]


def swap_halves(value):
    return pltpu.roll(value, LEV, 1)


def members(ens_refs, pair):
    result = []
    for member in (2 * pair, 2 * pair + 1):
        parts = [ref[:, member * CH : (member + 1) * CH].astype(F32) for ref in ens_refs]
        result.append(parts[0] if len(parts) == 1 else jnp.concatenate(parts, axis=0))
    return result


def field_sum(first, second, coarse, low_half):
    left, right = first * coarse, second * coarse
    return jnp.where(low_half, left, right) + swap_halves(jnp.where(low_half, right, left))


def gram(ens_refs, widths_ref, scales_ref, coarse, once_ref, twice_ref):
    distances = pair_distances()
    cells = coarse.shape[0]
    low_half = lax.broadcasted_iota(jnp.int32, coarse.shape, 1) < LEV

    def put(ref, pair, value):
        ref[pair, 0:cells, :], ref[pair, cells : 2 * cells, :] = split(value)

    def apply(ref, pair):
        matrix = hat(widths_ref, pair, distances)
        both = jnp.dot(ref[pair], matrix, preferred_element_type=F32)
        return both[:cells] + both[cells:]

    for pair in range(PAIRS):
        first, second = members(ens_refs, pair)
        put(once_ref, pair, field_sum(first, second, coarse, low_half))
    for pair in range(PAIRS):
        put(twice_ref, pair, apply(once_ref, pair))
    total = jnp.zeros(coarse.shape, F32)
    for pair in range(PAIRS):
        scale = scales_ref[pair : pair + 1, :]
        twice = apply(twice_ref, pair) * (scale * scale)
        swapped = swap_halves(twice)
        first, second = members(ens_refs, pair)
        total = total + (
            first * jnp.where(low_half, twice, swapped)
            + second * jnp.where(low_half, swapped, twice)
        )
    return total


def prepare_kernel(cols, rows):
    depth = FINE_HALO
    fine_cols, fine_rows = 2 * cols, 2 * rows
    spans = rows + 4
    wide = 2 * (cols + 4)

    def body(weight_ref, innovation_ref, lat_weight_ref, lat_offset_ref, band_ref,
             up_ref, down_ref, part_ref, own_ref, own_stencil_ref, widths_ref, scales_ref,
             spill_ref, sum_ref):
        row = lax.broadcasted_iota(jnp.int32, (fine_rows, fine_rows), 0)
        col = lax.broadcasted_iota(jnp.int32, (fine_rows, fine_rows), 1)

        def column(line):
            spread = jnp.broadcast_to(line, (fine_rows, fine_rows))
            values = jnp.sum(jnp.where(row == col, spread, 0.0), axis=1, keepdims=True)
            return jnp.broadcast_to(values, (fine_rows, CH))

        upper = column(lat_weight_ref[...])
        offset = column(lat_offset_ref[...].astype(F32))
        weighted = []
        for at in range(fine_cols):
            weight = weight_ref[at]
            own_ref[at] = weight
            up_ref[wide + depth * at : wide + depth * (at + 1), :] = weight[fine_rows - depth :]
            down_ref[wide + depth * at : wide + depth * (at + 1), :] = weight[:depth]
            weighted.append(weight * innovation_ref[at])
        coefs = stencil_coefficients(upper, offset)
        blank = jnp.zeros((8, CH), F32)
        for at in range(cols + 4):
            folded = None
            for tap in range(4):
                for taps, centre in ((EVEN_TAPS, at - tap), (ODD_TAPS, at - 1 - tap)):
                    if 0 <= centre < cols:
                        term = taps[tap] * weighted[2 * centre + (taps is ODD_TAPS)]
                        folded = term if folded is None else folded + term
            total = None
            for step in range(5):
                slot = at * 5 + step
                spill_ref[slot, 0:8, :] = blank
                spill_ref[slot, 8 + fine_rows : 16 + fine_rows, :] = blank
                spill_ref[slot, 8 : 8 + fine_rows, :] = coefs[step] * folded
                term = spill_ref[slot, 8 - 2 * step : 8 - 2 * step + 2 * spans, :]
                total = term if total is None else total + term
            sum_ref[at] = total
            down_ref[2 * at : 2 * at + 2, :] = (
                sum_ref[at, pl.ds(0, 2, stride=2), :] + sum_ref[at, pl.ds(1, 2, stride=2), :]
            )
            part_ref[at] = (
                sum_ref[at, pl.ds(4, rows, stride=2), :] + sum_ref[at, pl.ds(5, rows, stride=2), :]
            )
            end = 2 * rows + 4
            up_ref[2 * at : 2 * at + 2, :] = (
                sum_ref[at, pl.ds(end, 2, stride=2), :] + sum_ref[at, pl.ds(end + 1, 2, stride=2), :]
            )
        own_stencil_ref[0:fine_rows, :] = upper
        own_stencil_ref[fine_rows : 2 * fine_rows, :] = offset
        at = wide + depth * fine_cols
        up_ref[at : at + depth, :] = upper[fine_rows - depth :]
        up_ref[at + depth : at + 2 * depth, :] = offset[fine_rows - depth :]
        down_ref[at : at + depth, :] = upper[:depth]
        down_ref[at + depth : at + 2 * depth, :] = offset[:depth]
        bands = jnp.broadcast_to((band_ref[...] + 1).astype(F32), (PAIRS, M))
        pair = lax.broadcasted_iota(jnp.int32, (PAIRS, M), 0)
        member = lax.broadcasted_iota(jnp.int32, (PAIRS, M), 1)
        first = jnp.sum(jnp.where(member == 2 * pair, bands, 0.0), axis=1, keepdims=True)
        second = jnp.sum(jnp.where(member == 2 * pair + 1, bands, 0.0), axis=1, keepdims=True)
        lane = lax.broadcasted_iota(jnp.int32, (PAIRS, CH), 1)
        widths = jnp.where(lane < LEV, first, second)
        widths_ref[...] = widths
        scales_ref[...] = 1.0 / (widths * widths)

    return body


def join_kernel(cols, rows):
    depth = FINE_HALO
    fine_cols, fine_rows = 2 * cols, 2 * rows
    wide = 2 * (cols + 4)
    total = fine_rows + 2 * depth

    def body(low_ref, high_ref, part_ref, own_ref, own_stencil_ref, flags_ref,
             left_ref, right_ref, coarse_ref, west_ref, east_ref, tall_ref, stencil_ref):
        keep_low, keep_high = flags_ref[0:1, :], flags_ref[1:2, :]
        middle_rows = jnp.zeros((rows - 4, CH), F32)
        for at in range(cols + 4):
            low = low_ref[2 * at : 2 * at + 2, :] * keep_low
            high = high_ref[2 * at : 2 * at + 2, :] * keep_high
            block = part_ref[at] + jnp.concatenate([low, middle_rows, high], axis=0)
            if at < 2:
                left_ref[at * rows : (at + 1) * rows, :] = block
            elif at < cols + 2:
                coarse_ref[(at - 2) * rows : (at - 1) * rows, :] = block
            else:
                right_ref[(at - cols - 2) * rows : (at - cols - 1) * rows, :] = block
        for col in range(fine_cols):
            edge = slice(wide + depth * col, wide + depth * (col + 1))
            pieces = (
                (0, low_ref[edge, :] * keep_low),
                (depth, own_ref[col]),
                (depth + fine_rows, high_ref[edge, :] * keep_high),
            )
            for first, piece in pieces:
                last = first + piece.shape[0]
                tall_ref[col, first:last, :] = piece
                if col < 3:
                    west_ref[col, first:last, :] = piece
                if col >= fine_cols - 3:
                    east_ref[col - fine_cols + 3, first:last, :] = piece
        for part in range(2):
            base = part * total
            at = wide + depth * (fine_cols + part)
            stencil_ref[base : base + depth, :] = low_ref[at : at + depth, :]
            stencil_ref[base + depth : base + depth + fine_rows, :] = own_stencil_ref[
                part * fine_rows : (part + 1) * fine_rows, :
            ]
            stencil_ref[base + depth + fine_rows : base + total, :] = high_ref[at : at + depth, :]

    return body


def edges_kernel(cols, rows):
    def body(ens_ref, after_ref, up_ref, down_ref):
        row = lax.broadcasted_iota(jnp.int32, (8, CH), 0)
        for member in range(M):
            lanes = slice(member * CH, (member + 1) * CH)
            block = ens_ref[:, lanes].astype(F32)
            for ref, at in ((up_ref, rows - 1), (down_ref, 0)):
                picked = jnp.zeros((8, CH), F32)
                for col in range(cols):
                    line = block[col * rows + at : col * rows + at + 1]
                    picked = jnp.where(row == col, jnp.broadcast_to(line, (8, CH)), picked)
                ref[:, lanes] = picked[:cols]

    return body


def fine_span(rows, halo):
    return FINE_HALO - 4 - 2 * halo, 2 * rows + 8 + 4 * halo


def lat_coefficients(stencil_ref, rows, halo):
    first, count = fine_span(rows, halo)
    total = 2 * rows + 2 * FINE_HALO
    return stencil_coefficients(
        stencil_ref[first : first + count, :], stencil_ref[total + first : total + first + count, :]
    )


def stencil_coefficients(weight, offset):
    result = []
    for step in range(5):
        lower = jnp.where(offset == float(step), 1.0 - weight, 0.0)
        result.append(lower + jnp.where(offset == float(step - 1), weight, 0.0))
    return result


def restrict_block(even, odd, coefs, spill_ref, sum_ref, cols, rows, halo):
    count = fine_span(rows, halo)[1]
    out = rows + 2 * halo
    for col in range(cols):
        folded = None
        for tap in range(4):
            term = EVEN_TAPS[tap] * even[col + 3 - tap] + ODD_TAPS[tap] * odd[col + 3 - tap]
            folded = term if folded is None else folded + term
        total = None
        for step in range(5):
            slot = col * 5 + step
            spill_ref[slot, 0:count, :] = coefs[step] * folded
            term = spill_ref[slot, 8 - 2 * step : 8 - 2 * step + 2 * out, :]
            total = term if total is None else total + term
        sum_ref[col, 0 : 2 * out, :] = total
    blocks = [
        sum_ref[col, pl.ds(2 * halo, rows, stride=2), :]
        + sum_ref[col, pl.ds(2 * halo + 1, rows, stride=2), :]
        for col in range(cols)
    ]
    return jnp.concatenate(blocks, axis=0)


def weight_column(weight_refs, at, first, count):
    west_ref, tall_ref, east_ref = weight_refs
    fine_cols = tall_ref.shape[0]
    if 3 <= at < fine_cols + 3:
        return tall_ref[at - 3, first : first + count, :]
    ref, col = (west_ref, at) if at < 3 else (east_ref, at - fine_cols - 3)
    return ref[col, first : first + count, :]


def middle(mid_ref, left_ref, right_ref, weight_refs, coefs, dup_ref, spill_ref, sum_ref, rows, halo, mask=None):
    cols = mid_ref.shape[0]
    first, count = fine_span(rows, halo)
    given = rows + 2 * halo + 2
    lat = []
    for col in range(cols + 6):
        if col < 3:
            block = left_ref[col]
        elif col < cols + 3:
            block = mid_ref[col - 3]
        else:
            block = right_ref[col - cols - 3]
        if mask is not None:
            block = block * mask
        dup_ref[col] = jnp.zeros(dup_ref.shape[1:], F32)
        dup_ref[col, pl.ds(PAD, given, stride=2), :] = block
        dup_ref[col, pl.ds(PAD + 1, given, stride=2), :] = block
        total = None
        for step in range(5):
            at = 2 + 2 * step
            term = coefs[step] * dup_ref[col, at : at + count, :]
            total = term if total is None else total + term
        lat.append(total)
    even, odd = [], []
    for at in range(cols + 3):
        left = sum(EVEN_TAPS[tap] * lat[at + tap] for tap in range(4))
        right = sum(ODD_TAPS[tap] * lat[at + tap] for tap in range(4))
        even.append(left * weight_column(weight_refs, 2 * at + 1, first, count))
        odd.append(right * weight_column(weight_refs, 2 * at, first, count))
    return restrict_block(even, odd, coefs, spill_ref, sum_ref, cols, rows, halo)


def start_kernel(cols, rows):
    def body(own_ref, left_ref, right_ref, ens_ref, widths_ref, scales_ref, coarse_ref, image_ref, once_ref, twice_ref):
        coarse_ref[...] = own_ref[...]
        coarse_ref[0 : 2 * rows, :] += left_ref[...]
        coarse_ref[(cols - 2) * rows : cols * rows, :] += right_ref[...]
        image_ref[...] = gram(
            (ens_ref,), widths_ref, scales_ref, coarse_ref[...], once_ref, twice_ref
        )

    return body


def step_kernel(cols, rows):
    cells = cols * rows

    def body(mid_ref, left_ref, right_ref, west_ref, tall_ref, east_ref, stencil_ref, flags_ref, ens_ref, ens_low_ref, ens_high_ref,
             widths_ref, scales_ref, coarse_ref, image_ref, padded_ref, dup_ref, spill_ref, sum_ref, rim_ref, once_ref, twice_ref):
        coefs = lat_coefficients(stencil_ref, rows, 1)
        row = lax.broadcasted_iota(jnp.int32, (rows + 4, CH), 0)
        inside = jnp.where(row < 2, flags_ref[0:1, :], jnp.where(row < rows + 2, 1.0, flags_ref[1:2, :]))
        coarse = middle(
            mid_ref, left_ref, right_ref, (west_ref, tall_ref, east_ref), coefs, dup_ref, spill_ref, sum_ref, rows, 1, inside
        )
        coarse_ref[...] = coarse
        end = 2 * rows + 2
        for col in range(cols):
            low = sum_ref[col, 0:1, :] + sum_ref[col, 1:2, :]
            high = sum_ref[col, end : end + 1, :] + sum_ref[col, end + 1 : end + 2, :]
            rim_ref[col : col + 1, :] = low * flags_ref[0:1, :]
            rim_ref[cols + col : cols + col + 1, :] = high * flags_ref[1:2, :]
        image = gram(
            (ens_ref, ens_low_ref, ens_high_ref), widths_ref, scales_ref,
            jnp.concatenate([coarse, rim_ref[...]], axis=0), once_ref, twice_ref,
        )
        image_ref[...] = image[:cells]
        for col in range(cols):
            padded_ref[col, 0:1, :] = image[cells + col : cells + col + 1]
            padded_ref[col, 1 : rows + 1, :] = image[col * rows : (col + 1) * rows]
            padded_ref[col, rows + 1 : rows + 2, :] = image[
                cells + cols + col : cells + cols + col + 1
            ]

    return body


def last_kernel(rows, devices):
    def body(mid_ref, left_ref, right_ref, west_ref, tall_ref, east_ref, stencil_ref, y0_ref, b0_ref, y1_ref, b1_ref,
             coarse_ref, dots_ref, dup_ref, spill_ref, sum_ref):
        coefs = lat_coefficients(stencil_ref, rows, 0)
        coarse = middle(
            mid_ref, left_ref, right_ref, (west_ref, tall_ref, east_ref), coefs, dup_ref, spill_ref, sum_ref, rows, 0
        )
        coarse_ref[...] = coarse
        lane = lax.broadcasted_iota(jnp.int32, (1, CH), 1)
        row = jnp.zeros((1, CH), F32)
        b0, b1, y1 = b0_ref[...], b1_ref[...], y1_ref[...]
        pairs = (y0_ref[...] * b0, y1 * b0, y1 * b1, coarse * b1)
        for place, terms in enumerate(pairs):
            total = jnp.sum(jnp.sum(terms, axis=0, keepdims=True), axis=1, keepdims=True)
            row = jnp.where(lane == place, total, row)
        dots_ref[...] = jnp.broadcast_to(row, (devices, CH))

    return body


def final_kernel(entries):
    def body(dots_ref, y0_ref, y1_ref, y2_ref, ens_ref, widths_ref, scales_ref, coef_ref, vector_ref):
        sums = jnp.sum(dots_ref[...], axis=0, keepdims=True)
        lane = lax.broadcasted_iota(jnp.int32, (1, CH), 1)

        def pick(place):
            return jnp.sum(jnp.where(lane == place, sums, 0.0), axis=1, keepdims=True)

        m00, m01, m11, m12 = (pick(place) for place in range(4))
        square0 = m00 / entries + EPSILON
        inverse0 = 1.0 / square0
        alpha0 = ((m00 + m01) / entries) * inverse0
        g = 1.0 - alpha0
        u1u1 = (g * (g * m00 + 2.0 * m01) + m11) * inverse0
        u1lu1 = (g * (g * m01 + 2.0 * m11) + m12) * inverse0
        cross = ((g * (m00 + m01) + m01 + m11) / entries) * inverse0
        square1 = u1u1 / entries + EPSILON
        alpha1 = ((u1u1 + u1lu1) / entries) / square1
        beta0, beta1 = jnp.sqrt(square0), jnp.sqrt(square1)
        k2 = lax.rsqrt(square0) * lax.rsqrt(square1)
        k1 = k2 * (1.0 - alpha1 + g)
        k0 = k2 * ((1.0 - alpha1) * g - cross)
        row = lax.broadcasted_iota(jnp.int32, (2, 2), 0)
        col = lax.broadcasted_iota(jnp.int32, (2, 2), 1)
        coef_ref[...] = jnp.where(
            row == 0, jnp.where(col == 0, alpha0, alpha1), jnp.where(col == 0, beta0, beta1)
        )
        coarse = k0 * y0_ref[...] + k1 * y1_ref[...] + k2 * y2_ref[...]
        distances = pair_distances()
        low_half = lax.broadcasted_iota(jnp.int32, coarse.shape, 1) < LEV
        for pair in range(PAIRS):
            matrix = hat(widths_ref, pair, distances)
            first, second = members((ens_ref,), pair)
            summed = field_sum(first, second, coarse, low_half)
            out = product(summed, matrix) * scales_ref[pair : pair + 1, :]
            vector_ref[:, pair * CH : (pair + 1) * CH] = out.astype(BF16)

    return body


def gram_scratch(cells):
    return (pltpu.VMEM((PAIRS, 2 * cells, CH), BF16),) * 2


def from_neighbours(up, down, axis, paired):
    count = lax.axis_size(axis)
    if paired and count % 2 == 0:
        odd = lax.axis_index(axis) % 2 == 1
        outer = [(at, (at + 1) % count if at % 2 else (at - 1) % count) for at in range(count)]
        inner = [(at, at + 1 - 2 * (at % 2)) for at in range(count)]
        far = lax.ppermute(jnp.where(odd, up, down), axis, outer)
        near = lax.ppermute(jnp.where(odd, down, up), axis, inner)
        return jnp.where(odd, near, far), jnp.where(odd, far, near)
    low = lax.ppermute(up, axis, [(at, (at + 1) % count) for at in range(count)])
    high = lax.ppermute(down, axis, [((at + 1) % count, at) for at in range(count)])
    return low, high


def per_device(ensemble, innovation, obs_weight, lat_offset, lat_weight, band_widths):
    cols, rows = ensemble.shape[0], ensemble.shape[1]
    cells = cols * rows
    fine_cols, fine_rows = innovation.shape[0], innovation.shape[1]
    total = fine_rows + 2 * FINE_HALO
    lat_count, lon_count = lax.axis_size("lat"), lax.axis_size("lon")
    devices = lat_count * lon_count
    entries = float(cells * M * LEV * devices)
    position = lax.axis_index("lat")
    keeps = jnp.stack([position > 0, position < lat_count - 1]).astype(F32)
    flags = jnp.broadcast_to(keeps[:, None], (2, CH))

    cell_block = pltpu.VMEM((cells, CH), F32)
    pair_block = pltpu.VMEM((PAIRS, CH), F32)
    message = pltpu.VMEM((2 * (cols + 4) + (fine_cols + 2) * FINE_HALO, CH), F32)
    ens = ensemble.reshape(cells, M * CH)
    up, down, part, own, own_stencil, widths, scales = pl.pallas_call(
        prepare_kernel(cols, rows),
        out_shape=(
            message, message, pltpu.VMEM((cols + 4, rows, CH), F32),
            pltpu.VMEM((fine_cols, fine_rows, CH), F32),
            pltpu.VMEM((2 * fine_rows, CH), F32), pair_block, pair_block,
        ),
        in_specs=[VMEM_SPEC] * 5,
        out_specs=(VMEM_SPEC,) * 7,
        scratch_shapes=[
            pltpu.VMEM(((cols + 4) * 5, fine_rows + 16, CH), F32),
            pltpu.VMEM((cols + 4, fine_rows + 8, CH), F32),
        ],
        cost_estimate=pl.CostEstimate(flops=1 << 29, bytes_accessed=1 << 21, transcendentals=0),
    )(obs_weight, innovation, lat_weight[None], lat_offset[None], band_widths[None])
    low, high = from_neighbours(up, down, "lat", False)
    edge_rows = pltpu.VMEM((cols, M * CH), F32)
    ens_up, ens_down = kernel_call(
        edges_kernel(cols, rows), (edge_rows, edge_rows), (ens, own_stencil)
    )
    ens_low, ens_high = from_neighbours(ens_up, ens_down, "lat", False)
    side_block = pltpu.VMEM((2 * rows, CH), F32)
    wide_block = pltpu.VMEM((3, total, CH), F32)
    to_left, to_right, own_part, to_west, to_east, tall, stencil = kernel_call(
        join_kernel(cols, rows),
        (side_block, side_block, cell_block, wide_block, wide_block,
         pltpu.VMEM((fine_cols, total, CH), F32), pltpu.VMEM((2 * total, CH), F32)),
        (low, high, part, own, own_stencil, flags),
    )
    left, right = from_neighbours(to_right, to_left, "lon", True)
    west, east = from_neighbours(to_east, to_west, "lon", True)

    restrict_scratch = (
        pltpu.VMEM((cols * 5, total, CH), F32),
        pltpu.VMEM((cols, 2 * rows + 8, CH), F32),
    )
    middle_scratch = (pltpu.VMEM((cols + 6, total + 16, CH), F32),) + restrict_scratch

    y0, b0 = kernel_call(
        start_kernel(cols, rows), (cell_block, cell_block),
        (own_part, left, right, ens, widths, scales), gram_scratch(cells),
    )
    block = b0.reshape(cols, rows, CH)
    low_rows, high_rows = from_neighbours(block[:, -2:], block[:, :2], "lat", False)
    mid = jnp.concatenate([low_rows, block, high_rows], axis=1)
    mid_left, mid_right = from_neighbours(mid[-3:], mid[:3], "lon", True)
    y1, b1, mid1 = kernel_call(
        step_kernel(cols, rows), (cell_block, cell_block, pltpu.VMEM((cols, rows + 2, CH), F32)),
        (mid, mid_left, mid_right, west, tall, east, stencil, flags,
         ens, ens_low, ens_high, widths, scales),
        middle_scratch + (pltpu.VMEM((2 * cols, CH), F32),) + gram_scratch(cells + 2 * cols),
    )
    y2, dots = kernel_call(
        last_kernel(rows, devices), (cell_block, pltpu.VMEM((devices, CH), F32)),
        (mid1, *from_neighbours(mid1[-3:], mid1[:3], "lon", True), west, tall, east, stencil, y0, b0, y1, b1),
        middle_scratch,
    )
    shared = lax.all_to_all(dots.reshape(devices, 1, CH), ("lat", "lon"), 0, 0).reshape(devices, CH)
    coefficients, vector = kernel_call(
        final_kernel(entries),
        (jax.ShapeDtypeStruct((2, 2), F32), jax.ShapeDtypeStruct((cells, M * LEV), BF16)),
        (shared, y0, y1, y2, ens, widths, scales),
    )
    return coefficients, vector.reshape(cols, rows, M * LEV)


def solution(mesh):
    return jax.shard_map(
        per_device,
        mesh=mesh,
        in_specs=(
            P("lon", "lat", None),
            P("lon", "lat", None),
            P("lon", "lat", None),
            P("lat"),
            P("lat"),
            P(),
        ),
        out_specs=(P(), P("lon", "lat", None)),
        check_vma=False,
    )
```

```python
import jax
import jax.numpy as jnp
from jax import lax
from jax.experimental import pallas as pl
from jax.experimental.pallas import tpu as pltpu
from jax.sharding import PartitionSpec as P

M = 80
LEV = 64
FIELDS = 2

EVEN_TAPS = (-0.0234375, 0.2265625, 0.8671875, -0.0703125)
ODD_TAPS = (-0.0703125, 0.8671875, 0.2265625, -0.0234375)
EPSILON = 1e-06


F32 = jnp.float32
BF16 = jnp.bfloat16
CH = FIELDS * LEV
PAIRS = M // 2
PAD = 8
FINE_HALO = 6
VMEM_SPEC = pl.BlockSpec(memory_space=pltpu.VMEM)


def in_vmem(value):
    return pltpu.with_memory_space_constraint(value, pltpu.VMEM)


def kernel_call(body, outs, operands, scratch=()):
    return pl.pallas_call(
        body,
        out_shape=outs,
        in_specs=[VMEM_SPEC] * len(operands),
        out_specs=jax.tree.map(lambda _: VMEM_SPEC, outs),
        scratch_shapes=list(scratch),
    )(*[in_vmem(operand) for operand in operands])


def split(value):
    high = value.astype(BF16)
    return high, (value - high.astype(F32)).astype(BF16)


def pair_distances():
    row = lax.broadcasted_iota(jnp.int32, (CH, CH), 0)
    col = lax.broadcasted_iota(jnp.int32, (CH, CH), 1)
    distance = jnp.where(row // LEV == col // LEV, jnp.abs(row - col), CH)
    return distance.astype(F32).astype(BF16).reshape(CH // 16, 16, CH)


def hat(widths_ref, pair, distances):
    widths = jnp.broadcast_to(widths_ref[pair : pair + 1, :], (16, CH)).astype(BF16)
    return jnp.maximum(widths[None] - distances, jnp.zeros((), BF16)).reshape(CH, CH)


def product(value, matrix):
    cells = value.shape[0]
    parts = jnp.concatenate(split(value), axis=0)
    both = jnp.dot(parts, matrix, preferred_element_type=F32)
    return both[:cells] + both[cells:]


def swap_halves(value):
    return pltpu.roll(value, LEV, 1)


def by_field(value, low_half):
    swapped = swap_halves(value)
    return jnp.where(low_half, value, swapped), jnp.where(low_half, swapped, value)


def arrange_kernel(body_rows):
    def body(*refs):
        ens_refs, (one_ref, two_ref) = refs[:-2], refs[-2:]
        low_half = lax.broadcasted_iota(jnp.int32, (body_rows, CH), 1) < LEV
        for pair in range(PAIRS):
            both = []
            for member in (2 * pair, 2 * pair + 1):
                parts = [ref[:, member * CH : (member + 1) * CH].astype(F32) for ref in ens_refs]
                both.append(parts[0] if len(parts) == 1 else jnp.concatenate(parts, axis=0))
            first, second = both
            one_ref[pair] = jnp.where(low_half, first, swap_halves(second))
            two_ref[pair] = jnp.where(low_half, swap_halves(first), second)

    return body


def pair_members(ens_refs, pair):
    parts = [ref[pair] for ref in ens_refs]
    return parts[0] if len(parts) == 1 else jnp.concatenate(parts, axis=0)


def gram(ones, twos, widths_ref, scales_ref, coarse, once_ref, twice_ref):
    distances = pair_distances()
    cells = coarse.shape[0]
    low_half = lax.broadcasted_iota(jnp.int32, coarse.shape, 1) < LEV
    field_one, field_two = by_field(coarse, low_half)

    def put(ref, pair, value):
        ref[pair, 0:cells, :], ref[pair, cells : 2 * cells, :] = split(value)

    def apply(ref, pair):
        matrix = hat(widths_ref, pair, distances)
        both = jnp.dot(ref[pair], matrix, preferred_element_type=F32)
        return both[:cells] + both[cells:]

    for pair in range(PAIRS):
        summed = pair_members(ones, pair) * field_one + pair_members(twos, pair) * field_two
        put(once_ref, pair, summed)
    for pair in range(PAIRS):
        put(twice_ref, pair, apply(once_ref, pair))
    total_one = jnp.zeros(coarse.shape, F32)
    total_two = jnp.zeros(coarse.shape, F32)
    for pair in range(PAIRS):
        scale = scales_ref[pair : pair + 1, :]
        twice = apply(twice_ref, pair) * (scale * scale)
        total_one = total_one + pair_members(ones, pair) * twice
        total_two = total_two + pair_members(twos, pair) * twice
    return jnp.where(
        low_half, total_one + swap_halves(total_one), total_two + swap_halves(total_two)
    )


def prepare_kernel(cols, rows):
    depth = FINE_HALO
    fine_cols, fine_rows = 2 * cols, 2 * rows
    spans = rows + 4
    wide = 2 * (cols + 4)

    def body(weight_ref, innovation_ref, lat_weight_ref, lat_offset_ref, band_ref,
             up_ref, down_ref, part_ref, own_ref, own_stencil_ref, widths_ref, scales_ref,
             spill_ref, sum_ref):
        row = lax.broadcasted_iota(jnp.int32, (fine_rows, fine_rows), 0)
        col = lax.broadcasted_iota(jnp.int32, (fine_rows, fine_rows), 1)

        def column(line):
            spread = jnp.broadcast_to(line, (fine_rows, fine_rows))
            values = jnp.sum(jnp.where(row == col, spread, 0.0), axis=1, keepdims=True)
            return jnp.broadcast_to(values, (fine_rows, CH))

        upper = column(lat_weight_ref[...])
        offset = column(lat_offset_ref[...].astype(F32))
        weighted = []
        for at in range(fine_cols):
            weight = weight_ref[at]
            own_ref[at] = weight
            up_ref[wide + depth * at : wide + depth * (at + 1), :] = weight[fine_rows - depth :]
            down_ref[wide + depth * at : wide + depth * (at + 1), :] = weight[:depth]
            weighted.append(weight * innovation_ref[at])
        coefs = stencil_coefficients(upper, offset)
        blank = jnp.zeros((8, CH), F32)
        for at in range(cols + 4):
            folded = None
            for tap in range(4):
                for taps, centre in ((EVEN_TAPS, at - tap), (ODD_TAPS, at - 1 - tap)):
                    if 0 <= centre < cols:
                        term = taps[tap] * weighted[2 * centre + (taps is ODD_TAPS)]
                        folded = term if folded is None else folded + term
            total = None
            for step in range(5):
                slot = at * 5 + step
                spill_ref[slot, 0:8, :] = blank
                spill_ref[slot, 8 + fine_rows : 16 + fine_rows, :] = blank
                spill_ref[slot, 8 : 8 + fine_rows, :] = coefs[step] * folded
                term = spill_ref[slot, 8 - 2 * step : 8 - 2 * step + 2 * spans, :]
                total = term if total is None else total + term
            sum_ref[at] = total
            down_ref[2 * at : 2 * at + 2, :] = (
                sum_ref[at, pl.ds(0, 2, stride=2), :] + sum_ref[at, pl.ds(1, 2, stride=2), :]
            )
            part_ref[at] = (
                sum_ref[at, pl.ds(4, rows, stride=2), :] + sum_ref[at, pl.ds(5, rows, stride=2), :]
            )
            end = 2 * rows + 4
            up_ref[2 * at : 2 * at + 2, :] = (
                sum_ref[at, pl.ds(end, 2, stride=2), :] + sum_ref[at, pl.ds(end + 1, 2, stride=2), :]
            )
        own_stencil_ref[0:fine_rows, :] = upper
        own_stencil_ref[fine_rows : 2 * fine_rows, :] = offset
        at = wide + depth * fine_cols
        up_ref[at : at + depth, :] = upper[fine_rows - depth :]
        up_ref[at + depth : at + 2 * depth, :] = offset[fine_rows - depth :]
        down_ref[at : at + depth, :] = upper[:depth]
        down_ref[at + depth : at + 2 * depth, :] = offset[:depth]
        bands = jnp.broadcast_to((band_ref[...] + 1).astype(F32), (PAIRS, M))
        pair = lax.broadcasted_iota(jnp.int32, (PAIRS, M), 0)
        member = lax.broadcasted_iota(jnp.int32, (PAIRS, M), 1)
        first = jnp.sum(jnp.where(member == 2 * pair, bands, 0.0), axis=1, keepdims=True)
        second = jnp.sum(jnp.where(member == 2 * pair + 1, bands, 0.0), axis=1, keepdims=True)
        lane = lax.broadcasted_iota(jnp.int32, (PAIRS, CH), 1)
        widths = jnp.where(lane < LEV, first, second)
        widths_ref[...] = widths
        scales_ref[...] = 1.0 / (widths * widths)

    return body


def join_kernel(cols, rows):
    depth = FINE_HALO
    fine_cols, fine_rows = 2 * cols, 2 * rows
    wide = 2 * (cols + 4)
    total = fine_rows + 2 * depth

    def body(low_ref, high_ref, part_ref, own_ref, own_stencil_ref, flags_ref,
             left_ref, right_ref, coarse_ref, west_ref, east_ref, tall_ref, stencil_ref):
        keep_low, keep_high = flags_ref[0:1, :], flags_ref[1:2, :]
        middle_rows = jnp.zeros((rows - 4, CH), F32)
        for at in range(cols + 4):
            low = low_ref[2 * at : 2 * at + 2, :] * keep_low
            high = high_ref[2 * at : 2 * at + 2, :] * keep_high
            block = part_ref[at] + jnp.concatenate([low, middle_rows, high], axis=0)
            if at < 2:
                left_ref[at * rows : (at + 1) * rows, :] = block
            elif at < cols + 2:
                coarse_ref[(at - 2) * rows : (at - 1) * rows, :] = block
            else:
                right_ref[(at - cols - 2) * rows : (at - cols - 1) * rows, :] = block
        for col in range(fine_cols):
            edge = slice(wide + depth * col, wide + depth * (col + 1))
            pieces = (
                (0, low_ref[edge, :] * keep_low),
                (depth, own_ref[col]),
                (depth + fine_rows, high_ref[edge, :] * keep_high),
            )
            for first, piece in pieces:
                last = first + piece.shape[0]
                tall_ref[col, first:last, :] = piece
                if col < 3:
                    west_ref[col, first:last, :] = piece
                if col >= fine_cols - 3:
                    east_ref[col - fine_cols + 3, first:last, :] = piece
        for part in range(2):
            base = part * total
            at = wide + depth * (fine_cols + part)
            stencil_ref[base : base + depth, :] = low_ref[at : at + depth, :]
            stencil_ref[base + depth : base + depth + fine_rows, :] = own_stencil_ref[
                part * fine_rows : (part + 1) * fine_rows, :
            ]
            stencil_ref[base + depth + fine_rows : base + total, :] = high_ref[at : at + depth, :]

    return body


def edges_kernel(cols, rows):
    def body(ens_ref, after_ref, up_ref, down_ref):
        row = lax.broadcasted_iota(jnp.int32, (8, CH), 0)
        for member in range(M):
            lanes = slice(member * CH, (member + 1) * CH)
            block = ens_ref[:, lanes].astype(F32)
            for ref, at in ((up_ref, rows - 1), (down_ref, 0)):
                picked = jnp.zeros((8, CH), F32)
                for col in range(cols):
                    line = block[col * rows + at : col * rows + at + 1]
                    picked = jnp.where(row == col, jnp.broadcast_to(line, (8, CH)), picked)
                ref[:, lanes] = picked[:cols]

    return body


def fine_span(rows, halo):
    return FINE_HALO - 4 - 2 * halo, 2 * rows + 8 + 4 * halo


def lat_coefficients(stencil_ref, rows, halo):
    first, count = fine_span(rows, halo)
    total = 2 * rows + 2 * FINE_HALO
    return stencil_coefficients(
        stencil_ref[first : first + count, :], stencil_ref[total + first : total + first + count, :]
    )


def stencil_coefficients(weight, offset):
    result = []
    for step in range(5):
        lower = jnp.where(offset == float(step), 1.0 - weight, 0.0)
        result.append(lower + jnp.where(offset == float(step - 1), weight, 0.0))
    return result


def restrict_block(even, odd, coefs, spill_ref, sum_ref, cols, rows, halo):
    count = fine_span(rows, halo)[1]
    out = rows + 2 * halo
    for col in range(cols):
        folded = None
        for tap in range(4):
            term = EVEN_TAPS[tap] * even[col + 3 - tap] + ODD_TAPS[tap] * odd[col + 3 - tap]
            folded = term if folded is None else folded + term
        total = None
        for step in range(5):
            slot = col * 5 + step
            spill_ref[slot, 0:count, :] = coefs[step] * folded
            term = spill_ref[slot, 8 - 2 * step : 8 - 2 * step + 2 * out, :]
            total = term if total is None else total + term
        sum_ref[col, 0 : 2 * out, :] = total
    blocks = [
        sum_ref[col, pl.ds(2 * halo, rows, stride=2), :]
        + sum_ref[col, pl.ds(2 * halo + 1, rows, stride=2), :]
        for col in range(cols)
    ]
    return jnp.concatenate(blocks, axis=0)


def weight_column(weight_refs, at, first, count):
    west_ref, tall_ref, east_ref = weight_refs
    fine_cols = tall_ref.shape[0]
    if 3 <= at < fine_cols + 3:
        return tall_ref[at - 3, first : first + count, :]
    ref, col = (west_ref, at) if at < 3 else (east_ref, at - fine_cols - 3)
    return ref[col, first : first + count, :]


def middle(mid_ref, left_ref, right_ref, weight_refs, coefs, dup_ref, spill_ref, sum_ref, rows, halo, mask=None):
    cols = mid_ref.shape[0]
    first, count = fine_span(rows, halo)
    given = rows + 2 * halo + 2
    lat = []
    for col in range(cols + 6):
        if col < 3:
            block = left_ref[col]
        elif col < cols + 3:
            block = mid_ref[col - 3]
        else:
            block = right_ref[col - cols - 3]
        if mask is not None:
            block = block * mask
        dup_ref[col] = jnp.zeros(dup_ref.shape[1:], F32)
        dup_ref[col, pl.ds(PAD, given, stride=2), :] = block
        dup_ref[col, pl.ds(PAD + 1, given, stride=2), :] = block
        total = None
        for step in range(5):
            at = 2 + 2 * step
            term = coefs[step] * dup_ref[col, at : at + count, :]
            total = term if total is None else total + term
        lat.append(total)
    even, odd = [], []
    for at in range(cols + 3):
        left = sum(EVEN_TAPS[tap] * lat[at + tap] for tap in range(4))
        right = sum(ODD_TAPS[tap] * lat[at + tap] for tap in range(4))
        even.append(left * weight_column(weight_refs, 2 * at + 1, first, count))
        odd.append(right * weight_column(weight_refs, 2 * at, first, count))
    return restrict_block(even, odd, coefs, spill_ref, sum_ref, cols, rows, halo)


def start_kernel(cols, rows):
    def body(own_ref, left_ref, right_ref, one_ref, two_ref, widths_ref, scales_ref, coarse_ref, image_ref, once_ref, twice_ref):
        coarse_ref[...] = own_ref[...]
        coarse_ref[0 : 2 * rows, :] += left_ref[...]
        coarse_ref[(cols - 2) * rows : cols * rows, :] += right_ref[...]
        image_ref[...] = gram(
            (one_ref,), (two_ref,), widths_ref, scales_ref, coarse_ref[...], once_ref, twice_ref
        )

    return body


def step_kernel(cols, rows):
    cells = cols * rows

    def body(mid_ref, left_ref, right_ref, west_ref, tall_ref, east_ref, stencil_ref, flags_ref, one_ref, two_ref, rim_one_ref, rim_two_ref,
             widths_ref, scales_ref, coarse_ref, image_ref, padded_ref, dup_ref, spill_ref, sum_ref, rim_ref, once_ref, twice_ref):
        coefs = lat_coefficients(stencil_ref, rows, 1)
        row = lax.broadcasted_iota(jnp.int32, (rows + 4, CH), 0)
        inside = jnp.where(row < 2, flags_ref[0:1, :], jnp.where(row < rows + 2, 1.0, flags_ref[1:2, :]))
        coarse = middle(
            mid_ref, left_ref, right_ref, (west_ref, tall_ref, east_ref), coefs, dup_ref, spill_ref, sum_ref, rows, 1, inside
        )
        coarse_ref[...] = coarse
        end = 2 * rows + 2
        for col in range(cols):
            low = sum_ref[col, 0:1, :] + sum_ref[col, 1:2, :]
            high = sum_ref[col, end : end + 1, :] + sum_ref[col, end + 1 : end + 2, :]
            rim_ref[col : col + 1, :] = low * flags_ref[0:1, :]
            rim_ref[cols + col : cols + col + 1, :] = high * flags_ref[1:2, :]
        image = gram(
            (one_ref, rim_one_ref), (two_ref, rim_two_ref), widths_ref, scales_ref,
            jnp.concatenate([coarse, rim_ref[...]], axis=0), once_ref, twice_ref,
        )
        image_ref[...] = image[:cells]
        for col in range(cols):
            padded_ref[col, 0:1, :] = image[cells + col : cells + col + 1]
            padded_ref[col, 1 : rows + 1, :] = image[col * rows : (col + 1) * rows]
            padded_ref[col, rows + 1 : rows + 2, :] = image[
                cells + cols + col : cells + cols + col + 1
            ]

    return body


def last_kernel(rows, devices):
    def body(mid_ref, left_ref, right_ref, west_ref, tall_ref, east_ref, stencil_ref, y0_ref, b0_ref, y1_ref, b1_ref,
             coarse_ref, dots_ref, dup_ref, spill_ref, sum_ref):
        coefs = lat_coefficients(stencil_ref, rows, 0)
        coarse = middle(
            mid_ref, left_ref, right_ref, (west_ref, tall_ref, east_ref), coefs, dup_ref, spill_ref, sum_ref, rows, 0
        )
        coarse_ref[...] = coarse
        lane = lax.broadcasted_iota(jnp.int32, (1, CH), 1)
        row = jnp.zeros((1, CH), F32)
        b0, b1, y1 = b0_ref[...], b1_ref[...], y1_ref[...]
        pairs = (y0_ref[...] * b0, y1 * b0, y1 * b1, coarse * b1)
        for place, terms in enumerate(pairs):
            total = jnp.sum(jnp.sum(terms, axis=0, keepdims=True), axis=1, keepdims=True)
            row = jnp.where(lane == place, total, row)
        dots_ref[...] = jnp.broadcast_to(row, (devices, CH))

    return body


def final_kernel(entries):
    def body(dots_ref, y0_ref, y1_ref, y2_ref, one_ref, two_ref, widths_ref, scales_ref, coef_ref, vector_ref):
        sums = jnp.sum(dots_ref[...], axis=0, keepdims=True)
        lane = lax.broadcasted_iota(jnp.int32, (1, CH), 1)

        def pick(place):
            return jnp.sum(jnp.where(lane == place, sums, 0.0), axis=1, keepdims=True)

        m00, m01, m11, m12 = (pick(place) for place in range(4))
        square0 = m00 / entries + EPSILON
        inverse0 = 1.0 / square0
        alpha0 = ((m00 + m01) / entries) * inverse0
        g = 1.0 - alpha0
        u1u1 = (g * (g * m00 + 2.0 * m01) + m11) * inverse0
        u1lu1 = (g * (g * m01 + 2.0 * m11) + m12) * inverse0
        cross = ((g * (m00 + m01) + m01 + m11) / entries) * inverse0
        square1 = u1u1 / entries + EPSILON
        alpha1 = ((u1u1 + u1lu1) / entries) / square1
        beta0, beta1 = jnp.sqrt(square0), jnp.sqrt(square1)
        k2 = lax.rsqrt(square0) * lax.rsqrt(square1)
        k1 = k2 * (1.0 - alpha1 + g)
        k0 = k2 * ((1.0 - alpha1) * g - cross)
        row = lax.broadcasted_iota(jnp.int32, (2, 2), 0)
        col = lax.broadcasted_iota(jnp.int32, (2, 2), 1)
        coef_ref[...] = jnp.where(
            row == 0, jnp.where(col == 0, alpha0, alpha1), jnp.where(col == 0, beta0, beta1)
        )
        coarse = k0 * y0_ref[...] + k1 * y1_ref[...] + k2 * y2_ref[...]
        distances = pair_distances()
        low_half = lax.broadcasted_iota(jnp.int32, coarse.shape, 1) < LEV
        field_one, field_two = by_field(coarse, low_half)
        for pair in range(PAIRS):
            matrix = hat(widths_ref, pair, distances)
            summed = one_ref[pair] * field_one + two_ref[pair] * field_two
            out = product(summed, matrix) * scales_ref[pair : pair + 1, :]
            vector_ref[:, pair * CH : (pair + 1) * CH] = out.astype(BF16)

    return body


def gram_scratch(cells):
    return (pltpu.VMEM((PAIRS, 2 * cells, CH), BF16),) * 2


def from_neighbours(up, down, axis, paired):
    count = lax.axis_size(axis)
    if paired and count % 2 == 0:
        odd = lax.axis_index(axis) % 2 == 1
        outer = [(at, (at + 1) % count if at % 2 else (at - 1) % count) for at in range(count)]
        inner = [(at, at + 1 - 2 * (at % 2)) for at in range(count)]
        far = lax.ppermute(jnp.where(odd, up, down), axis, outer)
        near = lax.ppermute(jnp.where(odd, down, up), axis, inner)
        return jnp.where(odd, near, far), jnp.where(odd, far, near)
    low = lax.ppermute(up, axis, [(at, (at + 1) % count) for at in range(count)])
    high = lax.ppermute(down, axis, [((at + 1) % count, at) for at in range(count)])
    return low, high


def per_device(ensemble, innovation, obs_weight, lat_offset, lat_weight, band_widths):
    cols, rows = ensemble.shape[0], ensemble.shape[1]
    cells = cols * rows
    fine_cols, fine_rows = innovation.shape[0], innovation.shape[1]
    total = fine_rows + 2 * FINE_HALO
    lat_count, lon_count = lax.axis_size("lat"), lax.axis_size("lon")
    devices = lat_count * lon_count
    entries = float(cells * M * LEV * devices)
    position = lax.axis_index("lat")
    keeps = jnp.stack([position > 0, position < lat_count - 1]).astype(F32)
    flags = jnp.broadcast_to(keeps[:, None], (2, CH))

    cell_block = pltpu.VMEM((cells, CH), F32)
    pair_block = pltpu.VMEM((PAIRS, CH), F32)
    message = pltpu.VMEM((2 * (cols + 4) + (fine_cols + 2) * FINE_HALO, CH), F32)
    ens = ensemble.reshape(cells, M * CH)
    up, down, part, own, own_stencil, widths, scales = pl.pallas_call(
        prepare_kernel(cols, rows),
        out_shape=(
            message, message, pltpu.VMEM((cols + 4, rows, CH), F32),
            pltpu.VMEM((fine_cols, fine_rows, CH), F32),
            pltpu.VMEM((2 * fine_rows, CH), F32), pair_block, pair_block,
        ),
        in_specs=[VMEM_SPEC] * 5,
        out_specs=(VMEM_SPEC,) * 7,
        scratch_shapes=[
            pltpu.VMEM(((cols + 4) * 5, fine_rows + 16, CH), F32),
            pltpu.VMEM((cols + 4, fine_rows + 8, CH), F32),
        ],
        cost_estimate=pl.CostEstimate(flops=1 << 29, bytes_accessed=1 << 21, transcendentals=0),
    )(obs_weight, innovation, lat_weight[None], lat_offset[None], band_widths[None])
    low, high = from_neighbours(up, down, "lat", False)
    edge_rows = pltpu.VMEM((cols, M * CH), F32)
    ens_up, ens_down = kernel_call(
        edges_kernel(cols, rows), (edge_rows, edge_rows), (ens, own_stencil)
    )
    ens_low, ens_high = from_neighbours(ens_up, ens_down, "lat", False)
    side_block = pltpu.VMEM((2 * rows, CH), F32)
    wide_block = pltpu.VMEM((3, total, CH), F32)
    to_left, to_right, own_part, to_west, to_east, tall, stencil = kernel_call(
        join_kernel(cols, rows),
        (side_block, side_block, cell_block, wide_block, wide_block,
         pltpu.VMEM((fine_cols, total, CH), F32), pltpu.VMEM((2 * total, CH), F32)),
        (low, high, part, own, own_stencil, flags),
    )
    left, right = from_neighbours(to_right, to_left, "lon", True)
    west, east = from_neighbours(to_east, to_west, "lon", True)

    arranged = (pltpu.VMEM((PAIRS, cells, CH), F32),) * 2
    one, two = kernel_call(arrange_kernel(cells), arranged, (ens,))
    rim = (pltpu.VMEM((PAIRS, 2 * cols, CH), F32),) * 2
    rim_one, rim_two = kernel_call(arrange_kernel(2 * cols), rim, (ens_low, ens_high))

    restrict_scratch = (
        pltpu.VMEM((cols * 5, total, CH), F32),
        pltpu.VMEM((cols, 2 * rows + 8, CH), F32),
    )
    middle_scratch = (pltpu.VMEM((cols + 6, total + 16, CH), F32),) + restrict_scratch

    y0, b0 = kernel_call(
        start_kernel(cols, rows), (cell_block, cell_block),
        (own_part, left, right, one, two, widths, scales), gram_scratch(cells),
    )
    block = b0.reshape(cols, rows, CH)
    low_rows, high_rows = from_neighbours(block[:, -2:], block[:, :2], "lat", False)
    mid = jnp.concatenate([low_rows, block, high_rows], axis=1)
    mid_left, mid_right = from_neighbours(mid[-3:], mid[:3], "lon", True)
    y1, b1, mid1 = kernel_call(
        step_kernel(cols, rows), (cell_block, cell_block, pltpu.VMEM((cols, rows + 2, CH), F32)),
        (mid, mid_left, mid_right, west, tall, east, stencil, flags,
         one, two, rim_one, rim_two, widths, scales),
        middle_scratch + (pltpu.VMEM((2 * cols, CH), F32),) + gram_scratch(cells + 2 * cols),
    )
    y2, dots = kernel_call(
        last_kernel(rows, devices), (cell_block, pltpu.VMEM((devices, CH), F32)),
        (mid1, *from_neighbours(mid1[-3:], mid1[:3], "lon", True), west, tall, east, stencil, y0, b0, y1, b1),
        middle_scratch,
    )
    shared = lax.all_to_all(dots.reshape(devices, 1, CH), ("lat", "lon"), 0, 0).reshape(devices, CH)
    coefficients, vector = kernel_call(
        final_kernel(entries),
        (jax.ShapeDtypeStruct((2, 2), F32), jax.ShapeDtypeStruct((cells, M * LEV), BF16)),
        (shared, y0, y1, y2, one, two, widths, scales),
    )
    return coefficients, vector.reshape(cols, rows, M * LEV)


def solution(mesh):
    return jax.shard_map(
        per_device,
        mesh=mesh,
        in_specs=(
            P("lon", "lat", None),
            P("lon", "lat", None),
            P("lon", "lat", None),
            P("lat"),
            P("lat"),
            P(),
        ),
        out_specs=(P(), P("lon", "lat", None)),
        check_vma=False,
    )
```

```python
import jax
import jax.numpy as jnp
from jax import lax
from jax.experimental import pallas as pl
from jax.experimental.pallas import tpu as pltpu
from jax.sharding import PartitionSpec as P

M = 80
LEV = 64
FIELDS = 2

EVEN_TAPS = (-0.0234375, 0.2265625, 0.8671875, -0.0703125)
ODD_TAPS = (-0.0703125, 0.8671875, 0.2265625, -0.0234375)
EPSILON = 1e-06


F32 = jnp.float32
BF16 = jnp.bfloat16
CH = FIELDS * LEV
PAIRS = M // 2
PAD = 8
FINE_HALO = 6
VMEM_SPEC = pl.BlockSpec(memory_space=pltpu.VMEM)


def in_vmem(value):
    return pltpu.with_memory_space_constraint(value, pltpu.VMEM)


def kernel_call(body, outs, operands, scratch=()):
    return pl.pallas_call(
        body,
        out_shape=outs,
        in_specs=[VMEM_SPEC] * len(operands),
        out_specs=jax.tree.map(lambda _: VMEM_SPEC, outs),
        scratch_shapes=list(scratch),
    )(*[in_vmem(operand) for operand in operands])


def split(value):
    high = value.astype(BF16)
    return high, (value - high.astype(F32)).astype(BF16)


def pair_distances():
    row = lax.broadcasted_iota(jnp.int32, (CH, CH), 0)
    col = lax.broadcasted_iota(jnp.int32, (CH, CH), 1)
    distance = jnp.where(row // LEV == col // LEV, jnp.abs(row - col), CH)
    return distance.astype(F32).astype(BF16).reshape(CH // 16, 16, CH)


def hat(widths_ref, pair, distances):
    widths = jnp.broadcast_to(widths_ref[pair : pair + 1, :], (16, CH)).astype(BF16)
    return jnp.maximum(widths[None] - distances, jnp.zeros((), BF16)).reshape(CH, CH)


def product(value, matrix):
    cells = value.shape[0]
    parts = jnp.concatenate(split(value), axis=0)
    both = jnp.dot(parts, matrix, preferred_element_type=F32)
    return both[:cells] + both[cells:]


def swap_halves(value):
    return pltpu.roll(value, LEV, 1)


def by_field(value, low_half):
    swapped = swap_halves(value)
    return jnp.where(low_half, value, swapped), jnp.where(low_half, swapped, value)


def arrange_kernel(body_rows):
    def body(*refs):
        ens_refs, (one_ref, two_ref) = refs[:-2], refs[-2:]
        low_half = lax.broadcasted_iota(jnp.int32, (body_rows, CH), 1) < LEV
        for pair in range(PAIRS):
            both = []
            for member in (2 * pair, 2 * pair + 1):
                parts = [ref[:, member * CH : (member + 1) * CH].astype(F32) for ref in ens_refs]
                both.append(parts[0] if len(parts) == 1 else jnp.concatenate(parts, axis=0))
            first, second = both
            one_ref[pair] = jnp.where(low_half, first, swap_halves(second))
            two_ref[pair] = jnp.where(low_half, swap_halves(first), second)

    return body


def pair_members(ens_refs, pair):
    parts = [ref[pair] for ref in ens_refs]
    return parts[0] if len(parts) == 1 else jnp.concatenate(parts, axis=0)


def gram(ones, twos, widths_ref, scales_ref, coarse, once_ref, twice_ref):
    distances = pair_distances()
    cells = coarse.shape[0]
    low_half = lax.broadcasted_iota(jnp.int32, coarse.shape, 1) < LEV
    field_one, field_two = by_field(coarse, low_half)

    def put(ref, pair, value):
        ref[pair, 0:cells, :], ref[pair, cells : 2 * cells, :] = split(value)

    def apply(ref, pair):
        matrix = hat(widths_ref, pair, distances)
        both = jnp.dot(ref[pair], matrix, preferred_element_type=F32)
        return both[:cells] + both[cells:]

    for pair in range(PAIRS):
        summed = pair_members(ones, pair) * field_one + pair_members(twos, pair) * field_two
        put(once_ref, pair, summed)
    for pair in range(PAIRS):
        put(twice_ref, pair, apply(once_ref, pair))
    total_one = jnp.zeros(coarse.shape, F32)
    total_two = jnp.zeros(coarse.shape, F32)
    for pair in range(PAIRS):
        scale = scales_ref[pair : pair + 1, :]
        twice = apply(twice_ref, pair) * (scale * scale)
        total_one = total_one + pair_members(ones, pair) * twice
        total_two = total_two + pair_members(twos, pair) * twice
    return jnp.where(
        low_half, total_one + swap_halves(total_one), total_two + swap_halves(total_two)
    )


def prepare_kernel(cols, rows):
    depth = FINE_HALO
    fine_cols, fine_rows = 2 * cols, 2 * rows
    spans = rows + 4
    wide = 2 * (cols + 4)

    def body(weight_ref, innovation_ref, lat_weight_ref, lat_offset_ref, band_ref,
             up_ref, down_ref, part_ref, own_ref, own_stencil_ref, widths_ref, scales_ref,
             spill_ref, sum_ref):
        row = lax.broadcasted_iota(jnp.int32, (fine_rows, fine_rows), 0)
        col = lax.broadcasted_iota(jnp.int32, (fine_rows, fine_rows), 1)

        def column(line):
            spread = jnp.broadcast_to(line, (fine_rows, fine_rows))
            values = jnp.sum(jnp.where(row == col, spread, 0.0), axis=1, keepdims=True)
            return jnp.broadcast_to(values, (fine_rows, CH))

        upper = column(lat_weight_ref[...])
        offset = column(lat_offset_ref[...].astype(F32))
        weighted = []
        for at in range(fine_cols):
            weight = weight_ref[at]
            own_ref[at] = weight
            up_ref[wide + depth * at : wide + depth * (at + 1), :] = weight[fine_rows - depth :]
            down_ref[wide + depth * at : wide + depth * (at + 1), :] = weight[:depth]
            weighted.append(weight * innovation_ref[at])
        coefs = stencil_coefficients(upper, offset)
        blank = jnp.zeros((8, CH), F32)
        for at in range(cols + 4):
            folded = None
            for tap in range(4):
                for taps, centre in ((EVEN_TAPS, at - tap), (ODD_TAPS, at - 1 - tap)):
                    if 0 <= centre < cols:
                        term = taps[tap] * weighted[2 * centre + (taps is ODD_TAPS)]
                        folded = term if folded is None else folded + term
            total = None
            for step in range(5):
                slot = at * 5 + step
                spill_ref[slot, 0:8, :] = blank
                spill_ref[slot, 8 + fine_rows : 16 + fine_rows, :] = blank
                spill_ref[slot, 8 : 8 + fine_rows, :] = coefs[step] * folded
                term = spill_ref[slot, 8 - 2 * step : 8 - 2 * step + 2 * spans, :]
                total = term if total is None else total + term
            sum_ref[at] = total
            down_ref[2 * at : 2 * at + 2, :] = (
                sum_ref[at, pl.ds(0, 2, stride=2), :] + sum_ref[at, pl.ds(1, 2, stride=2), :]
            )
            part_ref[at] = (
                sum_ref[at, pl.ds(4, rows, stride=2), :] + sum_ref[at, pl.ds(5, rows, stride=2), :]
            )
            end = 2 * rows + 4
            up_ref[2 * at : 2 * at + 2, :] = (
                sum_ref[at, pl.ds(end, 2, stride=2), :] + sum_ref[at, pl.ds(end + 1, 2, stride=2), :]
            )
        own_stencil_ref[0:fine_rows, :] = upper
        own_stencil_ref[fine_rows : 2 * fine_rows, :] = offset
        at = wide + depth * fine_cols
        up_ref[at : at + depth, :] = upper[fine_rows - depth :]
        up_ref[at + depth : at + 2 * depth, :] = offset[fine_rows - depth :]
        down_ref[at : at + depth, :] = upper[:depth]
        down_ref[at + depth : at + 2 * depth, :] = offset[:depth]
        bands = jnp.broadcast_to((band_ref[...] + 1).astype(F32), (PAIRS, M))
        pair = lax.broadcasted_iota(jnp.int32, (PAIRS, M), 0)
        member = lax.broadcasted_iota(jnp.int32, (PAIRS, M), 1)
        first = jnp.sum(jnp.where(member == 2 * pair, bands, 0.0), axis=1, keepdims=True)
        second = jnp.sum(jnp.where(member == 2 * pair + 1, bands, 0.0), axis=1, keepdims=True)
        lane = lax.broadcasted_iota(jnp.int32, (PAIRS, CH), 1)
        widths = jnp.where(lane < LEV, first, second)
        widths_ref[...] = widths
        scales_ref[...] = 1.0 / (widths * widths)

    return body


def join_kernel(cols, rows):
    depth = FINE_HALO
    fine_cols, fine_rows = 2 * cols, 2 * rows
    wide = 2 * (cols + 4)
    total = fine_rows + 2 * depth

    def body(low_ref, high_ref, part_ref, own_ref, own_stencil_ref, flags_ref,
             left_ref, right_ref, coarse_ref, west_ref, east_ref, tall_ref, stencil_ref):
        keep_low, keep_high = flags_ref[0:1, :], flags_ref[1:2, :]
        middle_rows = jnp.zeros((rows - 4, CH), F32)
        for at in range(cols + 4):
            low = low_ref[2 * at : 2 * at + 2, :] * keep_low
            high = high_ref[2 * at : 2 * at + 2, :] * keep_high
            block = part_ref[at] + jnp.concatenate([low, middle_rows, high], axis=0)
            if at < 2:
                left_ref[at * rows : (at + 1) * rows, :] = block
            elif at < cols + 2:
                coarse_ref[(at - 2) * rows : (at - 1) * rows, :] = block
            else:
                right_ref[(at - cols - 2) * rows : (at - cols - 1) * rows, :] = block
        for col in range(fine_cols):
            edge = slice(wide + depth * col, wide + depth * (col + 1))
            pieces = (
                (0, low_ref[edge, :] * keep_low),
                (depth, own_ref[col]),
                (depth + fine_rows, high_ref[edge, :] * keep_high),
            )
            for first, piece in pieces:
                last = first + piece.shape[0]
                tall_ref[col, first:last, :] = piece
                if col < 3:
                    west_ref[col, first:last, :] = piece
                if col >= fine_cols - 3:
                    east_ref[col - fine_cols + 3, first:last, :] = piece
        for part in range(2):
            base = part * total
            at = wide + depth * (fine_cols + part)
            stencil_ref[base : base + depth, :] = low_ref[at : at + depth, :]
            stencil_ref[base + depth : base + depth + fine_rows, :] = own_stencil_ref[
                part * fine_rows : (part + 1) * fine_rows, :
            ]
            stencil_ref[base + depth + fine_rows : base + total, :] = high_ref[at : at + depth, :]

    return body


def edges_kernel(cols, rows):
    def body(ens_ref, after_ref, up_ref, down_ref):
        row = lax.broadcasted_iota(jnp.int32, (8, CH), 0)
        for member in range(M):
            lanes = slice(member * CH, (member + 1) * CH)
            block = ens_ref[:, lanes].astype(F32)
            for ref, at in ((up_ref, rows - 1), (down_ref, 0)):
                picked = jnp.zeros((8, CH), F32)
                for col in range(cols):
                    line = block[col * rows + at : col * rows + at + 1]
                    picked = jnp.where(row == col, jnp.broadcast_to(line, (8, CH)), picked)
                ref[:, lanes] = picked[:cols]

    return body


def fine_span(rows, halo):
    return FINE_HALO - 4 - 2 * halo, 2 * rows + 8 + 4 * halo


def lat_coefficients(stencil_ref, rows, halo):
    first, count = fine_span(rows, halo)
    total = 2 * rows + 2 * FINE_HALO
    return stencil_coefficients(
        stencil_ref[first : first + count, :], stencil_ref[total + first : total + first + count, :]
    )


def stencil_coefficients(weight, offset):
    result = []
    for step in range(5):
        lower = jnp.where(offset == float(step), 1.0 - weight, 0.0)
        result.append(lower + jnp.where(offset == float(step - 1), weight, 0.0))
    return result


def restrict_block(even, odd, coefs, spill_ref, sum_ref, cols, rows, halo):
    count = fine_span(rows, halo)[1]
    out = rows + 2 * halo
    for col in range(cols):
        folded = None
        for tap in range(4):
            term = EVEN_TAPS[tap] * even[col + 3 - tap] + ODD_TAPS[tap] * odd[col + 3 - tap]
            folded = term if folded is None else folded + term
        total = None
        for step in range(5):
            slot = col * 5 + step
            spill_ref[slot, 0:count, :] = coefs[step] * folded
            term = spill_ref[slot, 8 - 2 * step : 8 - 2 * step + 2 * out, :]
            total = term if total is None else total + term
        sum_ref[col, 0 : 2 * out, :] = total
    blocks = [
        sum_ref[col, pl.ds(2 * halo, rows, stride=2), :]
        + sum_ref[col, pl.ds(2 * halo + 1, rows, stride=2), :]
        for col in range(cols)
    ]
    return jnp.concatenate(blocks, axis=0)


def weight_column(weight_refs, at, first, count):
    west_ref, tall_ref, east_ref = weight_refs
    fine_cols = tall_ref.shape[0]
    if 3 <= at < fine_cols + 3:
        return tall_ref[at - 3, first : first + count, :]
    ref, col = (west_ref, at) if at < 3 else (east_ref, at - fine_cols - 3)
    return ref[col, first : first + count, :]


def middle(mid_ref, left_ref, right_ref, weight_refs, coefs, dup_ref, spill_ref, sum_ref, rows, halo, mask=None):
    cols = mid_ref.shape[0]
    first, count = fine_span(rows, halo)
    given = rows + 2 * halo + 2
    lat = []
    for col in range(cols + 6):
        if col < 3:
            block = left_ref[col]
        elif col < cols + 3:
            block = mid_ref[col - 3]
        else:
            block = right_ref[col - cols - 3]
        if mask is not None:
            block = block * mask
        dup_ref[col] = jnp.zeros(dup_ref.shape[1:], F32)
        dup_ref[col, pl.ds(PAD, given, stride=2), :] = block
        dup_ref[col, pl.ds(PAD + 1, given, stride=2), :] = block
        total = None
        for step in range(5):
            at = 2 + 2 * step
            term = coefs[step] * dup_ref[col, at : at + count, :]
            total = term if total is None else total + term
        lat.append(total)
    even, odd = [], []
    for at in range(cols + 3):
        left = sum(EVEN_TAPS[tap] * lat[at + tap] for tap in range(4))
        right = sum(ODD_TAPS[tap] * lat[at + tap] for tap in range(4))
        even.append(left * weight_column(weight_refs, 2 * at + 1, first, count))
        odd.append(right * weight_column(weight_refs, 2 * at, first, count))
    return restrict_block(even, odd, coefs, spill_ref, sum_ref, cols, rows, halo)


def start_kernel(cols, rows):
    def body(own_ref, left_ref, right_ref, one_ref, two_ref, widths_ref, scales_ref, coarse_ref, image_ref, once_ref, twice_ref):
        coarse_ref[...] = own_ref[...]
        coarse_ref[0 : 2 * rows, :] += left_ref[...]
        coarse_ref[(cols - 2) * rows : cols * rows, :] += right_ref[...]
        image_ref[...] = gram(
            (one_ref,), (two_ref,), widths_ref, scales_ref, coarse_ref[...], once_ref, twice_ref
        )

    return body


def step_kernel(cols, rows):
    cells = cols * rows

    def body(mid_ref, left_ref, right_ref, west_ref, tall_ref, east_ref, stencil_ref, flags_ref, one_ref, two_ref, rim_one_ref, rim_two_ref,
             widths_ref, scales_ref, coarse_ref, image_ref, padded_ref, dup_ref, spill_ref, sum_ref, rim_ref, once_ref, twice_ref):
        coefs = lat_coefficients(stencil_ref, rows, 1)
        row = lax.broadcasted_iota(jnp.int32, (rows + 4, CH), 0)
        inside = jnp.where(row < 2, flags_ref[0:1, :], jnp.where(row < rows + 2, 1.0, flags_ref[1:2, :]))
        coarse = middle(
            mid_ref, left_ref, right_ref, (west_ref, tall_ref, east_ref), coefs, dup_ref, spill_ref, sum_ref, rows, 1, inside
        )
        coarse_ref[...] = coarse
        end = 2 * rows + 2
        for col in range(cols):
            low = sum_ref[col, 0:1, :] + sum_ref[col, 1:2, :]
            high = sum_ref[col, end : end + 1, :] + sum_ref[col, end + 1 : end + 2, :]
            rim_ref[col : col + 1, :] = low * flags_ref[0:1, :]
            rim_ref[cols + col : cols + col + 1, :] = high * flags_ref[1:2, :]
        image = gram(
            (one_ref, rim_one_ref), (two_ref, rim_two_ref), widths_ref, scales_ref,
            jnp.concatenate([coarse, rim_ref[...]], axis=0), once_ref, twice_ref,
        )
        image_ref[...] = image[:cells]
        for col in range(cols):
            padded_ref[col, 0:1, :] = image[cells + col : cells + col + 1]
            padded_ref[col, 1 : rows + 1, :] = image[col * rows : (col + 1) * rows]
            padded_ref[col, rows + 1 : rows + 2, :] = image[
                cells + cols + col : cells + cols + col + 1
            ]

    return body


def last_kernel(rows, devices):
    def body(mid_ref, left_ref, right_ref, west_ref, tall_ref, east_ref, stencil_ref, y0_ref, b0_ref, y1_ref, b1_ref,
             coarse_ref, dots_ref, dup_ref, spill_ref, sum_ref):
        coefs = lat_coefficients(stencil_ref, rows, 0)
        coarse = middle(
            mid_ref, left_ref, right_ref, (west_ref, tall_ref, east_ref), coefs, dup_ref, spill_ref, sum_ref, rows, 0
        )
        coarse_ref[...] = coarse
        lane = lax.broadcasted_iota(jnp.int32, (1, CH), 1)
        row = jnp.zeros((1, CH), F32)
        b0, b1, y1 = b0_ref[...], b1_ref[...], y1_ref[...]
        pairs = (y0_ref[...] * b0, y1 * b0, y1 * b1, coarse * b1)
        for place, terms in enumerate(pairs):
            total = jnp.sum(jnp.sum(terms, axis=0, keepdims=True), axis=1, keepdims=True)
            row = jnp.where(lane == place, total, row)
        dots_ref[...] = jnp.broadcast_to(row, (devices, CH))

    return body


def final_kernel(entries):
    def body(dots_ref, y0_ref, y1_ref, y2_ref, one_ref, two_ref, widths_ref, scales_ref, coef_ref, vector_ref):
        sums = jnp.sum(dots_ref[...], axis=0, keepdims=True)
        lane = lax.broadcasted_iota(jnp.int32, (1, CH), 1)

        def pick(place):
            return jnp.sum(jnp.where(lane == place, sums, 0.0), axis=1, keepdims=True)

        m00, m01, m11, m12 = (pick(place) for place in range(4))
        square0 = m00 / entries + EPSILON
        inverse0 = 1.0 / square0
        alpha0 = ((m00 + m01) / entries) * inverse0
        shift = entries * EPSILON
        g = ((shift - m01) / entries) * inverse0
        u1u1 = (g * (g * m00 + 2.0 * m01) + m11) * inverse0
        u1lu1 = (g * (g * m01 + 2.0 * m11) + m12) * inverse0
        cross = ((g * (m00 + m01) + m01 + m11) / entries) * inverse0
        square1 = u1u1 / entries + EPSILON
        inverse1 = 1.0 / square1
        alpha1 = ((u1u1 + u1lu1) / entries) * inverse1
        h = ((shift - u1lu1) / entries) * inverse1
        beta0, beta1 = jnp.sqrt(square0), jnp.sqrt(square1)
        k2 = lax.rsqrt(square0) * lax.rsqrt(square1)
        k1 = k2 * (h + g)
        k0 = k2 * (h * g - cross)
        row = lax.broadcasted_iota(jnp.int32, (2, 2), 0)
        col = lax.broadcasted_iota(jnp.int32, (2, 2), 1)
        coef_ref[...] = jnp.where(
            row == 0, jnp.where(col == 0, alpha0, alpha1), jnp.where(col == 0, beta0, beta1)
        )
        coarse = k0 * y0_ref[...] + k1 * y1_ref[...] + k2 * y2_ref[...]
        distances = pair_distances()
        low_half = lax.broadcasted_iota(jnp.int32, coarse.shape, 1) < LEV
        field_one, field_two = by_field(coarse, low_half)
        for pair in range(PAIRS):
            matrix = hat(widths_ref, pair, distances)
            summed = one_ref[pair] * field_one + two_ref[pair] * field_two
            out = product(summed, matrix) * scales_ref[pair : pair + 1, :]
            vector_ref[:, pair * CH : (pair + 1) * CH] = out.astype(BF16)

    return body


def gram_scratch(cells):
    return (pltpu.VMEM((PAIRS, 2 * cells, CH), BF16),) * 2


def from_neighbours(up, down, axis, paired):
    count = lax.axis_size(axis)
    if paired and count % 2 == 0:
        odd = lax.axis_index(axis) % 2 == 1
        outer = [(at, (at + 1) % count if at % 2 else (at - 1) % count) for at in range(count)]
        inner = [(at, at + 1 - 2 * (at % 2)) for at in range(count)]
        far = lax.ppermute(jnp.where(odd, up, down), axis, outer)
        near = lax.ppermute(jnp.where(odd, down, up), axis, inner)
        return jnp.where(odd, near, far), jnp.where(odd, far, near)
    low = lax.ppermute(up, axis, [(at, (at + 1) % count) for at in range(count)])
    high = lax.ppermute(down, axis, [((at + 1) % count, at) for at in range(count)])
    return low, high


def per_device(ensemble, innovation, obs_weight, lat_offset, lat_weight, band_widths):
    cols, rows = ensemble.shape[0], ensemble.shape[1]
    cells = cols * rows
    fine_cols, fine_rows = innovation.shape[0], innovation.shape[1]
    total = fine_rows + 2 * FINE_HALO
    lat_count, lon_count = lax.axis_size("lat"), lax.axis_size("lon")
    devices = lat_count * lon_count
    entries = float(cells * M * LEV * devices)
    position = lax.axis_index("lat")
    keeps = jnp.stack([position > 0, position < lat_count - 1]).astype(F32)
    flags = jnp.broadcast_to(keeps[:, None], (2, CH))

    cell_block = pltpu.VMEM((cells, CH), F32)
    pair_block = pltpu.VMEM((PAIRS, CH), F32)
    message = pltpu.VMEM((2 * (cols + 4) + (fine_cols + 2) * FINE_HALO, CH), F32)
    ens = ensemble.reshape(cells, M * CH)
    up, down, part, own, own_stencil, widths, scales = pl.pallas_call(
        prepare_kernel(cols, rows),
        out_shape=(
            message, message, pltpu.VMEM((cols + 4, rows, CH), F32),
            pltpu.VMEM((fine_cols, fine_rows, CH), F32),
            pltpu.VMEM((2 * fine_rows, CH), F32), pair_block, pair_block,
        ),
        in_specs=[VMEM_SPEC] * 5,
        out_specs=(VMEM_SPEC,) * 7,
        scratch_shapes=[
            pltpu.VMEM(((cols + 4) * 5, fine_rows + 16, CH), F32),
            pltpu.VMEM((cols + 4, fine_rows + 8, CH), F32),
        ],
        cost_estimate=pl.CostEstimate(flops=1 << 29, bytes_accessed=1 << 21, transcendentals=0),
    )(obs_weight, innovation, lat_weight[None], lat_offset[None], band_widths[None])
    low, high = from_neighbours(up, down, "lat", False)
    edge_rows = pltpu.VMEM((cols, M * CH), F32)
    ens_up, ens_down = kernel_call(
        edges_kernel(cols, rows), (edge_rows, edge_rows), (ens, own_stencil)
    )
    ens_low, ens_high = from_neighbours(ens_up, ens_down, "lat", False)
    side_block = pltpu.VMEM((2 * rows, CH), F32)
    wide_block = pltpu.VMEM((3, total, CH), F32)
    to_left, to_right, own_part, to_west, to_east, tall, stencil = kernel_call(
        join_kernel(cols, rows),
        (side_block, side_block, cell_block, wide_block, wide_block,
         pltpu.VMEM((fine_cols, total, CH), F32), pltpu.VMEM((2 * total, CH), F32)),
        (low, high, part, own, own_stencil, flags),
    )
    left, right = from_neighbours(to_right, to_left, "lon", True)
    west, east = from_neighbours(to_east, to_west, "lon", True)

    arranged = (pltpu.VMEM((PAIRS, cells, CH), F32),) * 2
    one, two = kernel_call(arrange_kernel(cells), arranged, (ens,))
    rim = (pltpu.VMEM((PAIRS, 2 * cols, CH), F32),) * 2
    rim_one, rim_two = kernel_call(arrange_kernel(2 * cols), rim, (ens_low, ens_high))

    restrict_scratch = (
        pltpu.VMEM((cols * 5, total, CH), F32),
        pltpu.VMEM((cols, 2 * rows + 8, CH), F32),
    )
    middle_scratch = (pltpu.VMEM((cols + 6, total + 16, CH), F32),) + restrict_scratch

    y0, b0 = kernel_call(
        start_kernel(cols, rows), (cell_block, cell_block),
        (own_part, left, right, one, two, widths, scales), gram_scratch(cells),
    )
    block = b0.reshape(cols, rows, CH)
    low_rows, high_rows = from_neighbours(block[:, -2:], block[:, :2], "lat", False)
    mid = jnp.concatenate([low_rows, block, high_rows], axis=1)
    mid_left, mid_right = from_neighbours(mid[-3:], mid[:3], "lon", True)
    y1, b1, mid1 = kernel_call(
        step_kernel(cols, rows), (cell_block, cell_block, pltpu.VMEM((cols, rows + 2, CH), F32)),
        (mid, mid_left, mid_right, west, tall, east, stencil, flags,
         one, two, rim_one, rim_two, widths, scales),
        middle_scratch + (pltpu.VMEM((2 * cols, CH), F32),) + gram_scratch(cells + 2 * cols),
    )
    y2, dots = kernel_call(
        last_kernel(rows, devices), (cell_block, pltpu.VMEM((devices, CH), F32)),
        (mid1, *from_neighbours(mid1[-3:], mid1[:3], "lon", True), west, tall, east, stencil, y0, b0, y1, b1),
        middle_scratch,
    )
    shared = lax.all_to_all(dots.reshape(devices, 1, CH), ("lat", "lon"), 0, 0).reshape(devices, CH)
    coefficients, vector = kernel_call(
        final_kernel(entries),
        (jax.ShapeDtypeStruct((2, 2), F32), jax.ShapeDtypeStruct((cells, M * LEV), BF16)),
        (shared, y0, y1, y2, one, two, widths, scales),
    )
    return coefficients, vector.reshape(cols, rows, M * LEV)


def solution(mesh):
    return jax.shard_map(
        per_device,
        mesh=mesh,
        in_specs=(
            P("lon", "lat", None),
            P("lon", "lat", None),
            P("lon", "lat", None),
            P("lat"),
            P("lat"),
            P(),
        ),
        out_specs=(P(), P("lon", "lat", None)),
        check_vma=False,
    )
```

```python
import jax
import jax.numpy as jnp
from jax import lax
from jax.experimental import pallas as pl
from jax.experimental.pallas import tpu as pltpu
from jax.sharding import PartitionSpec as P

M = 80
LEV = 64
FIELDS = 2

EVEN_TAPS = (-0.0234375, 0.2265625, 0.8671875, -0.0703125)
ODD_TAPS = (-0.0703125, 0.8671875, 0.2265625, -0.0234375)
EPSILON = 1e-06


F32 = jnp.float32
BF16 = jnp.bfloat16
CH = FIELDS * LEV
PAIRS = M // 2
PAD = 8
FINE_HALO = 6
VMEM_SPEC = pl.BlockSpec(memory_space=pltpu.VMEM)


def in_vmem(value):
    return pltpu.with_memory_space_constraint(value, pltpu.VMEM)


def kernel_call(body, outs, operands, scratch=()):
    return pl.pallas_call(
        body,
        out_shape=outs,
        in_specs=[VMEM_SPEC] * len(operands),
        out_specs=jax.tree.map(lambda _: VMEM_SPEC, outs),
        scratch_shapes=list(scratch),
    )(*[in_vmem(operand) for operand in operands])


def split(value):
    high = value.astype(BF16)
    return high, (value - high.astype(F32)).astype(BF16)


def pair_distances():
    row = lax.broadcasted_iota(jnp.int32, (CH, CH), 0)
    col = lax.broadcasted_iota(jnp.int32, (CH, CH), 1)
    distance = jnp.where(row // LEV == col // LEV, jnp.abs(row - col), CH)
    return distance.astype(F32).astype(BF16).reshape(CH // 16, 16, CH)


def hat(widths_ref, pair, distances):
    widths = jnp.broadcast_to(widths_ref[pair : pair + 1, :], (16, CH)).astype(BF16)
    return jnp.maximum(widths[None] - distances, jnp.zeros((), BF16)).reshape(CH, CH)


def swap_halves(value):
    return pltpu.roll(value, LEV, 1)


def by_field(value, low_half):
    swapped = swap_halves(value)
    return jnp.where(low_half, value, swapped), jnp.where(low_half, swapped, value)


def arrange_kernel(body_rows):
    def body(*refs):
        ens_refs, (one_ref, two_ref) = refs[:-2], refs[-2:]
        low_half = lax.broadcasted_iota(jnp.int32, (body_rows, CH), 1) < LEV
        for pair in range(PAIRS):
            both = []
            for member in (2 * pair, 2 * pair + 1):
                parts = [ref[:, member * CH : (member + 1) * CH].astype(F32) for ref in ens_refs]
                both.append(parts[0] if len(parts) == 1 else jnp.concatenate(parts, axis=0))
            first, second = both
            one_ref[pair] = jnp.where(low_half, first, swap_halves(second))
            two_ref[pair] = jnp.where(low_half, swap_halves(first), second)

    return body


def pair_members(ens_refs, pair):
    parts = [ref[pair] for ref in ens_refs]
    return parts[0] if len(parts) == 1 else jnp.concatenate(parts, axis=0)


def gram(ones, twos, widths_ref, scales_ref, coarse, once_ref, twice_ref):
    distances = pair_distances()
    cells = coarse.shape[0]
    low_half = lax.broadcasted_iota(jnp.int32, coarse.shape, 1) < LEV
    field_one, field_two = by_field(coarse, low_half)

    def put(ref, pair, value):
        ref[pair, 0:cells, :], ref[pair, cells : 2 * cells, :] = split(value)

    def apply(ref, pair):
        matrix = hat(widths_ref, pair, distances)
        both = jnp.dot(ref[pair], matrix, preferred_element_type=F32)
        return both[:cells] + both[cells:]

    for pair in range(PAIRS):
        summed = pair_members(ones, pair) * field_one + pair_members(twos, pair) * field_two
        put(once_ref, pair, summed)
    for pair in range(PAIRS):
        put(twice_ref, pair, apply(once_ref, pair))
    total_one = jnp.zeros(coarse.shape, F32)
    total_two = jnp.zeros(coarse.shape, F32)
    for pair in range(PAIRS):
        scale = scales_ref[pair : pair + 1, :]
        twice = apply(twice_ref, pair) * (scale * scale)
        total_one = total_one + pair_members(ones, pair) * twice
        total_two = total_two + pair_members(twos, pair) * twice
    return jnp.where(
        low_half, total_one + swap_halves(total_one), total_two + swap_halves(total_two)
    )


def prepare_kernel(cols, rows):
    depth = FINE_HALO
    fine_cols, fine_rows = 2 * cols, 2 * rows
    spans = rows + 4
    wide = 2 * (cols + 4)

    def body(weight_ref, innovation_ref, lat_weight_ref, lat_offset_ref, band_ref,
             up_ref, down_ref, part_ref, own_ref, own_stencil_ref, widths_ref, scales_ref,
             spill_ref, sum_ref):
        row = lax.broadcasted_iota(jnp.int32, (fine_rows, fine_rows), 0)
        col = lax.broadcasted_iota(jnp.int32, (fine_rows, fine_rows), 1)

        def column(line):
            spread = jnp.broadcast_to(line, (fine_rows, fine_rows))
            values = jnp.sum(jnp.where(row == col, spread, 0.0), axis=1, keepdims=True)
            return jnp.broadcast_to(values, (fine_rows, CH))

        upper = column(lat_weight_ref[...])
        offset = column(lat_offset_ref[...].astype(F32))
        weighted = []
        for at in range(fine_cols):
            weight = weight_ref[at]
            own_ref[at] = weight
            up_ref[wide + depth * at : wide + depth * (at + 1), :] = weight[fine_rows - depth :]
            down_ref[wide + depth * at : wide + depth * (at + 1), :] = weight[:depth]
            weighted.append(weight * innovation_ref[at])
        coefs = stencil_coefficients(upper, offset)
        blank = jnp.zeros((8, CH), F32)
        for at in range(cols + 4):
            folded = None
            for tap in range(4):
                for taps, centre in ((EVEN_TAPS, at - tap), (ODD_TAPS, at - 1 - tap)):
                    if 0 <= centre < cols:
                        term = taps[tap] * weighted[2 * centre + (taps is ODD_TAPS)]
                        folded = term if folded is None else folded + term
            total = None
            for step in range(5):
                slot = at * 5 + step
                spill_ref[slot, 0:8, :] = blank
                spill_ref[slot, 8 + fine_rows : 16 + fine_rows, :] = blank
                spill_ref[slot, 8 : 8 + fine_rows, :] = coefs[step] * folded
                term = spill_ref[slot, 8 - 2 * step : 8 - 2 * step + 2 * spans, :]
                total = term if total is None else total + term
            sum_ref[at] = total
            down_ref[2 * at : 2 * at + 2, :] = (
                sum_ref[at, pl.ds(0, 2, stride=2), :] + sum_ref[at, pl.ds(1, 2, stride=2), :]
            )
            part_ref[at] = (
                sum_ref[at, pl.ds(4, rows, stride=2), :] + sum_ref[at, pl.ds(5, rows, stride=2), :]
            )
            end = 2 * rows + 4
            up_ref[2 * at : 2 * at + 2, :] = (
                sum_ref[at, pl.ds(end, 2, stride=2), :] + sum_ref[at, pl.ds(end + 1, 2, stride=2), :]
            )
        own_stencil_ref[0:fine_rows, :] = upper
        own_stencil_ref[fine_rows : 2 * fine_rows, :] = offset
        at = wide + depth * fine_cols
        up_ref[at : at + depth, :] = upper[fine_rows - depth :]
        up_ref[at + depth : at + 2 * depth, :] = offset[fine_rows - depth :]
        down_ref[at : at + depth, :] = upper[:depth]
        down_ref[at + depth : at + 2 * depth, :] = offset[:depth]
        bands = jnp.broadcast_to((band_ref[...] + 1).astype(F32), (PAIRS, M))
        pair = lax.broadcasted_iota(jnp.int32, (PAIRS, M), 0)
        member = lax.broadcasted_iota(jnp.int32, (PAIRS, M), 1)
        first = jnp.sum(jnp.where(member == 2 * pair, bands, 0.0), axis=1, keepdims=True)
        second = jnp.sum(jnp.where(member == 2 * pair + 1, bands, 0.0), axis=1, keepdims=True)
        lane = lax.broadcasted_iota(jnp.int32, (PAIRS, CH), 1)
        widths = jnp.where(lane < LEV, first, second)
        widths_ref[...] = widths
        scales_ref[...] = 1.0 / (widths * widths)

    return body


def join_kernel(cols, rows):
    depth = FINE_HALO
    fine_cols, fine_rows = 2 * cols, 2 * rows
    wide = 2 * (cols + 4)
    total = fine_rows + 2 * depth

    def body(low_ref, high_ref, part_ref, own_ref, own_stencil_ref, flags_ref,
             left_ref, right_ref, coarse_ref, west_ref, east_ref, tall_ref, stencil_ref):
        keep_low, keep_high = flags_ref[0:1, :], flags_ref[1:2, :]
        middle_rows = jnp.zeros((rows - 4, CH), F32)
        for at in range(cols + 4):
            low = low_ref[2 * at : 2 * at + 2, :] * keep_low
            high = high_ref[2 * at : 2 * at + 2, :] * keep_high
            block = part_ref[at] + jnp.concatenate([low, middle_rows, high], axis=0)
            if at < 2:
                left_ref[at * rows : (at + 1) * rows, :] = block
            elif at < cols + 2:
                coarse_ref[(at - 2) * rows : (at - 1) * rows, :] = block
            else:
                right_ref[(at - cols - 2) * rows : (at - cols - 1) * rows, :] = block
        for col in range(fine_cols):
            edge = slice(wide + depth * col, wide + depth * (col + 1))
            pieces = (
                (0, low_ref[edge, :] * keep_low),
                (depth, own_ref[col]),
                (depth + fine_rows, high_ref[edge, :] * keep_high),
            )
            for first, piece in pieces:
                last = first + piece.shape[0]
                tall_ref[col, first:last, :] = piece
                if col < 3:
                    west_ref[col, first:last, :] = piece
                if col >= fine_cols - 3:
                    east_ref[col - fine_cols + 3, first:last, :] = piece
        for part in range(2):
            base = part * total
            at = wide + depth * (fine_cols + part)
            stencil_ref[base : base + depth, :] = low_ref[at : at + depth, :]
            stencil_ref[base + depth : base + depth + fine_rows, :] = own_stencil_ref[
                part * fine_rows : (part + 1) * fine_rows, :
            ]
            stencil_ref[base + depth + fine_rows : base + total, :] = high_ref[at : at + depth, :]

    return body


def edges_kernel(cols, rows):
    def body(ens_ref, after_ref, up_ref, down_ref):
        row = lax.broadcasted_iota(jnp.int32, (8, CH), 0)
        for member in range(M):
            lanes = slice(member * CH, (member + 1) * CH)
            block = ens_ref[:, lanes].astype(F32)
            for ref, at in ((up_ref, rows - 1), (down_ref, 0)):
                picked = jnp.zeros((8, CH), F32)
                for col in range(cols):
                    line = block[col * rows + at : col * rows + at + 1]
                    picked = jnp.where(row == col, jnp.broadcast_to(line, (8, CH)), picked)
                ref[:, lanes] = picked[:cols]

    return body


def fine_span(rows, halo):
    return FINE_HALO - 4 - 2 * halo, 2 * rows + 8 + 4 * halo


def lat_coefficients(stencil_ref, rows, halo):
    first, count = fine_span(rows, halo)
    total = 2 * rows + 2 * FINE_HALO
    return stencil_coefficients(
        stencil_ref[first : first + count, :], stencil_ref[total + first : total + first + count, :]
    )


def stencil_coefficients(weight, offset):
    result = []
    for step in range(5):
        lower = jnp.where(offset == float(step), 1.0 - weight, 0.0)
        result.append(lower + jnp.where(offset == float(step - 1), weight, 0.0))
    return result


def restrict_block(even, odd, coefs, spill_ref, sum_ref, cols, rows, halo):
    count = fine_span(rows, halo)[1]
    out = rows + 2 * halo
    for col in range(cols):
        folded = None
        for tap in range(4):
            term = EVEN_TAPS[tap] * even[col + 3 - tap] + ODD_TAPS[tap] * odd[col + 3 - tap]
            folded = term if folded is None else folded + term
        total = None
        for step in range(5):
            slot = col * 5 + step
            spill_ref[slot, 0:count, :] = coefs[step] * folded
            term = spill_ref[slot, 8 - 2 * step : 8 - 2 * step + 2 * out, :]
            total = term if total is None else total + term
        sum_ref[col, 0 : 2 * out, :] = total
    blocks = [
        sum_ref[col, pl.ds(2 * halo, rows, stride=2), :]
        + sum_ref[col, pl.ds(2 * halo + 1, rows, stride=2), :]
        for col in range(cols)
    ]
    return jnp.concatenate(blocks, axis=0)


def weight_column(weight_refs, at, first, count):
    west_ref, tall_ref, east_ref = weight_refs
    fine_cols = tall_ref.shape[0]
    if 3 <= at < fine_cols + 3:
        return tall_ref[at - 3, first : first + count, :]
    ref, col = (west_ref, at) if at < 3 else (east_ref, at - fine_cols - 3)
    return ref[col, first : first + count, :]


def middle(mid_ref, left_ref, right_ref, weight_refs, coefs, dup_ref, spill_ref, sum_ref, rows, halo, mask=None):
    cols = mid_ref.shape[0]
    first, count = fine_span(rows, halo)
    given = rows + 2 * halo + 2
    lat = []
    for col in range(cols + 6):
        if col < 3:
            block = left_ref[col]
        elif col < cols + 3:
            block = mid_ref[col - 3]
        else:
            block = right_ref[col - cols - 3]
        if mask is not None:
            block = block * mask
        dup_ref[col] = jnp.zeros(dup_ref.shape[1:], F32)
        dup_ref[col, pl.ds(PAD, given, stride=2), :] = block
        dup_ref[col, pl.ds(PAD + 1, given, stride=2), :] = block
        total = None
        for step in range(5):
            at = 2 + 2 * step
            term = coefs[step] * dup_ref[col, at : at + count, :]
            total = term if total is None else total + term
        lat.append(total)
    even, odd = [], []
    for at in range(cols + 3):
        left = sum(EVEN_TAPS[tap] * lat[at + tap] for tap in range(4))
        right = sum(ODD_TAPS[tap] * lat[at + tap] for tap in range(4))
        even.append(left * weight_column(weight_refs, 2 * at + 1, first, count))
        odd.append(right * weight_column(weight_refs, 2 * at, first, count))
    return restrict_block(even, odd, coefs, spill_ref, sum_ref, cols, rows, halo)


def start_kernel(cols, rows):
    def body(own_ref, left_ref, right_ref, one_ref, two_ref, widths_ref, scales_ref, coarse_ref, image_ref, once_ref, twice_ref):
        coarse_ref[...] = own_ref[...]
        coarse_ref[0 : 2 * rows, :] += left_ref[...]
        coarse_ref[(cols - 2) * rows : cols * rows, :] += right_ref[...]
        image_ref[...] = gram(
            (one_ref,), (two_ref,), widths_ref, scales_ref, coarse_ref[...], once_ref, twice_ref
        )

    return body


def step_kernel(cols, rows):
    cells = cols * rows

    def body(mid_ref, left_ref, right_ref, west_ref, tall_ref, east_ref, stencil_ref, flags_ref, one_ref, two_ref, rim_one_ref, rim_two_ref,
             widths_ref, scales_ref, coarse_ref, image_ref, padded_ref, dup_ref, spill_ref, sum_ref, rim_ref, once_ref, twice_ref):
        coefs = lat_coefficients(stencil_ref, rows, 1)
        row = lax.broadcasted_iota(jnp.int32, (rows + 4, CH), 0)
        inside = jnp.where(row < 2, flags_ref[0:1, :], jnp.where(row < rows + 2, 1.0, flags_ref[1:2, :]))
        coarse = middle(
            mid_ref, left_ref, right_ref, (west_ref, tall_ref, east_ref), coefs, dup_ref, spill_ref, sum_ref, rows, 1, inside
        )
        coarse_ref[...] = coarse
        end = 2 * rows + 2
        for col in range(cols):
            low = sum_ref[col, 0:1, :] + sum_ref[col, 1:2, :]
            high = sum_ref[col, end : end + 1, :] + sum_ref[col, end + 1 : end + 2, :]
            rim_ref[col : col + 1, :] = low * flags_ref[0:1, :]
            rim_ref[cols + col : cols + col + 1, :] = high * flags_ref[1:2, :]
        image = gram(
            (one_ref, rim_one_ref), (two_ref, rim_two_ref), widths_ref, scales_ref,
            jnp.concatenate([coarse, rim_ref[...]], axis=0), once_ref, twice_ref,
        )
        image_ref[...] = image[:cells]
        for col in range(cols):
            padded_ref[col, 0:1, :] = image[cells + col : cells + col + 1]
            padded_ref[col, 1 : rows + 1, :] = image[col * rows : (col + 1) * rows]
            padded_ref[col, rows + 1 : rows + 2, :] = image[
                cells + cols + col : cells + cols + col + 1
            ]

    return body


def last_kernel(rows, devices):
    def body(mid_ref, left_ref, right_ref, west_ref, tall_ref, east_ref, stencil_ref, y0_ref, b0_ref, y1_ref, b1_ref,
             coarse_ref, dots_ref, dup_ref, spill_ref, sum_ref):
        coefs = lat_coefficients(stencil_ref, rows, 0)
        coarse = middle(
            mid_ref, left_ref, right_ref, (west_ref, tall_ref, east_ref), coefs, dup_ref, spill_ref, sum_ref, rows, 0
        )
        coarse_ref[...] = coarse
        lane = lax.broadcasted_iota(jnp.int32, (1, CH), 1)
        row = jnp.zeros((1, CH), F32)
        b0, b1, y1 = b0_ref[...], b1_ref[...], y1_ref[...]
        pairs = (y0_ref[...] * b0, y1 * b0, y1 * b1, coarse * b1)
        for place, terms in enumerate(pairs):
            total = jnp.sum(jnp.sum(terms, axis=0, keepdims=True), axis=1, keepdims=True)
            row = jnp.where(lane == place, total, row)
        dots_ref[...] = jnp.broadcast_to(row, (devices, CH))

    return body


def final_kernel(entries):
    def body(dots_ref, y0_ref, y1_ref, y2_ref, one_ref, two_ref, widths_ref, scales_ref, coef_ref, vector_ref, once_ref):
        sums = jnp.sum(dots_ref[...], axis=0, keepdims=True)
        lane = lax.broadcasted_iota(jnp.int32, (1, CH), 1)

        def pick(place):
            return jnp.sum(jnp.where(lane == place, sums, 0.0), axis=1, keepdims=True)

        m00, m01, m11, m12 = (pick(place) for place in range(4))
        square0 = m00 / entries + EPSILON
        inverse0 = 1.0 / square0
        alpha0 = ((m00 + m01) / entries) * inverse0
        g = 1.0 - alpha0
        u1u1 = (g * (g * m00 + 2.0 * m01) + m11) * inverse0
        u1lu1 = (g * (g * m01 + 2.0 * m11) + m12) * inverse0
        cross = ((g * (m00 + m01) + m01 + m11) / entries) * inverse0
        square1 = u1u1 / entries + EPSILON
        alpha1 = ((u1u1 + u1lu1) / entries) / square1
        beta0, beta1 = jnp.sqrt(square0), jnp.sqrt(square1)
        k2 = lax.rsqrt(square0) * lax.rsqrt(square1)
        k1 = k2 * (1.0 - alpha1 + g)
        k0 = k2 * ((1.0 - alpha1) * g - cross)
        row = lax.broadcasted_iota(jnp.int32, (2, 2), 0)
        col = lax.broadcasted_iota(jnp.int32, (2, 2), 1)
        coef_ref[...] = jnp.where(
            row == 0, jnp.where(col == 0, alpha0, alpha1), jnp.where(col == 0, beta0, beta1)
        )
        coarse = k0 * y0_ref[...] + k1 * y1_ref[...] + k2 * y2_ref[...]
        distances = pair_distances()
        low_half = lax.broadcasted_iota(jnp.int32, coarse.shape, 1) < LEV
        field_one, field_two = by_field(coarse, low_half)
        cells = coarse.shape[0]
        for pair in range(PAIRS):
            summed = one_ref[pair] * field_one + two_ref[pair] * field_two
            once_ref[pair, 0:cells, :], once_ref[pair, cells : 2 * cells, :] = split(summed)
        for pair in range(PAIRS):
            matrix = hat(widths_ref, pair, distances)
            both = jnp.dot(once_ref[pair], matrix, preferred_element_type=F32)
            out = (both[:cells] + both[cells:]) * scales_ref[pair : pair + 1, :]
            vector_ref[:, pair * CH : (pair + 1) * CH] = out.astype(BF16)

    return body


def gram_scratch(cells):
    return (pltpu.VMEM((PAIRS, 2 * cells, CH), BF16),) * 2


def from_neighbours(up, down, axis, paired):
    count = lax.axis_size(axis)
    if paired and count % 2 == 0:
        odd = lax.axis_index(axis) % 2 == 1
        outer = [(at, (at + 1) % count if at % 2 else (at - 1) % count) for at in range(count)]
        inner = [(at, at + 1 - 2 * (at % 2)) for at in range(count)]
        far = lax.ppermute(jnp.where(odd, up, down), axis, outer)
        near = lax.ppermute(jnp.where(odd, down, up), axis, inner)
        return jnp.where(odd, near, far), jnp.where(odd, far, near)
    low = lax.ppermute(up, axis, [(at, (at + 1) % count) for at in range(count)])
    high = lax.ppermute(down, axis, [((at + 1) % count, at) for at in range(count)])
    return low, high


def per_device(ensemble, innovation, obs_weight, lat_offset, lat_weight, band_widths):
    cols, rows = ensemble.shape[0], ensemble.shape[1]
    cells = cols * rows
    fine_cols, fine_rows = innovation.shape[0], innovation.shape[1]
    total = fine_rows + 2 * FINE_HALO
    lat_count, lon_count = lax.axis_size("lat"), lax.axis_size("lon")
    devices = lat_count * lon_count
    entries = float(cells * M * LEV * devices)
    position = lax.axis_index("lat")
    keeps = jnp.stack([position > 0, position < lat_count - 1]).astype(F32)
    flags = jnp.broadcast_to(keeps[:, None], (2, CH))

    cell_block = pltpu.VMEM((cells, CH), F32)
    pair_block = pltpu.VMEM((PAIRS, CH), F32)
    message = pltpu.VMEM((2 * (cols + 4) + (fine_cols + 2) * FINE_HALO, CH), F32)
    ens = ensemble.reshape(cells, M * CH)
    up, down, part, own, own_stencil, widths, scales = pl.pallas_call(
        prepare_kernel(cols, rows),
        out_shape=(
            message, message, pltpu.VMEM((cols + 4, rows, CH), F32),
            pltpu.VMEM((fine_cols, fine_rows, CH), F32),
            pltpu.VMEM((2 * fine_rows, CH), F32), pair_block, pair_block,
        ),
        in_specs=[VMEM_SPEC] * 5,
        out_specs=(VMEM_SPEC,) * 7,
        scratch_shapes=[
            pltpu.VMEM(((cols + 4) * 5, fine_rows + 16, CH), F32),
            pltpu.VMEM((cols + 4, fine_rows + 8, CH), F32),
        ],
        cost_estimate=pl.CostEstimate(flops=1 << 29, bytes_accessed=1 << 21, transcendentals=0),
    )(obs_weight, innovation, lat_weight[None], lat_offset[None], band_widths[None])
    low, high = from_neighbours(up, down, "lat", False)
    edge_rows = pltpu.VMEM((cols, M * CH), F32)
    ens_up, ens_down = kernel_call(
        edges_kernel(cols, rows), (edge_rows, edge_rows), (ens, own_stencil)
    )
    ens_low, ens_high = from_neighbours(ens_up, ens_down, "lat", False)
    side_block = pltpu.VMEM((2 * rows, CH), F32)
    wide_block = pltpu.VMEM((3, total, CH), F32)
    to_left, to_right, own_part, to_west, to_east, tall, stencil = kernel_call(
        join_kernel(cols, rows),
        (side_block, side_block, cell_block, wide_block, wide_block,
         pltpu.VMEM((fine_cols, total, CH), F32), pltpu.VMEM((2 * total, CH), F32)),
        (low, high, part, own, own_stencil, flags),
    )
    left, right = from_neighbours(to_right, to_left, "lon", True)
    west, east = from_neighbours(to_east, to_west, "lon", True)

    arranged = (pltpu.VMEM((PAIRS, cells, CH), F32),) * 2
    one, two = kernel_call(arrange_kernel(cells), arranged, (ens,))
    rim = (pltpu.VMEM((PAIRS, 2 * cols, CH), F32),) * 2
    rim_one, rim_two = kernel_call(arrange_kernel(2 * cols), rim, (ens_low, ens_high))

    restrict_scratch = (
        pltpu.VMEM((cols * 5, total, CH), F32),
        pltpu.VMEM((cols, 2 * rows + 8, CH), F32),
    )
    middle_scratch = (pltpu.VMEM((cols + 6, total + 16, CH), F32),) + restrict_scratch

    y0, b0 = kernel_call(
        start_kernel(cols, rows), (cell_block, cell_block),
        (own_part, left, right, one, two, widths, scales), gram_scratch(cells),
    )
    block = b0.reshape(cols, rows, CH)
    low_rows, high_rows = from_neighbours(block[:, -2:], block[:, :2], "lat", False)
    mid = jnp.concatenate([low_rows, block, high_rows], axis=1)
    mid_left, mid_right = from_neighbours(mid[-3:], mid[:3], "lon", True)
    y1, b1, mid1 = kernel_call(
        step_kernel(cols, rows), (cell_block, cell_block, pltpu.VMEM((cols, rows + 2, CH), F32)),
        (mid, mid_left, mid_right, west, tall, east, stencil, flags,
         one, two, rim_one, rim_two, widths, scales),
        middle_scratch + (pltpu.VMEM((2 * cols, CH), F32),) + gram_scratch(cells + 2 * cols),
    )
    y2, dots = kernel_call(
        last_kernel(rows, devices), (cell_block, pltpu.VMEM((devices, CH), F32)),
        (mid1, *from_neighbours(mid1[-3:], mid1[:3], "lon", True), west, tall, east, stencil, y0, b0, y1, b1),
        middle_scratch,
    )
    shared = lax.all_to_all(dots.reshape(devices, 1, CH), ("lat", "lon"), 0, 0).reshape(devices, CH)
    coefficients, vector = kernel_call(
        final_kernel(entries),
        (jax.ShapeDtypeStruct((2, 2), F32), jax.ShapeDtypeStruct((cells, M * LEV), BF16)),
        (shared, y0, y1, y2, one, two, widths, scales), gram_scratch(cells)[:1],
    )
    return coefficients, vector.reshape(cols, rows, M * LEV)


def solution(mesh):
    return jax.shard_map(
        per_device,
        mesh=mesh,
        in_specs=(
            P("lon", "lat", None),
            P("lon", "lat", None),
            P("lon", "lat", None),
            P("lat"),
            P("lat"),
            P(),
        ),
        out_specs=(P(), P("lon", "lat", None)),
        check_vma=False,
    )
```
